16 devices in a mesh: dp: 2 (over z), tp: 8 (over y, x, core).
Axes of the slice: x: 2, y: 2, z: 2, core: 2. Of those that a mesh axis runs over, the one named last changes fastest.
Arguments:
- tokens: int32 [64], P('dp'), parts along dimension 0
- positions: int32 [64], P('dp'), parts along dimension 0
- self_keys: bfloat16 [2, 64, 448, 16, 64], P(None, 'dp', None, 'tp'), parts along dimension 1
- self_vals: bfloat16 [2, 64, 448, 16, 64], P(None, 'dp', None, 'tp'), parts along dimension 1
- cross_keys: bfloat16 [2, 64, 1500, 16, 64], P(None, 'dp', None, 'tp'), parts along dimension 1
- cross_vals: bfloat16 [2, 64, 1500, 16, 64], P(None, 'dp', None, 'tp'), parts along dimension 1
- embed_table: bfloat16 [52224, 1024], P('tp')
- pos_table: bfloat16 [448, 1024], replicated
- w_qkv: bfloat16 [2, 1024, 3, 16, 64], P(None, None, None, 'tp')
- w_cq: bfloat16 [2, 1024, 16, 64], P(None, None, 'tp')
- in_bias: float32 [2, 3, 16, 64], P(None, None, 'tp')
- w_out: bfloat16 [2, 2, 16, 64, 1024], P(None, None, 'tp')
- out_bias: float32 [2, 3, 1024], replicated
- w_fc1: bfloat16 [2, 1024, 4096], P(None, None, 'tp')
- b_fc1: float32 [2, 4096], P(None, 'tp')
- w_fc2: bfloat16 [2, 4096, 1024], P(None, 'tp')
- ln_layers: float32 [2, 3, 2, 1024], replicated
- ln_final: float32 [2, 1024], replicated
Outputs:
- output 1: float32 [64, 52224], P('dp', 'tp'), parts along dimension 0
- output 2: bfloat16 [2, 64, 448, 16, 64], P(None, 'dp', None, 'tp'), parts along dimension 1
- output 3: bfloat16 [2, 64, 448, 16, 64], P(None, 'dp', None, 'tp'), parts along dimension 1
There are 2 independent parts. The reference program is written for one: setup_inputs(seed, part) draws one part's arguments, and reference() takes and returns one part's arrays. A program takes and returns all parts, laid end to end along the dimension named above; an argument that names none is the same for every part.
All inputs are finite; a program needn't handle non-finite values.
Results may differ from the reference program's by a relative error of at most 0.0122829.
Values are sent between devices in bfloat16 or wider.
A program may use at most 1 GiB of HBM per device.

```python
import jax
import jax.numpy as jnp
from jax import lax

SEQ_BATCH = 32
D_MODEL = 1024
N_HEADS = 16
HEAD_DIM = 64
FF_DIM = 4096
VOCAB_SIZE = 51864
VOCAB_PAD = 52224
TEXT_CTX = 448
FRAMES = 1500
LAYERS = 2
FRAME_RANK = 8


def setup_inputs(seed: int = 0, part: int = 0) -> dict:
    base_key = jax.random.key(seed)
    part_keys = jax.random.split(jax.random.fold_in(base_key, part), 12)
    shared_keys = jax.random.split(jax.random.fold_in(base_key, 1000003), 14)

    def normal_draw(key_in, draw_shape, factor):
        return jax.random.normal(key_in, draw_shape, jnp.float32) * factor

    def structured(code_key, basis_key, noise_key, length, factor, noise_std):
        frame_codes = normal_draw(code_key, (SEQ_BATCH, length, FRAME_RANK), 1.0)
        code_basis = normal_draw(basis_key, (LAYERS, SEQ_BATCH, FRAME_RANK, N_HEADS, HEAD_DIM), factor * FRAME_RANK ** -0.5)
        mixed_rows = jnp.einsum('btr,lbrhe->lbthe', frame_codes, code_basis)
        return mixed_rows + normal_draw(noise_key, (LAYERS, SEQ_BATCH, length, N_HEADS, HEAD_DIM), noise_std)

    tokens = jax.random.randint(part_keys[0], (SEQ_BATCH,), 0, VOCAB_SIZE, dtype=jnp.int32)
    tokens = tokens.at[0].set(VOCAB_SIZE - 1).at[1].set(0)
    positions = jax.random.randint(part_keys[1], (SEQ_BATCH,), 0, TEXT_CTX, dtype=jnp.int32)
    positions = positions.at[0].set(TEXT_CTX - 1).at[1].set(0)
    self_keys = structured(part_keys[2], part_keys[3], part_keys[4], TEXT_CTX, 1.0, 0.3).astype(jnp.bfloat16)
    self_vals = structured(part_keys[2], part_keys[5], part_keys[6], TEXT_CTX, 1.0, 0.5).astype(jnp.bfloat16)
    cross_keys = structured(part_keys[7], part_keys[8], part_keys[9], FRAMES, 1.0, 0.3).astype(jnp.bfloat16)
    cross_vals = structured(part_keys[7], part_keys[10], part_keys[11], FRAMES, 1.0, 0.5).astype(jnp.bfloat16)
    embed_table = normal_draw(shared_keys[12], (VOCAB_PAD, D_MODEL), D_MODEL ** -0.25).astype(jnp.bfloat16)
    pos_table = normal_draw(shared_keys[13], (TEXT_CTX, D_MODEL), 0.5).astype(jnp.bfloat16)
    w_qkv = normal_draw(shared_keys[0], (LAYERS, D_MODEL, 3, N_HEADS, HEAD_DIM), D_MODEL ** -0.5).astype(jnp.bfloat16)
    w_cq = normal_draw(shared_keys[1], (LAYERS, D_MODEL, N_HEADS, HEAD_DIM), D_MODEL ** -0.5).astype(jnp.bfloat16)
    in_bias = normal_draw(shared_keys[2], (LAYERS, 3, N_HEADS, HEAD_DIM), 0.3)
    w_out = normal_draw(shared_keys[3], (LAYERS, 2, N_HEADS, HEAD_DIM, D_MODEL), D_MODEL ** -0.5).astype(jnp.bfloat16)
    out_bias = normal_draw(shared_keys[4], (LAYERS, 3, D_MODEL), 0.3)
    w_fc1 = normal_draw(shared_keys[5], (LAYERS, D_MODEL, FF_DIM), D_MODEL ** -0.5).astype(jnp.bfloat16)
    b_fc1 = normal_draw(shared_keys[6], (LAYERS, FF_DIM), 0.3)
    w_fc2 = normal_draw(shared_keys[7], (LAYERS, FF_DIM, D_MODEL), FF_DIM ** -0.5).astype(jnp.bfloat16)
    ln_layers = jnp.concatenate([1.0 + normal_draw(shared_keys[8], (LAYERS, 3, 1, D_MODEL), 0.2), normal_draw(shared_keys[9], (LAYERS, 3, 1, D_MODEL), 0.2)], axis=2)
    ln_final = jnp.concatenate([1.0 + normal_draw(shared_keys[10], (1, D_MODEL), 0.2), normal_draw(shared_keys[11], (1, D_MODEL), 0.2)], axis=0)
    return {'tokens': tokens, 'positions': positions, 'self_keys': self_keys, 'self_vals': self_vals, 'cross_keys': cross_keys, 'cross_vals': cross_vals, 'embed_table': embed_table, 'pos_table': pos_table, 'w_qkv': w_qkv, 'w_cq': w_cq, 'in_bias': in_bias, 'w_out': w_out, 'out_bias': out_bias, 'w_fc1': w_fc1, 'b_fc1': b_fc1, 'w_fc2': w_fc2, 'ln_layers': ln_layers, 'ln_final': ln_final}


def layer_norm(resid_in, ln_gain, ln_shift):
    row_mean = jnp.mean(resid_in, axis=-1, keepdims=True)
    centred = resid_in - row_mean
    variance = jnp.mean(centred * centred, axis=-1, keepdims=True)
    return (centred * lax.rsqrt(variance + 1e-5) * ln_gain + ln_shift).astype(jnp.bfloat16)


def attend(queries, key_rows, val_rows, mask_add):
    scores = jnp.einsum('bhe,bthe->bht', queries.astype(jnp.float32), key_rows.astype(jnp.float32)) * (HEAD_DIM ** -0.5) + mask_add
    weights = jax.nn.softmax(scores, axis=-1).astype(jnp.bfloat16)
    mixed_vals = jnp.einsum('bht,bthe->bhe', weights.astype(jnp.float32), val_rows.astype(jnp.float32))
    return mixed_vals.astype(jnp.bfloat16)


def project_out(attended, out_weight):
    summed = jnp.einsum('bhe,hed->bd', attended.astype(jnp.float32), out_weight.astype(jnp.float32))
    return summed.astype(jnp.bfloat16).astype(jnp.float32)


def reference(tokens, positions, self_keys, self_vals, cross_keys, cross_vals, embed_table, pos_table, w_qkv, w_cq, in_bias, w_out, out_bias, w_fc1, b_fc1, w_fc2, ln_layers, ln_final):
    residual = embed_table[tokens].astype(jnp.float32) + pos_table[positions].astype(jnp.float32)
    cache_pos = jnp.arange(TEXT_CTX)[None, :]
    write_mask = (cache_pos == positions[:, None])[:, :, None, None]
    self_mask = jnp.where(cache_pos <= positions[:, None], 0.0, -1e30)[:, None, :]

    def layer_body(resid_in, layer_args):
        (cache_keys, cache_vals, frame_keys, frame_vals, qkv_weight, cq_weight, bias_in, out_weight, bias_out, fc1_weight, fc1_bias, fc2_weight, ln_params) = layer_args
        hidden = layer_norm(resid_in, ln_params[0, 0], ln_params[0, 1])
        projected = jnp.einsum('bd,dthe->bthe', hidden.astype(jnp.float32), qkv_weight.astype(jnp.float32))
        queries = (projected[:, 0] + bias_in[0]).astype(jnp.bfloat16)
        key_new = projected[:, 1].astype(jnp.bfloat16)
        val_new = (projected[:, 2] + bias_in[1]).astype(jnp.bfloat16)
        keys_now = jnp.where(write_mask, key_new[:, None], cache_keys)
        vals_now = jnp.where(write_mask, val_new[:, None], cache_vals)
        resid_mid = resid_in + project_out(attend(queries, keys_now, vals_now, self_mask), out_weight[0]) + bias_out[0]
        hidden = layer_norm(resid_mid, ln_params[1, 0], ln_params[1, 1])
        cross_q = (jnp.einsum('bd,dhe->bhe', hidden.astype(jnp.float32), cq_weight.astype(jnp.float32)) + bias_in[2]).astype(jnp.bfloat16)
        resid_mid = resid_mid + project_out(attend(cross_q, frame_keys, frame_vals, 0.0), out_weight[1]) + bias_out[1]
        hidden = layer_norm(resid_mid, ln_params[2, 0], ln_params[2, 1])
        fc1_out = jnp.dot(hidden, fc1_weight, preferred_element_type=jnp.float32) + fc1_bias
        active = jax.nn.gelu(fc1_out, approximate=False).astype(jnp.bfloat16)
        fc2_out = jnp.dot(active, fc2_weight, preferred_element_type=jnp.float32).astype(jnp.bfloat16).astype(jnp.float32)
        resid_out = resid_mid + fc2_out + bias_out[2]
        return resid_out, (keys_now, vals_now)

    residual, new_caches = lax.scan(layer_body, residual, (self_keys, self_vals, cross_keys, cross_vals, w_qkv, w_cq, in_bias, w_out, out_bias, w_fc1, b_fc1, w_fc2, ln_layers))
    final_hidden = layer_norm(residual, ln_final[0], ln_final[1])
    logits = jnp.dot(final_hidden, embed_table.T, preferred_element_type=jnp.float32)
    return logits, new_caches[0], new_caches[1]
```

```python
import functools
import jax
import jax.numpy as jnp
from jax import lax
from jax.experimental import pallas as pl
from jax.experimental.pallas import tpu as pltpu
from jax.sharding import PartitionSpec as P

MESH = pl.DeviceIdType.MESH
F32 = jnp.float32
BF16 = jnp.bfloat16
NT = (((1,), (1,)), ((), ()))
TP = 8
HALVES = 2
PARITY = 2


def gather_kernel(tok_ref, pos_ref, emb_hbm, pos_hbm, picked_ref, posrow_ref, prow_ref, ebuf, pbuf, xbuf, ybuf, sem):
    shard_rows = emb_hbm.shape[0]
    n = tok_ref.shape[0]
    base = lax.axis_index('tp') * shard_rows

    def start(b, carry):
        tid = jnp.clip(tok_ref[b] - base, 0, shard_rows - 1)
        pid = pos_ref[b]
        pltpu.make_async_copy(emb_hbm.at[pl.ds(pl.multiple_of(tid // 8 * 8, 8), 8), :], ebuf.at[b], sem.at[0]).start()
        pltpu.make_async_copy(pos_hbm.at[pl.ds(pl.multiple_of(pid // 8 * 8, 8), 8), :], pbuf.at[b], sem.at[1]).start()
        return carry

    lax.fori_loop(0, n, start, 0)
    pltpu.make_async_copy(ebuf, ebuf, sem.at[0]).wait()
    pltpu.make_async_copy(pbuf, pbuf, sem.at[1]).wait()
    row8 = lax.broadcasted_iota(jnp.int32, (8, 1), 0)

    def pick(b, carry):
        tid = tok_ref[b] - base
        owned = (tid >= 0) & (tid < shard_rows)
        sub = jnp.where(owned, lax.rem(jnp.clip(tid, 0, shard_rows - 1), 8), 8)
        pid = pos_ref[b]
        erow = jnp.sum(jnp.where(row8 == sub, ebuf[b].astype(F32), 0.0), axis=0, keepdims=True)
        prow = jnp.sum(jnp.where(row8 == lax.rem(pid, 8), pbuf[b].astype(F32), 0.0), axis=0, keepdims=True)
        xbuf[pl.ds(b, 1), :] = erow
        ybuf[pl.ds(b, 1), :] = prow
        prow_ref[pl.ds(b, 1), :] = jnp.full((1, 128), pid, jnp.int32)
        return carry

    lax.fori_loop(0, n, pick, 0)
    picked_ref[...] = xbuf[...].astype(BF16)
    posrow_ref[...] = ybuf[...]


def norm_rows(x, ln):
    mean = jnp.mean(x, axis=-1, keepdims=True)
    centred = x - mean
    var = jnp.mean(centred * centred, axis=-1, keepdims=True)
    return (centred * lax.rsqrt(var + 1e-5) * ln[0:1, :] + ln[1:2, :]).astype(BF16)


def block_diag(q8):
    lane = lax.broadcasted_iota(jnp.int32, (8, 128), 1)
    qf = q8.astype(F32)
    both = jnp.concatenate([jnp.where(lane < 64, qf, 0.0), jnp.where(lane < 64, 0.0, qf)], axis=0)
    row = lax.rem(lax.broadcasted_iota(jnp.int32, (16, 128), 0), 8)
    blocks = [jnp.where(row == b, both, 0.0).astype(BF16) for b in range(8)]
    return both, jnp.concatenate(blocks, axis=1)


def fold_heads(o16):
    lane = lax.broadcasted_iota(jnp.int32, (8, 128), 1)
    row = lax.broadcasted_iota(jnp.int32, (8, 128), 0)
    out = jnp.zeros((8, 128), F32)
    for b in range(8):
        blk = jnp.where(lane < 64, o16[0:8, b * 128:(b + 1) * 128], o16[8:16, b * 128:(b + 1) * 128])
        out = jnp.where(row == b, blk, out)
    return out


def decoder_kernel(dims, pos_smem, picked_ref, posrow_ref, prow_ref, in_bias, out_bias, b_fc1, ln_layers, ln_final,
                   sk_hbm, sv_hbm, ck_hbm, cv_hbm, emb_hbm, wqkv_hbm, wcq_hbm, wout_hbm, fc1_hbm, fc2_hbm,
                   kvo, eo, fh_ref,
                   kbuf, vbuf, wqkv, wcq, wout, fc1, fc2,
                   xres, part, part0, rs_recv, rs_recv0, ag_full, qscr, oscr, knew, vnew,
                   self_sem, cross_sem, w_sem, e_sem, send_sem, recv_sem):
    layers, batch, ctx, frames = dims
    me = lax.axis_index('tp')
    ko, vo = kvo.at[0], kvo.at[1]
    hb = batch // HALVES
    rows_per = 128

    def self_copy(layer, which):
        src, dst = ((sk_hbm, ko), (sv_hbm, vo))[which]
        return pltpu.make_async_copy(src.at[layer], dst.at[layer], self_sem.at[layer, which])

    def cross_copy(layer, which, octet):
        src, dst = ((ck_hbm, kbuf), (cv_hbm, vbuf))[which]
        at = pl.ds(pl.multiple_of(octet * 1024, 1024), 1024)
        return pltpu.make_async_copy(src.at[layer, at, :], dst.at[at, :], cross_sem.at[layer, which, octet])

    weights = ((wqkv_hbm, wqkv), (wout_hbm, wout), (wcq_hbm, wcq), (fc1_hbm, fc1), (fc2_hbm, fc2))

    def w_copy(which, layer):
        src, dst = weights[which]
        return pltpu.make_async_copy(src.at[layer], dst.at[layer], w_sem.at[which, layer])

    w_copy(0, 0).start()
    self_copy(0, 0).start()
    self_copy(0, 1).start()
    w_copy(1, 0).start()
    w_copy(2, 0).start()
    for octet in range(batch // 8):
        cross_copy(0, 0, octet).start()
        cross_copy(0, 1, octet).start()
    w_copy(3, 0).start()
    w_copy(4, 0).start()
    w_copy(0, 1).start()
    self_copy(1, 0).start()
    self_copy(1, 1).start()
    for which in range(1, 5):
        w_copy(which, 1).start()

    barrier = pltpu.get_barrier_semaphore()
    for k in range(1, TP):
        pl.semaphore_signal(barrier, 1, device_id={'tp': lax.rem(me + k, TP)}, device_id_type=MESH)
    pl.semaphore_wait(barrier, TP - 1)

    def bufs(ph, s):
        if ph == 0:
            return part0.at[s], rs_recv0.at[s], ag_full.at[0, s]
        slot = ph % PARITY
        return part.at[slot, s], rs_recv.at[slot, s], ag_full.at[slot, s]

    def rs_start(ph, s):
        src, dst, _ = bufs(ph, s)
        for k in range(1, TP):
            peer = lax.rem(me + k, TP)
            pltpu.make_async_remote_copy(src.at[peer], dst.at[k - 1], send_sem.at[ph, s, 0], recv_sem.at[ph, s, 0],
                                         device_id={'tp': peer}, device_id_type=MESH).start()

    def wait_for(ref, sem):
        pltpu.make_async_copy(ref, ref, sem).wait()

    def rs_finish(ph, s):
        src, dst, full = bufs(ph, s)
        wait_for(dst, recv_sem.at[ph, s, 0])
        total = src[me].astype(F32)
        for k in range(TP - 1):
            total = total + dst[k].astype(F32)
        full[me] = total.astype(BF16)
        for k in range(1, TP):
            peer = lax.rem(me + k, TP)
            pltpu.make_async_remote_copy(full.at[me], full.at[me], send_sem.at[ph, s, 1], recv_sem.at[ph, s, 1],
                                         device_id={'tp': peer}, device_id_type=MESH).start()
        wait_for(dst, send_sem.at[ph, s, 0])

    def ag_finish(ph, s):
        _, _, full = bufs(ph, s)
        seven = full.at[pl.ds(0, TP - 1)]
        wait_for(seven, recv_sem.at[ph, s, 1])
        wait_for(seven, send_sem.at[ph, s, 1])
        return jnp.concatenate([full[j].astype(F32) for j in range(TP)], axis=1)

    def put_part(ph, s, value):
        dst = bufs(ph, s)[0]
        for j in range(TP):
            dst[j] = value[:, j * 128:(j + 1) * 128]

    def head_bias(layer, which):
        b = in_bias[layer, which]
        return jnp.concatenate([b[0:1, :], b[1:2, :]], axis=1)

    def half(s):
        return pl.ds(s * hb, hb)

    def self_block(layer, s):
        hidden = norm_rows(xres[half(s), :], ln_layers[layer, 0])
        proj = lax.dot_general(hidden, wqkv[layer], NT, preferred_element_type=F32)
        qscr[half(s), :] = (proj[:, 0:128] + head_bias(layer, 0)).astype(BF16).astype(F32)
        knew[layer, half(s), :] = proj[:, 128:256].astype(BF16).astype(F32)
        vnew[layer, half(s), :] = (proj[:, 256:384] + head_bias(layer, 1)).astype(BF16).astype(F32)

        def octet_body(i, carry):
            octet = s * (hb // 8) + i
            r8 = pl.ds(pl.multiple_of(octet * 8, 8), 8)
            at = pl.ds(pl.multiple_of(octet * 1024, 1024), 1024)
            both, qbd = block_diag(qscr[r8, :])
            p8 = prow_ref[r8, :][:, 0:1]
            past = jnp.dot(qbd, ko[layer, at, :], preferred_element_type=F32) * 0.125
            t = lax.broadcasted_iota(jnp.int32, (16, ctx), 1)
            past = jnp.where(t < jnp.concatenate([p8, p8], axis=0), past, -1e30)
            kn = knew[layer, r8, :]
            vn = vnew[layer, r8, :]
            new = jnp.sum(both * jnp.concatenate([kn, kn], axis=0), axis=1, keepdims=True) * 0.125
            peak = jnp.maximum(jnp.max(past, axis=1, keepdims=True), new)
            past_e = jnp.exp(past - peak)
            new_e = jnp.exp(new - peak)
            denom = jnp.sum(past_e, axis=1, keepdims=True) + new_e
            past_w = (past_e / denom).astype(BF16)
            new_w = (new_e / denom).astype(BF16).astype(F32)
            o16 = lax.dot_general(past_w, vo[layer, at, :], NT, preferred_element_type=F32)
            lane = lax.broadcasted_iota(jnp.int32, (8, 128), 1)
            oscr[r8, :] = fold_heads(o16) + jnp.where(lane < 64, new_w[0:8], new_w[8:16]) * vn
            return carry

        lax.fori_loop(0, hb // 8, octet_body, 0)
        return jnp.dot(oscr[half(s), :].astype(BF16), wout[layer, 0], preferred_element_type=F32)

    def cross_block(layer, s):
        hidden = norm_rows(xres[half(s), :], ln_layers[layer, 1])
        proj = lax.dot_general(hidden, wcq[layer], NT, preferred_element_type=F32)
        qscr[half(s), :] = (proj + head_bias(layer, 2)).astype(BF16).astype(F32)

        def octet_body(i, carry):
            octet = s * (hb // 8) + i
            r8 = pl.ds(pl.multiple_of(octet * 8, 8), 8)
            at = pl.ds(pl.multiple_of(octet * 1024, 1024), 1024)
            _, qbd = block_diag(qscr[r8, :])
            cross_copy(layer, 0, octet).wait()
            scores = jnp.dot(qbd, kbuf[at, :], preferred_element_type=F32) * 0.125
            if layer + 1 < layers:
                cross_copy(layer + 1, 0, octet).start()
            peak = jnp.max(scores, axis=1, keepdims=True)
            exps = jnp.exp(scores - peak)
            w = (exps / jnp.sum(exps, axis=1, keepdims=True)).astype(BF16)
            cross_copy(layer, 1, octet).wait()
            o16 = lax.dot_general(w, vbuf[at, :], NT, preferred_element_type=F32)
            if layer + 1 < layers:
                cross_copy(layer + 1, 1, octet).start()
            oscr[r8, :] = fold_heads(o16)
            return carry

        lax.fori_loop(0, hb // 8, octet_body, 0)
        return jnp.dot(oscr[half(s), :].astype(BF16), wout[layer, 1], preferred_element_type=F32)

    def mlp_block(layer, s):
        hidden = norm_rows(xres[half(s), :], ln_layers[layer, 2])
        pre = jnp.dot(hidden, fc1[layer], preferred_element_type=F32) + b_fc1[layer:layer + 1, :]
        active = (0.5 * pre * (1.0 + lax.erf(pre * (0.5 ** 0.5)))).astype(BF16)
        return jnp.dot(active, fc2[layer], preferred_element_type=F32)

    def write_new(layer, s):
        t = lax.broadcasted_iota(jnp.int32, (rows_per, ctx), 1)
        for new, cache in ((knew, ko), (vnew, vo)):
            cols = new[layer, half(s), :].T
            for i in range(hb):
                b = s * hb + i
                at = pl.ds(b * rows_per, rows_per)
                old = cache[layer, at, :].astype(F32)
                cache[layer, at, :] = jnp.where(t == pos_smem[b], cols[:, i:i + 1], old).astype(BF16)

    for s in range(HALVES):
        put_part(0, s, picked_ref[half(s), :])
        rs_start(0, s)
    for s in range(HALVES):
        rs_finish(0, s)
    for s in range(HALVES):
        xres[half(s), :] = ag_finish(0, s) + posrow_ref[half(s), :]
        if s == 0:
            w_copy(0, 0).wait()
            self_copy(0, 0).wait()
            self_copy(0, 1).wait()
            w_copy(1, 0).wait()
        put_part(1, s, self_block(0, s))
        rs_start(1, s)
    ph = 1
    for layer in range(layers):
        for kind in range(3):
            if kind == 0:
                for s in range(HALVES):
                    write_new(layer, s)
            if layer == 0 and kind == 0:
                pltpu.make_async_copy(emb_hbm, eo, e_sem).start()
            for s in range(HALVES):
                rs_finish(ph, s)
            for s in range(HALVES):
                xres[half(s), :] = xres[half(s), :] + ag_finish(ph, s) + out_bias[kind, layer:layer + 1, :]
                nxt = layer * 3 + kind + 1
                if nxt == layers * 3:
                    fh_ref[half(s), :] = norm_rows(xres[half(s), :], ln_final)
                    continue
                nl, nk = divmod(nxt, 3)
                if s == 0:
                    if nk == 0:
                        w_copy(0, nl).wait()
                        self_copy(nl, 0).wait()
                        self_copy(nl, 1).wait()
                        w_copy(1, nl).wait()
                    if nk == 1:
                        w_copy(2, nl).wait()
                    if nk == 2:
                        w_copy(3, nl).wait()
                        w_copy(4, nl).wait()
                put_part(ph + 1, s, (self_block, cross_block, mlp_block)[nk](nl, s))
                rs_start(ph + 1, s)
            ph += 1
    pltpu.make_async_copy(emb_hbm, eo, e_sem).wait()


def final_kernel(kv_ref, e_ref, fh_ref, logits_ref, ko_hbm, vo_hbm, sem):
    layers = kv_ref.shape[1]
    copies = []
    for layer in range(layers):
        for which, dst in enumerate((ko_hbm, vo_hbm)):
            c = pltpu.make_async_copy(kv_ref.at[which, layer], dst.at[layer], sem.at[layer, which])
            c.start()
            copies.append(c)
    fh = fh_ref[...]
    step = 384

    def body(i, carry):
        at = pl.ds(pl.multiple_of(i * step, step), step)
        logits_ref[:, at] = lax.dot_general(fh, e_ref[at, :], NT, preferred_element_type=F32)
        return carry

    lax.fori_loop(0, e_ref.shape[0] // step, body, 0)
    for c in copies:
        c.wait()


def solution(mesh):
    vm = pl.BlockSpec(memory_space=pltpu.VMEM)
    sm = pl.BlockSpec(memory_space=pltpu.SMEM)
    hbm = pl.BlockSpec(memory_space=pltpu.HBM)

    def local_step(tokens, positions, self_keys, self_vals, cross_keys, cross_vals, embed_table, pos_table, w_qkv, w_cq, in_bias, w_out, out_bias, w_fc1, b_fc1, w_fc2, ln_layers, ln_final):
        batch = tokens.shape[0]
        layers, _, ctx, heads, hd = self_keys.shape
        frames = cross_keys.shape[2]
        vocab, d = embed_table.shape
        ff = w_fc1.shape[2]
        rows = batch * heads * hd
        hb = batch // HALVES

        def flat(cache):
            return cache.transpose(0, 1, 3, 4, 2).reshape(layers, rows, cache.shape[2])

        picked, posrow, prow = pl.pallas_call(
            gather_kernel,
            out_shape=(jax.ShapeDtypeStruct((batch, d), BF16), jax.ShapeDtypeStruct((batch, d), F32), jax.ShapeDtypeStruct((batch, 128), jnp.int32)),
            in_specs=[sm, sm, hbm, hbm], out_specs=(vm, vm, vm),
            scratch_shapes=[pltpu.VMEM((batch, 8, d), BF16), pltpu.VMEM((batch, 8, d), BF16), pltpu.VMEM((batch, d), F32), pltpu.VMEM((batch, d), F32), pltpu.SemaphoreType.DMA((2,))],
            compiler_params=pltpu.CompilerParams(vmem_limit_bytes=60 * 2 ** 20),
            name='gather_rows',
        )(tokens, positions, embed_table, pos_table)

        kvo, eo, fh = pl.pallas_call(
            functools.partial(decoder_kernel, (layers, batch, ctx, frames)),
            out_shape=(pltpu.VMEM((2, layers, rows, ctx), BF16), pltpu.VMEM((vocab, d), BF16), jax.ShapeDtypeStruct((batch, d), BF16)),
            in_specs=[sm] + [vm] * 8 + [hbm] * 10,
            out_specs=(vm, vm, vm),
            scratch_shapes=[
                pltpu.VMEM((rows, frames), BF16), pltpu.VMEM((rows, frames), BF16),
                pltpu.VMEM((layers, 3 * heads * hd, d), BF16), pltpu.VMEM((layers, heads * hd, d), BF16),
                pltpu.VMEM((layers, 2, heads * hd, d), BF16), pltpu.VMEM((layers, d, ff), BF16), pltpu.VMEM((layers, ff, d), BF16),
                pltpu.VMEM((batch, d), F32),
                pltpu.VMEM((PARITY, HALVES, TP, hb, 128), F32), pltpu.VMEM((HALVES, TP, hb, 128), BF16),
                pltpu.VMEM((PARITY, HALVES, TP - 1, hb, 128), F32), pltpu.VMEM((HALVES, TP - 1, hb, 128), BF16),
                pltpu.VMEM((PARITY, HALVES, TP, hb, 128), BF16),
                pltpu.VMEM((batch, 128), F32), pltpu.VMEM((batch, 128), F32),
                pltpu.VMEM((layers, batch, 128), F32), pltpu.VMEM((layers, batch, 128), F32),
                pltpu.SemaphoreType.DMA((layers, 2)), pltpu.SemaphoreType.DMA((layers, 2, batch // 8)),
                pltpu.SemaphoreType.DMA((5, layers)), pltpu.SemaphoreType.DMA,
                pltpu.SemaphoreType.DMA((3 * layers + 1, HALVES, 2)), pltpu.SemaphoreType.DMA((3 * layers + 1, HALVES, 2)),
            ],
            compiler_params=pltpu.CompilerParams(collective_id=0, has_side_effects=True, vmem_limit_bytes=67 * 2 ** 19),
            name='decoder_layers',
        )(positions, picked, posrow, prow, in_bias, out_bias.transpose(1, 0, 2), b_fc1, ln_layers, ln_final,
          flat(self_keys), flat(self_vals), flat(cross_keys), flat(cross_vals), embed_table,
          w_qkv.transpose(0, 2, 3, 4, 1).reshape(layers, 3 * heads * hd, d), w_cq.transpose(0, 2, 3, 1).reshape(layers, heads * hd, d),
          w_out.reshape(layers, 2, heads * hd, d), w_fc1, w_fc2)

        logits, nk, nv = pl.pallas_call(
            final_kernel,
            out_shape=(jax.ShapeDtypeStruct((batch, vocab), F32), jax.ShapeDtypeStruct((layers, rows, ctx), BF16), jax.ShapeDtypeStruct((layers, rows, ctx), BF16)),
            in_specs=[vm] * 3, out_specs=(vm, hbm, hbm),
            scratch_shapes=[pltpu.SemaphoreType.DMA((layers, 2))],
            compiler_params=pltpu.CompilerParams(vmem_limit_bytes=2 * 2 ** 20),
            name='final_logits',
        )(kvo, eo, fh)

        def unflat(cache):
            return cache.reshape(layers, batch, heads, hd, ctx).transpose(0, 1, 4, 2, 3)

        return logits, unflat(nk), unflat(nv)

    batch_spec = P('dp')
    cache_spec = P(None, 'dp', None, 'tp', None)
    in_specs = (batch_spec, batch_spec, cache_spec, cache_spec, cache_spec, cache_spec, P('tp', None), P(None, None), P(None, None, None, 'tp', None), P(None, None, 'tp', None), P(None, None, 'tp', None), P(None, None, 'tp', None, None), P(None, None, None), P(None, None, 'tp'), P(None, 'tp'), P(None, 'tp', None), P(None, None, None, None), P(None, None))
    out_specs = (P('dp', 'tp'), cache_spec, cache_spec)
    return jax.shard_map(local_step, mesh=mesh, in_specs=in_specs, out_specs=out_specs, check_vma=False)
```

```python
import functools
import jax
import jax.numpy as jnp
from jax import lax
from jax.experimental import pallas as pl
from jax.experimental.pallas import tpu as pltpu
from jax.sharding import PartitionSpec as P

MESH = pl.DeviceIdType.MESH
F32 = jnp.float32
BF16 = jnp.bfloat16
NT = (((1,), (1,)), ((), ()))
TN = (((0,), (0,)), ((), ()))
TP = 8
HALVES = 2
PARITY = 2


def gather_kernel(tok_ref, pos_ref, tokv_ref, posv_ref, emb_hbm, pos_hbm, picked_ref, posrow_ref, ebuf, pbuf, sem):
    shard_rows = emb_hbm.shape[0]
    n = tok_ref.shape[0]
    base = lax.axis_index('tp') * shard_rows

    def start(b, carry):
        tid = jnp.clip(tok_ref[b] - base, 0, shard_rows - 1)
        pid = pos_ref[b]
        at = pl.ds(pl.multiple_of(b * 16, 16), 16)
        pltpu.make_async_copy(emb_hbm.at[pl.ds(pl.multiple_of(tid // 16 * 16, 16), 16), :], ebuf.at[at, :], sem.at[0]).start()
        pltpu.make_async_copy(pos_hbm.at[pl.ds(pl.multiple_of(pid // 16 * 16, 16), 16), :], pbuf.at[at, :], sem.at[1]).start()
        return carry

    lax.fori_loop(0, n, start, 0, unroll=4)
    tid = tokv_ref[...] - base
    owned = (tid >= 0) & (tid < shard_rows)
    lane16 = lax.broadcasted_iota(jnp.int32, (1, n), 1) * 16
    tok_row = jnp.where(owned, lane16 + jnp.clip(tid, 0, shard_rows - 1) % 16, -1)
    pos_row = lane16 + posv_ref[...] % 16
    row = lax.broadcasted_iota(jnp.int32, (16 * n, n), 0)
    tok_hot = jnp.where(row == tok_row, 1.0, 0.0).astype(BF16)
    pos_hot = jnp.where(row == pos_row, 1.0, 0.0).astype(BF16)
    pltpu.make_async_copy(ebuf, ebuf, sem.at[0]).wait()
    picked_ref[...] = lax.dot_general(tok_hot, ebuf[...], TN, preferred_element_type=F32).astype(BF16)
    pltpu.make_async_copy(pbuf, pbuf, sem.at[1]).wait()
    posrow_ref[...] = lax.dot_general(pos_hot, pbuf[...], TN, preferred_element_type=F32)


def norm_rows(x, ln):
    mean = jnp.mean(x, axis=-1, keepdims=True)
    centred = x - mean
    var = jnp.mean(centred * centred, axis=-1, keepdims=True)
    return (centred * lax.rsqrt(var + 1e-5) * ln[0:1, :] + ln[1:2, :]).astype(BF16)


def block_diag(q8):
    lane = lax.broadcasted_iota(jnp.int32, (8, 128), 1)
    qf = q8.astype(F32)
    both = jnp.concatenate([jnp.where(lane < 64, qf, 0.0), jnp.where(lane < 64, 0.0, qf)], axis=0)
    row = lax.rem(lax.broadcasted_iota(jnp.int32, (16, 128), 0), 8)
    blocks = [jnp.where(row == b, both, 0.0).astype(BF16) for b in range(8)]
    return both, jnp.concatenate(blocks, axis=1)


def fold_heads(o16):
    lane = lax.broadcasted_iota(jnp.int32, (8, 128), 1)
    row = lax.broadcasted_iota(jnp.int32, (8, 128), 0)
    out = jnp.zeros((8, 128), F32)
    for b in range(8):
        blk = jnp.where(lane < 64, o16[0:8, b * 128:(b + 1) * 128], o16[8:16, b * 128:(b + 1) * 128])
        out = jnp.where(row == b, blk, out)
    return out


def decoder_kernel(dims, pos_smem, picked_ref, posrow_ref, in_bias_hbm, out_bias_hbm, b_fc1_hbm, ln_layers_hbm, ln_final_hbm,
                   sk_hbm, sv_hbm, ck_hbm, cv_hbm, emb_hbm, wqkv_hbm, wcq_hbm, wout_hbm, fc1_hbm, fc2_hbm,
                   kvo, eo, fh_ref,
                   in_bias, out_bias, b_fc1, ln_layers, ln_final, kbuf, vbuf, wqkv, wcq, wout, fc1, fc2,
                   xres, part, part0, rs_recv, rs_recv0, ag_full, qscr, oscr, knew, vnew,
                   small_sem, self_sem, cross_sem, w_sem, e_sem, send_sem, recv_sem):
    layers, batch, ctx, frames = dims
    me = lax.axis_index('tp')
    ko, vo = kvo.at[0], kvo.at[1]
    hb = batch // HALVES
    rows_per = 128

    def self_copy(layer, which):
        src, dst = ((sk_hbm, ko), (sv_hbm, vo))[which]
        return pltpu.make_async_copy(src.at[layer], dst.at[layer], self_sem.at[layer, which])

    def cross_copy(layer, which, octet):
        src, dst = ((ck_hbm, kbuf), (cv_hbm, vbuf))[which]
        at = pl.ds(pl.multiple_of(octet * 1024, 1024), 1024)
        return pltpu.make_async_copy(src.at[layer, at, :], dst.at[at, :], cross_sem.at[layer, which, octet])

    weights = ((wqkv_hbm, wqkv), (wout_hbm, wout), (wcq_hbm, wcq), (fc1_hbm, fc1), (fc2_hbm, fc2))

    def w_copy(which, layer):
        src, dst = weights[which]
        return pltpu.make_async_copy(src.at[layer], dst.at[layer], w_sem.at[which, layer])

    small = [pltpu.make_async_copy(src, dst, small_sem.at[i]) for i, (src, dst) in enumerate((
        (ln_layers_hbm, ln_layers), (in_bias_hbm, in_bias), (out_bias_hbm, out_bias), (b_fc1_hbm, b_fc1), (ln_final_hbm, ln_final)))]
    for c in small:
        c.start()
    w_copy(0, 0).start()
    self_copy(0, 0).start()
    self_copy(0, 1).start()
    w_copy(1, 0).start()
    w_copy(2, 0).start()

    barrier = pltpu.get_barrier_semaphore()
    for k in range(1, TP):
        pl.semaphore_signal(barrier, 1, device_id={'tp': lax.rem(me + k, TP)}, device_id_type=MESH)
    pl.semaphore_wait(barrier, TP - 1)

    def bufs(ph, s):
        if ph == 0:
            return part0.at[s], rs_recv0.at[s], ag_full.at[0, s]
        slot = ph % PARITY
        return part.at[slot, s], rs_recv.at[slot, s], ag_full.at[slot, s]

    def rs_start(ph, s):
        src, dst, _ = bufs(ph, s)
        for k in range(1, TP):
            peer = lax.rem(me + k, TP)
            pltpu.make_async_remote_copy(src.at[peer], dst.at[k - 1], send_sem.at[ph, s, 0], recv_sem.at[ph, s, 0],
                                         device_id={'tp': peer}, device_id_type=MESH).start()

    def wait_for(ref, sem):
        pltpu.make_async_copy(ref, ref, sem).wait()

    def rs_finish(ph, s):
        src, dst, full = bufs(ph, s)
        wait_for(dst, recv_sem.at[ph, s, 0])
        total = src[me].astype(F32)
        for k in range(TP - 1):
            total = total + dst[k].astype(F32)
        full[me] = total.astype(BF16)
        for k in range(1, TP):
            peer = lax.rem(me + k, TP)
            pltpu.make_async_remote_copy(full.at[me], full.at[me], send_sem.at[ph, s, 1], recv_sem.at[ph, s, 1],
                                         device_id={'tp': peer}, device_id_type=MESH).start()
        wait_for(dst, send_sem.at[ph, s, 0])

    def ag_finish(ph, s):
        _, _, full = bufs(ph, s)
        seven = full.at[pl.ds(0, TP - 1)]
        wait_for(seven, recv_sem.at[ph, s, 1])
        wait_for(seven, send_sem.at[ph, s, 1])
        return jnp.concatenate([full[j].astype(F32) for j in range(TP)], axis=1)

    def put_part(ph, s, value):
        dst = bufs(ph, s)[0]
        for j in range(TP):
            dst[j] = value[:, j * 128:(j + 1) * 128]

    def head_bias(layer, which):
        b = in_bias[layer, which]
        return jnp.concatenate([b[0:1, :], b[1:2, :]], axis=1)

    def half(s):
        return pl.ds(s * hb, hb)

    def self_block(layer, s):
        hidden = norm_rows(xres[half(s), :], ln_layers[layer, 0])
        proj = lax.dot_general(hidden, wqkv[layer], NT, preferred_element_type=F32)
        qscr[half(s), :] = (proj[:, 0:128] + head_bias(layer, 0)).astype(BF16).astype(F32)
        knew[layer, half(s), :] = proj[:, 128:256].astype(BF16).astype(F32)
        vnew[layer, half(s), :] = (proj[:, 256:384] + head_bias(layer, 1)).astype(BF16).astype(F32)

        def octet_body(i, carry):
            octet = s * (hb // 8) + i
            r8 = pl.ds(pl.multiple_of(octet * 8, 8), 8)
            at = pl.ds(pl.multiple_of(octet * 1024, 1024), 1024)
            both, qbd = block_diag(qscr[r8, :])
            seq = lax.rem(lax.broadcasted_iota(jnp.int32, (16, 1), 0), 8)
            limit = jnp.zeros((16, 1), jnp.int32)
            for b in range(8):
                limit = jnp.where(seq == b, pos_smem[octet * 8 + b], limit)
            past = jnp.dot(qbd, ko[layer, at, :], preferred_element_type=F32) * 0.125
            t = lax.broadcasted_iota(jnp.int32, (16, ctx), 1)
            past = jnp.where(t < limit, past, -1e30)
            kn = knew[layer, r8, :]
            vn = vnew[layer, r8, :]
            new = jnp.sum(both * jnp.concatenate([kn, kn], axis=0), axis=1, keepdims=True) * 0.125
            peak = jnp.maximum(jnp.max(past, axis=1, keepdims=True), new)
            past_e = jnp.exp(past - peak)
            new_e = jnp.exp(new - peak)
            denom = jnp.sum(past_e, axis=1, keepdims=True) + new_e
            past_w = (past_e / denom).astype(BF16)
            new_w = (new_e / denom).astype(BF16).astype(F32)
            o16 = lax.dot_general(past_w, vo[layer, at, :], NT, preferred_element_type=F32)
            lane = lax.broadcasted_iota(jnp.int32, (8, 128), 1)
            oscr[r8, :] = fold_heads(o16) + jnp.where(lane < 64, new_w[0:8], new_w[8:16]) * vn
            return carry

        lax.fori_loop(0, hb // 8, octet_body, 0)
        return jnp.dot(oscr[half(s), :].astype(BF16), wout[layer, 0], preferred_element_type=F32)

    def cross_block(layer, s):
        hidden = norm_rows(xres[half(s), :], ln_layers[layer, 1])
        proj = lax.dot_general(hidden, wcq[layer], NT, preferred_element_type=F32)
        qscr[half(s), :] = (proj + head_bias(layer, 2)).astype(BF16).astype(F32)

        def octet_body(i, carry):
            octet = s * (hb // 8) + i
            r8 = pl.ds(pl.multiple_of(octet * 8, 8), 8)
            at = pl.ds(pl.multiple_of(octet * 1024, 1024), 1024)
            _, qbd = block_diag(qscr[r8, :])
            cross_copy(layer, 0, octet).wait()
            scores = jnp.dot(qbd, kbuf[at, :], preferred_element_type=F32) * 0.125
            if layer + 1 < layers:
                cross_copy(layer + 1, 0, octet).start()
            peak = jnp.max(scores, axis=1, keepdims=True)
            exps = jnp.exp(scores - peak)
            w = (exps / jnp.sum(exps, axis=1, keepdims=True)).astype(BF16)
            cross_copy(layer, 1, octet).wait()
            o16 = lax.dot_general(w, vbuf[at, :], NT, preferred_element_type=F32)
            if layer + 1 < layers:
                cross_copy(layer + 1, 1, octet).start()
            oscr[r8, :] = fold_heads(o16)
            return carry

        lax.fori_loop(0, hb // 8, octet_body, 0)
        return jnp.dot(oscr[half(s), :].astype(BF16), wout[layer, 1], preferred_element_type=F32)

    def mlp_block(layer, s):
        hidden = norm_rows(xres[half(s), :], ln_layers[layer, 2])
        pre = jnp.dot(hidden, fc1[layer], preferred_element_type=F32) + b_fc1[layer:layer + 1, :]
        active = (0.5 * pre * (1.0 + lax.erf(pre * (0.5 ** 0.5)))).astype(BF16)
        return jnp.dot(active, fc2[layer], preferred_element_type=F32)

    def write_new(layer, s):
        t = lax.broadcasted_iota(jnp.int32, (rows_per, ctx), 1)
        for new, cache in ((knew, ko), (vnew, vo)):
            cols = new[layer, half(s), :].T
            for i in range(hb):
                b = s * hb + i
                at = pl.ds(b * rows_per, rows_per)
                old = cache[layer, at, :].astype(F32)
                cache[layer, at, :] = jnp.where(t == pos_smem[b], cols[:, i:i + 1], old).astype(BF16)

    for s in range(HALVES):
        put_part(0, s, picked_ref[half(s), :])
        rs_start(0, s)
    for octet in range(batch // 8):
        cross_copy(0, 0, octet).start()
        cross_copy(0, 1, octet).start()
    for s in range(HALVES):
        rs_finish(0, s)
    for c in small:
        c.wait()
    for s in range(HALVES):
        xres[half(s), :] = ag_finish(0, s) + posrow_ref[half(s), :]
        if s == 0:
            w_copy(0, 0).wait()
            self_copy(0, 0).wait()
            self_copy(0, 1).wait()
            w_copy(1, 0).wait()
        put_part(1, s, self_block(0, s))
        rs_start(1, s)
    w_copy(3, 0).start()
    w_copy(4, 0).start()
    ph = 1
    for layer in range(layers):
        for kind in range(3):
            if kind == 0:
                for s in range(HALVES):
                    write_new(layer, s)
            if layer == 0 and kind == 0:
                w_copy(0, 1).start()
                self_copy(1, 0).start()
                self_copy(1, 1).start()
                for which in range(1, 5):
                    w_copy(which, 1).start()
            if layer == 1 and kind == 0:
                pltpu.make_async_copy(emb_hbm, eo, e_sem).start()
            for s in range(HALVES):
                rs_finish(ph, s)
            for s in range(HALVES):
                xres[half(s), :] = xres[half(s), :] + ag_finish(ph, s) + out_bias[kind, layer:layer + 1, :]
                nxt = layer * 3 + kind + 1
                if nxt == layers * 3:
                    fh_ref[half(s), :] = norm_rows(xres[half(s), :], ln_final)
                    continue
                nl, nk = divmod(nxt, 3)
                if s == 0:
                    if nk == 0:
                        w_copy(0, nl).wait()
                        self_copy(nl, 0).wait()
                        self_copy(nl, 1).wait()
                        w_copy(1, nl).wait()
                    if nk == 1:
                        w_copy(2, nl).wait()
                    if nk == 2:
                        w_copy(3, nl).wait()
                        w_copy(4, nl).wait()
                put_part(ph + 1, s, (self_block, cross_block, mlp_block)[nk](nl, s))
                rs_start(ph + 1, s)
            ph += 1
    pltpu.make_async_copy(emb_hbm, eo, e_sem).wait()


def final_kernel(kv_ref, e_ref, fh_ref, logits_hbm, ko_hbm, vo_hbm, logits, sem, out_sem):
    layers, rows = kv_ref.shape[1:3]
    copies = []
    for layer in range(layers):
        for which, dst in enumerate((ko_hbm, vo_hbm)):
            for part in range(4):
                at = pl.ds(part * (rows // 4), rows // 4)
                c = pltpu.make_async_copy(kv_ref.at[which, layer, at, :], dst.at[layer, at, :], sem.at[layer, which, part])
                c.start()
                copies.append(c)
    fh = fh_ref[...]
    step = 384
    n = e_ref.shape[0] // step

    def out_copy(i):
        at = pl.ds(pl.multiple_of(i * step, step), step)
        return pltpu.make_async_copy(logits.at[:, at], logits_hbm.at[:, at], out_sem)

    def body(i, carry):
        at = pl.ds(pl.multiple_of(i * step, step), step)
        logits[:, at] = lax.dot_general(fh, e_ref[at, :], NT, preferred_element_type=F32)
        out_copy(i).start()
        return carry

    lax.fori_loop(0, n, body, 0)
    pltpu.make_async_copy(logits, logits_hbm, out_sem).wait()
    for c in copies:
        c.wait()


def solution(mesh):
    vm = pl.BlockSpec(memory_space=pltpu.VMEM)
    sm = pl.BlockSpec(memory_space=pltpu.SMEM)
    hbm = pl.BlockSpec(memory_space=pltpu.HBM)

    def local_step(tokens, positions, self_keys, self_vals, cross_keys, cross_vals, embed_table, pos_table, w_qkv, w_cq, in_bias, w_out, out_bias, w_fc1, b_fc1, w_fc2, ln_layers, ln_final):
        batch = tokens.shape[0]
        layers, _, ctx, heads, hd = self_keys.shape
        frames = cross_keys.shape[2]
        vocab, d = embed_table.shape
        ff = w_fc1.shape[2]
        rows = batch * heads * hd
        hb = batch // HALVES

        def flat(cache):
            return cache.transpose(0, 1, 3, 4, 2).reshape(layers, rows, cache.shape[2])

        picked, posrow = pl.pallas_call(
            gather_kernel,
            out_shape=(pltpu.VMEM((batch, d), BF16), pltpu.VMEM((batch, d), F32)),
            in_specs=[sm, sm, vm, vm, hbm, hbm], out_specs=(vm, vm),
            scratch_shapes=[pltpu.VMEM((16 * batch, d), BF16), pltpu.VMEM((16 * batch, d), BF16), pltpu.SemaphoreType.DMA((2,))],
            compiler_params=pltpu.CompilerParams(vmem_limit_bytes=60 * 2 ** 20),
            name='gather_rows',
        )(tokens, positions, tokens.reshape(1, batch), positions.reshape(1, batch), embed_table, pos_table)

        picked, posrow = (pltpu.with_memory_space_constraint(a, pltpu.VMEM) for a in (picked, posrow))
        kvo, eo, fh = pl.pallas_call(
            functools.partial(decoder_kernel, (layers, batch, ctx, frames)),
            out_shape=(pltpu.VMEM((2, layers, rows, ctx), BF16), pltpu.VMEM((vocab, d), BF16), pltpu.VMEM((batch, d), BF16)),
            in_specs=[sm] + [vm] * 2 + [hbm] * 15,
            out_specs=(vm, vm, vm),
            scratch_shapes=[
                pltpu.VMEM(in_bias.shape, F32), pltpu.VMEM((3, layers, d), F32), pltpu.VMEM(b_fc1.shape, F32), pltpu.VMEM(ln_layers.shape, F32), pltpu.VMEM(ln_final.shape, F32),
                pltpu.VMEM((rows, frames), BF16), pltpu.VMEM((rows, frames), BF16),
                pltpu.VMEM((layers, 3 * heads * hd, d), BF16), pltpu.VMEM((layers, heads * hd, d), BF16),
                pltpu.VMEM((layers, 2, heads * hd, d), BF16), pltpu.VMEM((layers, d, ff), BF16), pltpu.VMEM((layers, ff, d), BF16),
                pltpu.VMEM((batch, d), F32),
                pltpu.VMEM((PARITY, HALVES, TP, hb, 128), F32), pltpu.VMEM((HALVES, TP, hb, 128), BF16),
                pltpu.VMEM((PARITY, HALVES, TP - 1, hb, 128), F32), pltpu.VMEM((HALVES, TP - 1, hb, 128), BF16),
                pltpu.VMEM((PARITY, HALVES, TP, hb, 128), BF16),
                pltpu.VMEM((batch, 128), F32), pltpu.VMEM((batch, 128), F32),
                pltpu.VMEM((layers, batch, 128), F32), pltpu.VMEM((layers, batch, 128), F32),
                pltpu.SemaphoreType.DMA((5,)), pltpu.SemaphoreType.DMA((layers, 2)), pltpu.SemaphoreType.DMA((layers, 2, batch // 8)),
                pltpu.SemaphoreType.DMA((5, layers)), pltpu.SemaphoreType.DMA,
                pltpu.SemaphoreType.DMA((3 * layers + 1, HALVES, 2)), pltpu.SemaphoreType.DMA((3 * layers + 1, HALVES, 2)),
            ],
            compiler_params=pltpu.CompilerParams(collective_id=0, has_side_effects=True, vmem_limit_bytes=67 * 2 ** 19),
            name='decoder_layers',
        )(positions, picked, posrow, in_bias, out_bias.transpose(1, 0, 2), b_fc1, ln_layers, ln_final,
          flat(self_keys), flat(self_vals), flat(cross_keys), flat(cross_vals), embed_table,
          w_qkv.transpose(0, 2, 3, 4, 1).reshape(layers, 3 * heads * hd, d), w_cq.transpose(0, 2, 3, 1).reshape(layers, heads * hd, d),
          w_out.reshape(layers, 2, heads * hd, d), w_fc1, w_fc2)

        logits, nk, nv = pl.pallas_call(
            final_kernel,
            out_shape=(jax.ShapeDtypeStruct((batch, vocab), F32), jax.ShapeDtypeStruct((layers, rows, ctx), BF16), jax.ShapeDtypeStruct((layers, rows, ctx), BF16)),
            in_specs=[vm] * 3, out_specs=(hbm, hbm, hbm),
            scratch_shapes=[pltpu.VMEM((batch, vocab), F32), pltpu.SemaphoreType.DMA((layers, 2, 4)), pltpu.SemaphoreType.DMA],
            compiler_params=pltpu.CompilerParams(vmem_limit_bytes=2 * 2 ** 20),
            name='final_logits',
        )(kvo, eo, fh)

        def unflat(cache):
            return cache.reshape(layers, batch, heads, hd, ctx).transpose(0, 1, 4, 2, 3)

        return logits, unflat(nk), unflat(nv)

    batch_spec = P('dp')
    cache_spec = P(None, 'dp', None, 'tp', None)
    in_specs = (batch_spec, batch_spec, cache_spec, cache_spec, cache_spec, cache_spec, P('tp', None), P(None, None), P(None, None, None, 'tp', None), P(None, None, 'tp', None), P(None, None, 'tp', None), P(None, None, 'tp', None, None), P(None, None, None), P(None, None, 'tp'), P(None, 'tp'), P(None, 'tp', None), P(None, None, None, None), P(None, None))
    out_specs = (P('dp', 'tp'), cache_spec, cache_spec)
    return jax.shard_map(local_step, mesh=mesh, in_specs=in_specs, out_specs=out_specs, check_vma=False)
```

```python
import functools
import jax
import jax.numpy as jnp
from jax import lax
from jax.experimental import pallas as pl
from jax.experimental.pallas import tpu as pltpu
from jax.sharding import PartitionSpec as P

MESH = pl.DeviceIdType.MESH
F32 = jnp.float32
BF16 = jnp.bfloat16
NT = (((1,), (1,)), ((), ()))
TN = (((0,), (0,)), ((), ()))
TP = 8
HALVES = 2
PARITY = 2


def gather_kernel(tok_ref, pos_ref, tokv_ref, posv_ref, emb_hbm, pos_hbm, picked_ref, posrow_ref, ebuf, pbuf, sem):
    shard_rows = emb_hbm.shape[0]
    n = tok_ref.shape[0]
    base = lax.axis_index('tp') * shard_rows

    def start(b, carry):
        tid = jnp.clip(tok_ref[b] - base, 0, shard_rows - 1)
        pid = pos_ref[b]
        at = pl.ds(pl.multiple_of(b * 16, 16), 16)
        pltpu.make_async_copy(emb_hbm.at[pl.ds(pl.multiple_of(tid // 16 * 16, 16), 16), :], ebuf.at[at, :], sem.at[0]).start()
        pltpu.make_async_copy(pos_hbm.at[pl.ds(pl.multiple_of(pid // 16 * 16, 16), 16), :], pbuf.at[at, :], sem.at[1]).start()
        return carry

    lax.fori_loop(0, n, start, 0, unroll=4)
    tid = tokv_ref[...] - base
    owned = (tid >= 0) & (tid < shard_rows)
    lane16 = lax.broadcasted_iota(jnp.int32, (1, n), 1) * 16
    tok_row = jnp.where(owned, lane16 + jnp.clip(tid, 0, shard_rows - 1) % 16, -1)
    pos_row = lane16 + posv_ref[...] % 16
    row = lax.broadcasted_iota(jnp.int32, (16 * n, n), 0)
    tok_hot = jnp.where(row == tok_row, 1.0, 0.0).astype(BF16)
    pos_hot = jnp.where(row == pos_row, 1.0, 0.0).astype(BF16)
    pltpu.make_async_copy(ebuf, ebuf, sem.at[0]).wait()
    picked_ref[...] = lax.dot_general(tok_hot, ebuf[...], TN, preferred_element_type=F32).astype(BF16)
    pltpu.make_async_copy(pbuf, pbuf, sem.at[1]).wait()
    posrow_ref[...] = lax.dot_general(pos_hot, pbuf[...], TN, preferred_element_type=F32)


def norm_rows(x, ln):
    mean = jnp.mean(x, axis=-1, keepdims=True)
    centred = x - mean
    var = jnp.mean(centred * centred, axis=-1, keepdims=True)
    return (centred * lax.rsqrt(var + 1e-5) * ln[0:1, :] + ln[1:2, :]).astype(BF16)


def block_diag(q8):
    lane = lax.broadcasted_iota(jnp.int32, (8, 128), 1)
    qf = q8.astype(F32)
    both = jnp.concatenate([jnp.where(lane < 64, qf, 0.0), jnp.where(lane < 64, 0.0, qf)], axis=0)
    row = lax.rem(lax.broadcasted_iota(jnp.int32, (16, 128), 0), 8)
    blocks = [jnp.where(row == b, both, 0.0).astype(BF16) for b in range(8)]
    return both, jnp.concatenate(blocks, axis=1)


def fold_heads(o16):
    lane = lax.broadcasted_iota(jnp.int32, (8, 128), 1)
    row = lax.broadcasted_iota(jnp.int32, (8, 128), 0)
    out = jnp.zeros((8, 128), F32)
    for b in range(8):
        blk = jnp.where(lane < 64, o16[0:8, b * 128:(b + 1) * 128], o16[8:16, b * 128:(b + 1) * 128])
        out = jnp.where(row == b, blk, out)
    return out


def decoder_kernel(dims, pos_smem, picked_ref, posrow_ref, in_bias_hbm, out_bias_hbm, b_fc1_hbm, ln_layers_hbm, ln_final_hbm,
                   sk_hbm, sv_hbm, ck_hbm, cv_hbm, emb_hbm, wqkv_hbm, wcq_hbm, wout_hbm, fc1_hbm, fc2_hbm,
                   kvo, eo, fh_ref,
                   in_bias, out_bias, b_fc1, ln_layers, ln_final, kbuf, vbuf, wqkv, wcq, wout, fc1, fc2,
                   xres, part, part0, rs_recv, rs_recv0, ag_full, qscr, oscr, knew, vnew,
                   small_sem, self_sem, cross_sem, w_sem, e_sem, send_sem, recv_sem):
    layers, batch, ctx, frames = dims
    me = lax.axis_index('tp')
    ko, vo = kvo.at[0], kvo.at[1]
    hb = batch // HALVES
    rows_per = 128

    def self_copy(layer, which):
        src, dst = ((sk_hbm, ko), (sv_hbm, vo))[which]
        return pltpu.make_async_copy(src.at[layer], dst.at[layer], self_sem.at[layer, which])

    def cross_copy(layer, which, octet):
        src, dst = ((ck_hbm, kbuf), (cv_hbm, vbuf))[which]
        at = pl.ds(pl.multiple_of(octet * 1024, 1024), 1024)
        return pltpu.make_async_copy(src.at[layer, at, :], dst.at[at, :], cross_sem.at[layer, which, octet])

    weights = ((wqkv_hbm, wqkv), (wout_hbm, wout), (wcq_hbm, wcq), (fc1_hbm, fc1), (fc2_hbm, fc2))

    def w_copy(which, layer):
        src, dst = weights[which]
        return pltpu.make_async_copy(src.at[layer], dst.at[layer], w_sem.at[which, layer])

    small = [pltpu.make_async_copy(src, dst, small_sem.at[i]) for i, (src, dst) in enumerate((
        (ln_layers_hbm, ln_layers), (in_bias_hbm, in_bias), (out_bias_hbm, out_bias), (b_fc1_hbm, b_fc1), (ln_final_hbm, ln_final)))]
    for c in small:
        c.start()
    e_rows = emb_hbm.shape[0] // 4

    def e_copy(i):
        at = pl.ds(i * e_rows, e_rows)
        return pltpu.make_async_copy(emb_hbm.at[at, :], eo.at[at, :], e_sem.at[i])

    pending = []

    def pump(n):
        for group in pending[:n]:
            for c in group:
                c.start()
        del pending[:n]

    for octet in range(batch // 8):
        for which in range(2):
            pending.append([cross_copy(0, which, octet)])
    pending.append([w_copy(3, 0), w_copy(4, 0)])
    pending.append([w_copy(0, 1), w_copy(1, 1), w_copy(2, 1)])
    pending.append([self_copy(1, 0)])
    pending.append([self_copy(1, 1)])
    for octet in range(batch // 8):
        for which in range(2):
            pending.append([cross_copy(1, which, octet)])
    pending.append([w_copy(3, 1), w_copy(4, 1)])
    for i in range(4):
        pending.append([e_copy(i)])

    w_copy(0, 0).start()
    self_copy(0, 0).start()
    self_copy(0, 1).start()
    w_copy(1, 0).start()
    w_copy(2, 0).start()

    barrier = pltpu.get_barrier_semaphore()
    for k in range(1, TP):
        pl.semaphore_signal(barrier, 1, device_id={'tp': lax.rem(me + k, TP)}, device_id_type=MESH)
    pl.semaphore_wait(barrier, TP - 1)

    def bufs(ph, s):
        if ph == 0:
            return part0.at[s], rs_recv0.at[s], ag_full.at[0, s]
        slot = ph % PARITY
        return part.at[slot, s], rs_recv.at[slot, s], ag_full.at[slot, s]

    def rs_start(ph, s):
        src, dst, _ = bufs(ph, s)
        for k in range(1, TP):
            peer = lax.rem(me + k, TP)
            pltpu.make_async_remote_copy(src.at[peer], dst.at[k - 1], send_sem.at[ph, s, 0], recv_sem.at[ph, s, 0],
                                         device_id={'tp': peer}, device_id_type=MESH).start()

    def wait_for(ref, sem):
        pltpu.make_async_copy(ref, ref, sem).wait()

    def rs_finish(ph, s):
        src, dst, full = bufs(ph, s)
        wait_for(dst, recv_sem.at[ph, s, 0])
        total = src[me].astype(F32)
        for k in range(TP - 1):
            total = total + dst[k].astype(F32)
        full[me] = total.astype(BF16)
        for k in range(1, TP):
            peer = lax.rem(me + k, TP)
            pltpu.make_async_remote_copy(full.at[me], full.at[me], send_sem.at[ph, s, 1], recv_sem.at[ph, s, 1],
                                         device_id={'tp': peer}, device_id_type=MESH).start()
        wait_for(dst, send_sem.at[ph, s, 0])

    def ag_finish(ph, s):
        _, _, full = bufs(ph, s)
        seven = full.at[pl.ds(0, TP - 1)]
        wait_for(seven, recv_sem.at[ph, s, 1])
        wait_for(seven, send_sem.at[ph, s, 1])
        return jnp.concatenate([full[j].astype(F32) for j in range(TP)], axis=1)

    def put_part(ph, s, value):
        dst = bufs(ph, s)[0]
        for j in range(TP):
            dst[j] = value[:, j * 128:(j + 1) * 128]

    def head_bias(layer, which):
        b = in_bias[layer, which]
        return jnp.concatenate([b[0:1, :], b[1:2, :]], axis=1)

    def half(s):
        return pl.ds(s * hb, hb)

    def self_block(layer, s):
        hidden = norm_rows(xres[half(s), :], ln_layers[layer, 0])
        proj = lax.dot_general(hidden, wqkv[layer], NT, preferred_element_type=F32)
        qscr[half(s), :] = (proj[:, 0:128] + head_bias(layer, 0)).astype(BF16).astype(F32)
        knew[layer, half(s), :] = proj[:, 128:256].astype(BF16).astype(F32)
        vnew[layer, half(s), :] = (proj[:, 256:384] + head_bias(layer, 1)).astype(BF16).astype(F32)

        def octet_body(i, carry):
            octet = s * (hb // 8) + i
            r8 = pl.ds(pl.multiple_of(octet * 8, 8), 8)
            at = pl.ds(pl.multiple_of(octet * 1024, 1024), 1024)
            both, qbd = block_diag(qscr[r8, :])
            seq = lax.rem(lax.broadcasted_iota(jnp.int32, (16, 1), 0), 8)
            limit = jnp.zeros((16, 1), jnp.int32)
            for b in range(8):
                limit = jnp.where(seq == b, pos_smem[octet * 8 + b], limit)
            past = jnp.dot(qbd, ko[layer, at, :], preferred_element_type=F32) * 0.125
            t = lax.broadcasted_iota(jnp.int32, (16, ctx), 1)
            past = jnp.where(t < limit, past, -1e30)
            kn = knew[layer, r8, :]
            vn = vnew[layer, r8, :]
            new = jnp.sum(both * jnp.concatenate([kn, kn], axis=0), axis=1, keepdims=True) * 0.125
            peak = jnp.maximum(jnp.max(past, axis=1, keepdims=True), new)
            past_e = jnp.exp(past - peak)
            new_e = jnp.exp(new - peak)
            denom = jnp.sum(past_e, axis=1, keepdims=True) + new_e
            past_w = (past_e / denom).astype(BF16)
            new_w = (new_e / denom).astype(BF16).astype(F32)
            o16 = lax.dot_general(past_w, vo[layer, at, :], NT, preferred_element_type=F32)
            lane = lax.broadcasted_iota(jnp.int32, (8, 128), 1)
            oscr[r8, :] = fold_heads(o16) + jnp.where(lane < 64, new_w[0:8], new_w[8:16]) * vn
            return carry

        lax.fori_loop(0, hb // 8, octet_body, 0)
        return jnp.dot(oscr[half(s), :].astype(BF16), wout[layer, 0], preferred_element_type=F32)

    def cross_block(layer, s):
        hidden = norm_rows(xres[half(s), :], ln_layers[layer, 1])
        proj = lax.dot_general(hidden, wcq[layer], NT, preferred_element_type=F32)
        qscr[half(s), :] = (proj + head_bias(layer, 2)).astype(BF16).astype(F32)

        def octet_body(i, carry):
            octet = s * (hb // 8) + i
            r8 = pl.ds(pl.multiple_of(octet * 8, 8), 8)
            at = pl.ds(pl.multiple_of(octet * 1024, 1024), 1024)
            _, qbd = block_diag(qscr[r8, :])
            cross_copy(layer, 0, octet).wait()
            scores = jnp.dot(qbd, kbuf[at, :], preferred_element_type=F32) * 0.125
            peak = jnp.max(scores, axis=1, keepdims=True)
            exps = jnp.exp(scores - peak)
            w = (exps / jnp.sum(exps, axis=1, keepdims=True)).astype(BF16)
            cross_copy(layer, 1, octet).wait()
            o16 = lax.dot_general(w, vbuf[at, :], NT, preferred_element_type=F32)
            oscr[r8, :] = fold_heads(o16)
            return carry

        lax.fori_loop(0, hb // 8, octet_body, 0)
        return jnp.dot(oscr[half(s), :].astype(BF16), wout[layer, 1], preferred_element_type=F32)

    def mlp_block(layer, s):
        hidden = norm_rows(xres[half(s), :], ln_layers[layer, 2])
        pre = jnp.dot(hidden, fc1[layer], preferred_element_type=F32) + b_fc1[layer:layer + 1, :]
        active = (0.5 * pre * (1.0 + lax.erf(pre * (0.5 ** 0.5)))).astype(BF16)
        return jnp.dot(active, fc2[layer], preferred_element_type=F32)

    def write_new(layer, s):
        t = lax.broadcasted_iota(jnp.int32, (rows_per, ctx), 1)
        for new, cache in ((knew, ko), (vnew, vo)):
            cols = new[layer, half(s), :].T
            for i in range(hb):
                b = s * hb + i
                at = pl.ds(b * rows_per, rows_per)
                old = cache[layer, at, :].astype(F32)
                cache[layer, at, :] = jnp.where(t == pos_smem[b], cols[:, i:i + 1], old).astype(BF16)

    for s in range(HALVES):
        put_part(0, s, picked_ref[half(s), :])
        rs_start(0, s)
    pump(2)
    for s in range(HALVES):
        rs_finish(0, s)
    pump(2)
    for c in small:
        c.wait()
    for s in range(HALVES):
        xres[half(s), :] = ag_finish(0, s) + posrow_ref[half(s), :]
        if s == 0:
            w_copy(0, 0).wait()
            self_copy(0, 0).wait()
            self_copy(0, 1).wait()
            w_copy(1, 0).wait()
        put_part(1, s, self_block(0, s))
        rs_start(1, s)
    ph = 1
    for layer in range(layers):
        for kind in range(3):
            pump(2)
            if kind == 0:
                for s in range(HALVES):
                    write_new(layer, s)
            for s in range(HALVES):
                rs_finish(ph, s)
            pump(2)
            for s in range(HALVES):
                xres[half(s), :] = xres[half(s), :] + ag_finish(ph, s) + out_bias[kind, layer:layer + 1, :]
                nxt = layer * 3 + kind + 1
                if nxt == layers * 3:
                    fh_ref[half(s), :] = norm_rows(xres[half(s), :], ln_final)
                    continue
                nl, nk = divmod(nxt, 3)
                if s == 0:
                    if nk == 0:
                        w_copy(0, nl).wait()
                        self_copy(nl, 0).wait()
                        self_copy(nl, 1).wait()
                        w_copy(1, nl).wait()
                    if nk == 1:
                        w_copy(2, nl).wait()
                    if nk == 2:
                        w_copy(3, nl).wait()
                        w_copy(4, nl).wait()
                put_part(ph + 1, s, (self_block, cross_block, mlp_block)[nk](nl, s))
                rs_start(ph + 1, s)
            ph += 1
    for i in range(4):
        e_copy(i).wait()


def final_kernel(kv_ref, e_ref, fh_ref, logits_hbm, ko_hbm, vo_hbm, logits, sem, out_sem):
    layers, rows = kv_ref.shape[1:3]
    copies = []
    for layer in range(layers):
        for which, dst in enumerate((ko_hbm, vo_hbm)):
            for part in range(4):
                at = pl.ds(part * (rows // 4), rows // 4)
                c = pltpu.make_async_copy(kv_ref.at[which, layer, at, :], dst.at[layer, at, :], sem.at[layer, which, part])
                c.start()
                copies.append(c)
    fh = fh_ref[...]
    step = 384
    n = e_ref.shape[0] // step

    def out_copy(i):
        at = pl.ds(pl.multiple_of(i * step, step), step)
        return pltpu.make_async_copy(logits.at[:, at], logits_hbm.at[:, at], out_sem)

    def body(i, carry):
        at = pl.ds(pl.multiple_of(i * step, step), step)
        logits[:, at] = lax.dot_general(fh, e_ref[at, :], NT, preferred_element_type=F32)
        out_copy(i).start()
        return carry

    lax.fori_loop(0, n, body, 0)
    pltpu.make_async_copy(logits, logits_hbm, out_sem).wait()
    for c in copies:
        c.wait()


def solution(mesh):
    vm = pl.BlockSpec(memory_space=pltpu.VMEM)
    sm = pl.BlockSpec(memory_space=pltpu.SMEM)
    hbm = pl.BlockSpec(memory_space=pltpu.HBM)

    def local_step(tokens, positions, self_keys, self_vals, cross_keys, cross_vals, embed_table, pos_table, w_qkv, w_cq, in_bias, w_out, out_bias, w_fc1, b_fc1, w_fc2, ln_layers, ln_final):
        batch = tokens.shape[0]
        layers, _, ctx, heads, hd = self_keys.shape
        frames = cross_keys.shape[2]
        vocab, d = embed_table.shape
        ff = w_fc1.shape[2]
        rows = batch * heads * hd
        hb = batch // HALVES

        def flat(cache):
            return cache.transpose(0, 1, 3, 4, 2).reshape(layers, rows, cache.shape[2])

        picked, posrow = pl.pallas_call(
            gather_kernel,
            out_shape=(pltpu.VMEM((batch, d), BF16), pltpu.VMEM((batch, d), F32)),
            in_specs=[sm, sm, vm, vm, hbm, hbm], out_specs=(vm, vm),
            scratch_shapes=[pltpu.VMEM((16 * batch, d), BF16), pltpu.VMEM((16 * batch, d), BF16), pltpu.SemaphoreType.DMA((2,))],
            compiler_params=pltpu.CompilerParams(vmem_limit_bytes=60 * 2 ** 20),
            name='gather_rows',
        )(tokens, positions, tokens.reshape(1, batch), positions.reshape(1, batch), embed_table, pos_table)

        picked, posrow = (pltpu.with_memory_space_constraint(a, pltpu.VMEM) for a in (picked, posrow))
        kvo, eo, fh = pl.pallas_call(
            functools.partial(decoder_kernel, (layers, batch, ctx, frames)),
            out_shape=(pltpu.VMEM((2, layers, rows, ctx), BF16), pltpu.VMEM((vocab, d), BF16), pltpu.VMEM((batch, d), BF16)),
            in_specs=[sm] + [vm] * 2 + [hbm] * 15,
            out_specs=(vm, vm, vm),
            scratch_shapes=[
                pltpu.VMEM(in_bias.shape, F32), pltpu.VMEM((3, layers, d), F32), pltpu.VMEM(b_fc1.shape, F32), pltpu.VMEM(ln_layers.shape, F32), pltpu.VMEM(ln_final.shape, F32),
                pltpu.VMEM((rows, frames), BF16), pltpu.VMEM((rows, frames), BF16),
                pltpu.VMEM((layers, 3 * heads * hd, d), BF16), pltpu.VMEM((layers, heads * hd, d), BF16),
                pltpu.VMEM((layers, 2, heads * hd, d), BF16), pltpu.VMEM((layers, d, ff), BF16), pltpu.VMEM((layers, ff, d), BF16),
                pltpu.VMEM((batch, d), F32),
                pltpu.VMEM((PARITY, HALVES, TP, hb, 128), F32), pltpu.VMEM((HALVES, TP, hb, 128), BF16),
                pltpu.VMEM((PARITY, HALVES, TP - 1, hb, 128), F32), pltpu.VMEM((HALVES, TP - 1, hb, 128), BF16),
                pltpu.VMEM((PARITY, HALVES, TP, hb, 128), BF16),
                pltpu.VMEM((batch, 128), F32), pltpu.VMEM((batch, 128), F32),
                pltpu.VMEM((layers, batch, 128), F32), pltpu.VMEM((layers, batch, 128), F32),
                pltpu.SemaphoreType.DMA((5,)), pltpu.SemaphoreType.DMA((layers, 2)), pltpu.SemaphoreType.DMA((layers, 2, batch // 8)),
                pltpu.SemaphoreType.DMA((5, layers)), pltpu.SemaphoreType.DMA((4,)),
                pltpu.SemaphoreType.DMA((3 * layers + 1, HALVES, 2)), pltpu.SemaphoreType.DMA((3 * layers + 1, HALVES, 2)),
            ],
            compiler_params=pltpu.CompilerParams(collective_id=0, has_side_effects=True, vmem_limit_bytes=67 * 2 ** 19),
            name='decoder_layers',
        )(positions, picked, posrow, in_bias, out_bias.transpose(1, 0, 2), b_fc1, ln_layers, ln_final,
          flat(self_keys), flat(self_vals), flat(cross_keys), flat(cross_vals), embed_table,
          w_qkv.transpose(0, 2, 3, 4, 1).reshape(layers, 3 * heads * hd, d), w_cq.transpose(0, 2, 3, 1).reshape(layers, heads * hd, d),
          w_out.reshape(layers, 2, heads * hd, d), w_fc1, w_fc2)

        logits, nk, nv = pl.pallas_call(
            final_kernel,
            out_shape=(jax.ShapeDtypeStruct((batch, vocab), F32), jax.ShapeDtypeStruct((layers, rows, ctx), BF16), jax.ShapeDtypeStruct((layers, rows, ctx), BF16)),
            in_specs=[vm] * 3, out_specs=(hbm, hbm, hbm),
            scratch_shapes=[pltpu.VMEM((batch, vocab), F32), pltpu.SemaphoreType.DMA((layers, 2, 4)), pltpu.SemaphoreType.DMA],
            compiler_params=pltpu.CompilerParams(vmem_limit_bytes=2 * 2 ** 20),
            name='final_logits',
        )(kvo, eo, fh)

        def unflat(cache):
            return cache.reshape(layers, batch, heads, hd, ctx).transpose(0, 1, 4, 2, 3)

        return logits, unflat(nk), unflat(nv)

    batch_spec = P('dp')
    cache_spec = P(None, 'dp', None, 'tp', None)
    in_specs = (batch_spec, batch_spec, cache_spec, cache_spec, cache_spec, cache_spec, P('tp', None), P(None, None), P(None, None, None, 'tp', None), P(None, None, 'tp', None), P(None, None, 'tp', None), P(None, None, 'tp', None, None), P(None, None, None), P(None, None, 'tp'), P(None, 'tp'), P(None, 'tp', None), P(None, None, None, None), P(None, None))
    out_specs = (P('dp', 'tp'), cache_spec, cache_spec)
    return jax.shard_map(local_step, mesh=mesh, in_specs=in_specs, out_specs=out_specs, check_vma=False)
```

```python
import functools
import jax
import jax.numpy as jnp
from jax import lax
from jax.experimental import pallas as pl
from jax.experimental.pallas import tpu as pltpu
from jax.sharding import PartitionSpec as P

MESH = pl.DeviceIdType.MESH
F32 = jnp.float32
BF16 = jnp.bfloat16
NT = (((1,), (1,)), ((), ()))
TN = (((0,), (0,)), ((), ()))
TP = 8
HALVES = 1
PARITY = 2


def gather_kernel(tok_ref, pos_ref, tokv_ref, posv_ref, emb_hbm, pos_hbm, picked_ref, posrow_ref, ebuf, pbuf, sem):
    shard_rows = emb_hbm.shape[0]
    n = tok_ref.shape[0]
    base = lax.axis_index('tp') * shard_rows

    def start(b, carry):
        tid = jnp.clip(tok_ref[b] - base, 0, shard_rows - 1)
        pid = pos_ref[b]
        at = pl.ds(pl.multiple_of(b * 16, 16), 16)
        pltpu.make_async_copy(emb_hbm.at[pl.ds(pl.multiple_of(tid // 16 * 16, 16), 16), :], ebuf.at[at, :], sem.at[0]).start()
        pltpu.make_async_copy(pos_hbm.at[pl.ds(pl.multiple_of(pid // 16 * 16, 16), 16), :], pbuf.at[at, :], sem.at[1]).start()
        return carry

    lax.fori_loop(0, n, start, 0, unroll=4)
    tid = tokv_ref[...] - base
    owned = (tid >= 0) & (tid < shard_rows)
    lane16 = lax.broadcasted_iota(jnp.int32, (1, n), 1) * 16
    tok_row = jnp.where(owned, lane16 + jnp.clip(tid, 0, shard_rows - 1) % 16, -1)
    pos_row = lane16 + posv_ref[...] % 16
    row = lax.broadcasted_iota(jnp.int32, (16 * n, n), 0)
    tok_hot = jnp.where(row == tok_row, 1.0, 0.0).astype(BF16)
    pos_hot = jnp.where(row == pos_row, 1.0, 0.0).astype(BF16)
    pltpu.make_async_copy(ebuf, ebuf, sem.at[0]).wait()
    picked_ref[...] = lax.dot_general(tok_hot, ebuf[...], TN, preferred_element_type=F32).astype(BF16)
    pltpu.make_async_copy(pbuf, pbuf, sem.at[1]).wait()
    posrow_ref[...] = lax.dot_general(pos_hot, pbuf[...], TN, preferred_element_type=F32)


def norm_rows(x, ln):
    mean = jnp.mean(x, axis=-1, keepdims=True)
    centred = x - mean
    var = jnp.mean(centred * centred, axis=-1, keepdims=True)
    return (centred * lax.rsqrt(var + 1e-5) * ln[0:1, :] + ln[1:2, :]).astype(BF16)


def block_diag(q8):
    lane = lax.broadcasted_iota(jnp.int32, (8, 128), 1)
    qf = q8.astype(F32)
    both = jnp.concatenate([jnp.where(lane < 64, qf, 0.0), jnp.where(lane < 64, 0.0, qf)], axis=0)
    row = lax.rem(lax.broadcasted_iota(jnp.int32, (16, 128), 0), 8)
    blocks = [jnp.where(row == b, both, 0.0).astype(BF16) for b in range(8)]
    return both, jnp.concatenate(blocks, axis=1)


def fold_heads(o16):
    lane = lax.broadcasted_iota(jnp.int32, (8, 128), 1)
    row = lax.broadcasted_iota(jnp.int32, (8, 128), 0)
    out = jnp.zeros((8, 128), F32)
    for b in range(8):
        blk = jnp.where(lane < 64, o16[0:8, b * 128:(b + 1) * 128], o16[8:16, b * 128:(b + 1) * 128])
        out = jnp.where(row == b, blk, out)
    return out


def decoder_kernel(dims, pos_smem, picked_ref, posrow_ref, in_bias_hbm, out_bias_hbm, b_fc1_hbm, ln_layers_hbm, ln_final_hbm,
                   sk_hbm, sv_hbm, ck_hbm, cv_hbm, emb_hbm, wqkv_hbm, wcq_hbm, wout_hbm, fc1_hbm, fc2_hbm,
                   kvo, eo, fh_ref,
                   in_bias, out_bias, b_fc1, ln_layers, ln_final, kbuf, vbuf, wqkv, wcq, wout, fc1, fc2,
                   xres, part, part0, rs_recv, rs_recv0, ag_full, qscr, oscr, knew, vnew,
                   small_sem, self_sem, cross_sem, w_sem, e_sem, send_sem, recv_sem):
    layers, batch, ctx, frames = dims
    me = lax.axis_index('tp')
    ko, vo = kvo.at[0], kvo.at[1]
    hb = batch // HALVES
    rows_per = 128

    def self_copy(layer, which):
        src, dst = ((sk_hbm, ko), (sv_hbm, vo))[which]
        return pltpu.make_async_copy(src.at[layer], dst.at[layer], self_sem.at[layer, which])

    def cross_copy(layer, which, octet):
        src, dst = ((ck_hbm, kbuf), (cv_hbm, vbuf))[which]
        at = pl.ds(pl.multiple_of(octet * 1024, 1024), 1024)
        return pltpu.make_async_copy(src.at[layer, at, :], dst.at[at, :], cross_sem.at[layer, which, octet])

    weights = ((wqkv_hbm, wqkv), (wout_hbm, wout), (wcq_hbm, wcq), (fc1_hbm, fc1), (fc2_hbm, fc2))

    def w_copy(which, layer):
        src, dst = weights[which]
        return pltpu.make_async_copy(src.at[layer], dst.at[layer], w_sem.at[which, layer])

    small = [pltpu.make_async_copy(src, dst, small_sem.at[i]) for i, (src, dst) in enumerate((
        (ln_layers_hbm, ln_layers), (in_bias_hbm, in_bias), (out_bias_hbm, out_bias), (b_fc1_hbm, b_fc1), (ln_final_hbm, ln_final)))]
    for c in small:
        c.start()
    e_rows = emb_hbm.shape[0] // 4

    def e_copy(i):
        at = pl.ds(i * e_rows, e_rows)
        return pltpu.make_async_copy(emb_hbm.at[at, :], eo.at[at, :], e_sem.at[i])

    pending = []

    def pump(n):
        for group in pending[:n]:
            for c in group:
                c.start()
        del pending[:n]

    for octet in range(batch // 8):
        for which in range(2):
            pending.append([cross_copy(0, which, octet)])
    pending.append([w_copy(3, 0), w_copy(4, 0)])
    pending.append([w_copy(0, 1), w_copy(1, 1), w_copy(2, 1)])
    pending.append([self_copy(1, 0)])
    pending.append([self_copy(1, 1)])
    for octet in range(batch // 8):
        for which in range(2):
            pending.append([cross_copy(1, which, octet)])
    pending.append([w_copy(3, 1), w_copy(4, 1)])
    for i in range(4):
        pending.append([e_copy(i)])

    w_copy(0, 0).start()
    self_copy(0, 0).start()
    self_copy(0, 1).start()
    w_copy(1, 0).start()
    w_copy(2, 0).start()

    barrier = pltpu.get_barrier_semaphore()
    for k in range(1, TP):
        pl.semaphore_signal(barrier, 1, device_id={'tp': lax.rem(me + k, TP)}, device_id_type=MESH)
    pl.semaphore_wait(barrier, TP - 1)

    def bufs(ph, s):
        if ph == 0:
            return part0.at[s], rs_recv0.at[s], ag_full.at[0, s]
        slot = ph % PARITY
        return part.at[slot, s], rs_recv.at[slot, s], ag_full.at[slot, s]

    def rs_start(ph, s):
        src, dst, _ = bufs(ph, s)
        for k in range(1, TP):
            peer = lax.rem(me + k, TP)
            pltpu.make_async_remote_copy(src.at[peer], dst.at[k - 1], send_sem.at[ph, s, 0], recv_sem.at[ph, s, 0],
                                         device_id={'tp': peer}, device_id_type=MESH).start()

    def wait_for(ref, sem):
        pltpu.make_async_copy(ref, ref, sem).wait()

    def rs_finish(ph, s):
        src, dst, full = bufs(ph, s)
        wait_for(dst, recv_sem.at[ph, s, 0])
        total = src[me].astype(F32)
        for k in range(TP - 1):
            total = total + dst[k].astype(F32)
        full[me] = total.astype(BF16)
        for k in range(1, TP):
            peer = lax.rem(me + k, TP)
            pltpu.make_async_remote_copy(full.at[me], full.at[me], send_sem.at[ph, s, 1], recv_sem.at[ph, s, 1],
                                         device_id={'tp': peer}, device_id_type=MESH).start()
        wait_for(dst, send_sem.at[ph, s, 0])

    def ag_finish(ph, s):
        _, _, full = bufs(ph, s)
        seven = full.at[pl.ds(0, TP - 1)]
        wait_for(seven, recv_sem.at[ph, s, 1])
        wait_for(seven, send_sem.at[ph, s, 1])
        return jnp.concatenate([full[j].astype(F32) for j in range(TP)], axis=1)

    def put_part(ph, s, value):
        dst = bufs(ph, s)[0]
        for j in range(TP):
            dst[j] = value[:, j * 128:(j + 1) * 128]

    def head_bias(layer, which):
        b = in_bias[layer, which]
        return jnp.concatenate([b[0:1, :], b[1:2, :]], axis=1)

    def half(s):
        return pl.ds(s * hb, hb)

    def self_block(layer, s):
        hidden = norm_rows(xres[half(s), :], ln_layers[layer, 0])
        proj = lax.dot_general(hidden, wqkv[layer], NT, preferred_element_type=F32)
        qscr[half(s), :] = (proj[:, 0:128] + head_bias(layer, 0)).astype(BF16).astype(F32)
        knew[layer, half(s), :] = proj[:, 128:256].astype(BF16).astype(F32)
        vnew[layer, half(s), :] = (proj[:, 256:384] + head_bias(layer, 1)).astype(BF16).astype(F32)

        def octet_body(i, carry):
            octet = s * (hb // 8) + i
            r8 = pl.ds(pl.multiple_of(octet * 8, 8), 8)
            at = pl.ds(pl.multiple_of(octet * 1024, 1024), 1024)
            both, qbd = block_diag(qscr[r8, :])
            seq = lax.rem(lax.broadcasted_iota(jnp.int32, (16, 1), 0), 8)
            limit = jnp.zeros((16, 1), jnp.int32)
            for b in range(8):
                limit = jnp.where(seq == b, pos_smem[octet * 8 + b], limit)
            past = jnp.dot(qbd, ko[layer, at, :], preferred_element_type=F32) * 0.125
            t = lax.broadcasted_iota(jnp.int32, (16, ctx), 1)
            past = jnp.where(t < limit, past, -1e30)
            kn = knew[layer, r8, :]
            vn = vnew[layer, r8, :]
            new = jnp.sum(both * jnp.concatenate([kn, kn], axis=0), axis=1, keepdims=True) * 0.125
            peak = jnp.maximum(jnp.max(past, axis=1, keepdims=True), new)
            past_e = jnp.exp(past - peak)
            new_e = jnp.exp(new - peak)
            denom = jnp.sum(past_e, axis=1, keepdims=True) + new_e
            past_w = (past_e / denom).astype(BF16)
            new_w = (new_e / denom).astype(BF16).astype(F32)
            o16 = lax.dot_general(past_w, vo[layer, at, :], NT, preferred_element_type=F32)
            lane = lax.broadcasted_iota(jnp.int32, (8, 128), 1)
            oscr[r8, :] = fold_heads(o16) + jnp.where(lane < 64, new_w[0:8], new_w[8:16]) * vn
            return carry

        lax.fori_loop(0, hb // 8, octet_body, 0)
        return jnp.dot(oscr[half(s), :].astype(BF16), wout[layer, 0], preferred_element_type=F32)

    def cross_block(layer, s):
        hidden = norm_rows(xres[half(s), :], ln_layers[layer, 1])
        proj = lax.dot_general(hidden, wcq[layer], NT, preferred_element_type=F32)
        qscr[half(s), :] = (proj + head_bias(layer, 2)).astype(BF16).astype(F32)

        def octet_body(i, carry):
            octet = s * (hb // 8) + i
            r8 = pl.ds(pl.multiple_of(octet * 8, 8), 8)
            at = pl.ds(pl.multiple_of(octet * 1024, 1024), 1024)
            _, qbd = block_diag(qscr[r8, :])
            cross_copy(layer, 0, octet).wait()
            scores = jnp.dot(qbd, kbuf[at, :], preferred_element_type=F32) * 0.125
            peak = jnp.max(scores, axis=1, keepdims=True)
            exps = jnp.exp(scores - peak)
            w = (exps / jnp.sum(exps, axis=1, keepdims=True)).astype(BF16)
            cross_copy(layer, 1, octet).wait()
            o16 = lax.dot_general(w, vbuf[at, :], NT, preferred_element_type=F32)
            oscr[r8, :] = fold_heads(o16)
            return carry

        lax.fori_loop(0, hb // 8, octet_body, 0)
        return jnp.dot(oscr[half(s), :].astype(BF16), wout[layer, 1], preferred_element_type=F32)

    def mlp_block(layer, s):
        hidden = norm_rows(xres[half(s), :], ln_layers[layer, 2])
        pre = jnp.dot(hidden, fc1[layer], preferred_element_type=F32) + b_fc1[layer:layer + 1, :]
        active = (0.5 * pre * (1.0 + lax.erf(pre * (0.5 ** 0.5)))).astype(BF16)
        return jnp.dot(active, fc2[layer], preferred_element_type=F32)

    def write_new(layer, s):
        t = lax.broadcasted_iota(jnp.int32, (rows_per, ctx), 1)
        for new, cache in ((knew, ko), (vnew, vo)):
            cols = new[layer, half(s), :].T
            for i in range(hb):
                b = s * hb + i
                at = pl.ds(b * rows_per, rows_per)
                old = cache[layer, at, :].astype(F32)
                cache[layer, at, :] = jnp.where(t == pos_smem[b], cols[:, i:i + 1], old).astype(BF16)

    for s in range(HALVES):
        put_part(0, s, picked_ref[half(s), :])
        rs_start(0, s)
    pump(2)
    for s in range(HALVES):
        rs_finish(0, s)
    pump(2)
    for c in small:
        c.wait()
    for s in range(HALVES):
        xres[half(s), :] = ag_finish(0, s) + posrow_ref[half(s), :]
        if s == 0:
            w_copy(0, 0).wait()
            self_copy(0, 0).wait()
            self_copy(0, 1).wait()
            w_copy(1, 0).wait()
        put_part(1, s, self_block(0, s))
        rs_start(1, s)
    ph = 1
    for layer in range(layers):
        for kind in range(3):
            pump(2)
            if kind == 0:
                for s in range(HALVES):
                    write_new(layer, s)
            for s in range(HALVES):
                rs_finish(ph, s)
            pump(2)
            for s in range(HALVES):
                xres[half(s), :] = xres[half(s), :] + ag_finish(ph, s) + out_bias[kind, layer:layer + 1, :]
                nxt = layer * 3 + kind + 1
                if nxt == layers * 3:
                    fh_ref[half(s), :] = norm_rows(xres[half(s), :], ln_final)
                    continue
                nl, nk = divmod(nxt, 3)
                if s == 0:
                    if nk == 0:
                        w_copy(0, nl).wait()
                        self_copy(nl, 0).wait()
                        self_copy(nl, 1).wait()
                        w_copy(1, nl).wait()
                    if nk == 1:
                        w_copy(2, nl).wait()
                    if nk == 2:
                        w_copy(3, nl).wait()
                        w_copy(4, nl).wait()
                put_part(ph + 1, s, (self_block, cross_block, mlp_block)[nk](nl, s))
                rs_start(ph + 1, s)
            ph += 1
    for i in range(4):
        e_copy(i).wait()


def final_kernel(kv_ref, e_ref, fh_ref, logits_hbm, ko_hbm, vo_hbm, logits, sem, out_sem):
    layers, rows = kv_ref.shape[1:3]
    copies = []
    for layer in range(layers):
        for which, dst in enumerate((ko_hbm, vo_hbm)):
            for part in range(4):
                at = pl.ds(part * (rows // 4), rows // 4)
                c = pltpu.make_async_copy(kv_ref.at[which, layer, at, :], dst.at[layer, at, :], sem.at[layer, which, part])
                c.start()
                copies.append(c)
    fh = fh_ref[...]
    step = 384
    n = e_ref.shape[0] // step

    def out_copy(i):
        at = pl.ds(pl.multiple_of(i * step, step), step)
        return pltpu.make_async_copy(logits.at[:, at], logits_hbm.at[:, at], out_sem)

    def body(i, carry):
        at = pl.ds(pl.multiple_of(i * step, step), step)
        logits[:, at] = lax.dot_general(fh, e_ref[at, :], NT, preferred_element_type=F32)
        out_copy(i).start()
        return carry

    lax.fori_loop(0, n, body, 0)
    pltpu.make_async_copy(logits, logits_hbm, out_sem).wait()
    for c in copies:
        c.wait()


def solution(mesh):
    vm = pl.BlockSpec(memory_space=pltpu.VMEM)
    sm = pl.BlockSpec(memory_space=pltpu.SMEM)
    hbm = pl.BlockSpec(memory_space=pltpu.HBM)

    def local_step(tokens, positions, self_keys, self_vals, cross_keys, cross_vals, embed_table, pos_table, w_qkv, w_cq, in_bias, w_out, out_bias, w_fc1, b_fc1, w_fc2, ln_layers, ln_final):
        batch = tokens.shape[0]
        layers, _, ctx, heads, hd = self_keys.shape
        frames = cross_keys.shape[2]
        vocab, d = embed_table.shape
        ff = w_fc1.shape[2]
        rows = batch * heads * hd
        hb = batch // HALVES

        def flat(cache):
            return cache.transpose(0, 1, 3, 4, 2).reshape(layers, rows, cache.shape[2])

        picked, posrow = pl.pallas_call(
            gather_kernel,
            out_shape=(pltpu.VMEM((batch, d), BF16), pltpu.VMEM((batch, d), F32)),
            in_specs=[sm, sm, vm, vm, hbm, hbm], out_specs=(vm, vm),
            scratch_shapes=[pltpu.VMEM((16 * batch, d), BF16), pltpu.VMEM((16 * batch, d), BF16), pltpu.SemaphoreType.DMA((2,))],
            compiler_params=pltpu.CompilerParams(vmem_limit_bytes=60 * 2 ** 20),
            name='gather_rows',
        )(tokens, positions, tokens.reshape(1, batch), positions.reshape(1, batch), embed_table, pos_table)

        picked, posrow = (pltpu.with_memory_space_constraint(a, pltpu.VMEM) for a in (picked, posrow))
        kvo, eo, fh = pl.pallas_call(
            functools.partial(decoder_kernel, (layers, batch, ctx, frames)),
            out_shape=(pltpu.VMEM((2, layers, rows, ctx), BF16), pltpu.VMEM((vocab, d), BF16), pltpu.VMEM((batch, d), BF16)),
            in_specs=[sm] + [vm] * 2 + [hbm] * 15,
            out_specs=(vm, vm, vm),
            scratch_shapes=[
                pltpu.VMEM(in_bias.shape, F32), pltpu.VMEM((3, layers, d), F32), pltpu.VMEM(b_fc1.shape, F32), pltpu.VMEM(ln_layers.shape, F32), pltpu.VMEM(ln_final.shape, F32),
                pltpu.VMEM((rows, frames), BF16), pltpu.VMEM((rows, frames), BF16),
                pltpu.VMEM((layers, 3 * heads * hd, d), BF16), pltpu.VMEM((layers, heads * hd, d), BF16),
                pltpu.VMEM((layers, 2, heads * hd, d), BF16), pltpu.VMEM((layers, d, ff), BF16), pltpu.VMEM((layers, ff, d), BF16),
                pltpu.VMEM((batch, d), F32),
                pltpu.VMEM((PARITY, HALVES, TP, hb, 128), F32), pltpu.VMEM((HALVES, TP, hb, 128), BF16),
                pltpu.VMEM((PARITY, HALVES, TP - 1, hb, 128), F32), pltpu.VMEM((HALVES, TP - 1, hb, 128), BF16),
                pltpu.VMEM((PARITY, HALVES, TP, hb, 128), BF16),
                pltpu.VMEM((batch, 128), F32), pltpu.VMEM((batch, 128), F32),
                pltpu.VMEM((layers, batch, 128), F32), pltpu.VMEM((layers, batch, 128), F32),
                pltpu.SemaphoreType.DMA((5,)), pltpu.SemaphoreType.DMA((layers, 2)), pltpu.SemaphoreType.DMA((layers, 2, batch // 8)),
                pltpu.SemaphoreType.DMA((5, layers)), pltpu.SemaphoreType.DMA((4,)),
                pltpu.SemaphoreType.DMA((3 * layers + 1, HALVES, 2)), pltpu.SemaphoreType.DMA((3 * layers + 1, HALVES, 2)),
            ],
            compiler_params=pltpu.CompilerParams(collective_id=0, has_side_effects=True, vmem_limit_bytes=67 * 2 ** 19),
            name='decoder_layers',
        )(positions, picked, posrow, in_bias, out_bias.transpose(1, 0, 2), b_fc1, ln_layers, ln_final,
          flat(self_keys), flat(self_vals), flat(cross_keys), flat(cross_vals), embed_table,
          w_qkv.transpose(0, 2, 3, 4, 1).reshape(layers, 3 * heads * hd, d), w_cq.transpose(0, 2, 3, 1).reshape(layers, heads * hd, d),
          w_out.reshape(layers, 2, heads * hd, d), w_fc1, w_fc2)

        logits, nk, nv = pl.pallas_call(
            final_kernel,
            out_shape=(jax.ShapeDtypeStruct((batch, vocab), F32), jax.ShapeDtypeStruct((layers, rows, ctx), BF16), jax.ShapeDtypeStruct((layers, rows, ctx), BF16)),
            in_specs=[vm] * 3, out_specs=(hbm, hbm, hbm),
            scratch_shapes=[pltpu.VMEM((batch, vocab), F32), pltpu.SemaphoreType.DMA((layers, 2, 4)), pltpu.SemaphoreType.DMA],
            compiler_params=pltpu.CompilerParams(vmem_limit_bytes=2 * 2 ** 20),
            name='final_logits',
        )(kvo, eo, fh)

        def unflat(cache):
            return cache.reshape(layers, batch, heads, hd, ctx).transpose(0, 1, 4, 2, 3)

        return logits, unflat(nk), unflat(nv)

    batch_spec = P('dp')
    cache_spec = P(None, 'dp', None, 'tp', None)
    in_specs = (batch_spec, batch_spec, cache_spec, cache_spec, cache_spec, cache_spec, P('tp', None), P(None, None), P(None, None, None, 'tp', None), P(None, None, 'tp', None), P(None, None, 'tp', None), P(None, None, 'tp', None, None), P(None, None, None), P(None, None, 'tp'), P(None, 'tp'), P(None, 'tp', None), P(None, None, None, None), P(None, None))
    out_specs = (P('dp', 'tp'), cache_spec, cache_spec)
    return jax.shard_map(local_step, mesh=mesh, in_specs=in_specs, out_specs=out_specs, check_vma=False)
```

```python
import functools
import jax
import jax.numpy as jnp
from jax import lax
from jax.experimental import pallas as pl
from jax.experimental.pallas import tpu as pltpu
from jax.sharding import PartitionSpec as P

MESH = pl.DeviceIdType.MESH
F32 = jnp.float32
BF16 = jnp.bfloat16
NT = (((1,), (1,)), ((), ()))
TN = (((0,), (0,)), ((), ()))
TP = 8
HALVES = 2
PARITY = 2


def gather_kernel(tok_ref, pos_ref, tokv_ref, posv_ref, emb_hbm, pos_hbm, picked_ref, posrow_ref, ebuf, pbuf, sem):
    shard_rows = emb_hbm.shape[0]
    n = tok_ref.shape[0]
    base = lax.axis_index('tp') * shard_rows

    def start(b, carry):
        tid = jnp.clip(tok_ref[b] - base, 0, shard_rows - 1)
        pid = pos_ref[b]
        at = pl.ds(pl.multiple_of(b * 16, 16), 16)
        pltpu.make_async_copy(emb_hbm.at[pl.ds(pl.multiple_of(tid // 16 * 16, 16), 16), :], ebuf.at[at, :], sem.at[0]).start()
        pltpu.make_async_copy(pos_hbm.at[pl.ds(pl.multiple_of(pid // 16 * 16, 16), 16), :], pbuf.at[at, :], sem.at[1]).start()
        return carry

    lax.fori_loop(0, n, start, 0, unroll=4)
    tid = tokv_ref[...] - base
    owned = (tid >= 0) & (tid < shard_rows)
    lane16 = lax.broadcasted_iota(jnp.int32, (1, n), 1) * 16
    tok_row = jnp.where(owned, lane16 + jnp.clip(tid, 0, shard_rows - 1) % 16, -1)
    pos_row = lane16 + posv_ref[...] % 16
    row = lax.broadcasted_iota(jnp.int32, (16 * n, n), 0)
    tok_hot = jnp.where(row == tok_row, 1.0, 0.0).astype(BF16)
    pos_hot = jnp.where(row == pos_row, 1.0, 0.0).astype(BF16)
    pltpu.make_async_copy(ebuf, ebuf, sem.at[0]).wait()
    picked_ref[...] = lax.dot_general(tok_hot, ebuf[...], TN, preferred_element_type=F32).astype(BF16)
    pltpu.make_async_copy(pbuf, pbuf, sem.at[1]).wait()
    posrow_ref[...] = lax.dot_general(pos_hot, pbuf[...], TN, preferred_element_type=F32)


def norm_rows(x, ln):
    mean = jnp.mean(x, axis=-1, keepdims=True)
    centred = x - mean
    var = jnp.mean(centred * centred, axis=-1, keepdims=True)
    return (centred * lax.rsqrt(var + 1e-5) * ln[0:1, :] + ln[1:2, :]).astype(BF16)


def block_diag(q8):
    lane = lax.broadcasted_iota(jnp.int32, (8, 128), 1)
    qf = q8.astype(F32)
    both = jnp.concatenate([jnp.where(lane < 64, qf, 0.0), jnp.where(lane < 64, 0.0, qf)], axis=0)
    row = lax.rem(lax.broadcasted_iota(jnp.int32, (16, 128), 0), 8)
    blocks = [jnp.where(row == b, both, 0.0).astype(BF16) for b in range(8)]
    return both, jnp.concatenate(blocks, axis=1)


def fold_heads(o16):
    lane = lax.broadcasted_iota(jnp.int32, (8, 128), 1)
    row = lax.broadcasted_iota(jnp.int32, (8, 128), 0)
    out = jnp.zeros((8, 128), F32)
    for b in range(8):
        blk = jnp.where(lane < 64, o16[0:8, b * 128:(b + 1) * 128], o16[8:16, b * 128:(b + 1) * 128])
        out = jnp.where(row == b, blk, out)
    return out


def decoder_kernel(dims, pos_smem, picked_ref, posrow_ref, in_bias_hbm, out_bias_hbm, b_fc1_hbm, ln_layers_hbm, ln_final_hbm,
                   sk_hbm, sv_hbm, ck_hbm, cv_hbm, emb_hbm, wqkv_hbm, wcq_hbm, wout_hbm, fc1_hbm, fc2_hbm,
                   kvo, eo, fh_ref,
                   in_bias, out_bias, b_fc1, ln_layers, ln_final, kbuf, vbuf, wqkv, wcq, wout, fc1, fc2,
                   xres, stage, stage0, pair, pair0, chips, chips0, full, qscr, oscr, knew, vnew,
                   small_sem, self_sem, cross_sem, w_sem, e_sem, send_sem, recv_sem):
    layers, batch, ctx, frames = dims
    me = lax.axis_index('tp')
    ko, vo = kvo.at[0], kvo.at[1]
    hb = batch // HALVES
    rows_per = 128

    def self_copy(layer, which):
        src, dst = ((sk_hbm, ko), (sv_hbm, vo))[which]
        return pltpu.make_async_copy(src.at[layer], dst.at[layer], self_sem.at[layer, which])

    def cross_copy(layer, which, octet):
        src, dst = ((ck_hbm, kbuf), (cv_hbm, vbuf))[which]
        at = pl.ds(pl.multiple_of(octet * 1024, 1024), 1024)
        return pltpu.make_async_copy(src.at[layer, at, :], dst.at[at, :], cross_sem.at[layer, which, octet])

    weights = ((wqkv_hbm, wqkv), (wout_hbm, wout), (wcq_hbm, wcq), (fc1_hbm, fc1), (fc2_hbm, fc2))

    def w_copy(which, layer):
        src, dst = weights[which]
        return pltpu.make_async_copy(src.at[layer], dst.at[layer], w_sem.at[which, layer])

    small = [pltpu.make_async_copy(src, dst, small_sem.at[i]) for i, (src, dst) in enumerate((
        (ln_layers_hbm, ln_layers), (in_bias_hbm, in_bias), (out_bias_hbm, out_bias), (b_fc1_hbm, b_fc1), (ln_final_hbm, ln_final)))]
    for c in small:
        c.start()
    e_rows = emb_hbm.shape[0] // 4

    def e_copy(i):
        at = pl.ds(i * e_rows, e_rows)
        return pltpu.make_async_copy(emb_hbm.at[at, :], eo.at[at, :], e_sem.at[i])

    pending = []

    def pump(n):
        for group in pending[:n]:
            for c in group:
                c.start()
        del pending[:n]

    for octet in range(batch // 8):
        for which in range(2):
            pending.append([cross_copy(0, which, octet)])
    pending.append([w_copy(3, 0), w_copy(4, 0)])
    pending.append([w_copy(0, 1), w_copy(1, 1), w_copy(2, 1)])
    pending.append([self_copy(1, 0)])
    pending.append([self_copy(1, 1)])
    for octet in range(batch // 8):
        for which in range(2):
            pending.append([cross_copy(1, which, octet)])
    pending.append([w_copy(3, 1), w_copy(4, 1)])
    for i in range(4):
        pending.append([e_copy(i)])

    w_copy(0, 0).start()
    self_copy(0, 0).start()
    self_copy(0, 1).start()
    w_copy(1, 0).start()
    w_copy(2, 0).start()

    barrier = pltpu.get_barrier_semaphore()
    for k in range(1, TP):
        pl.semaphore_signal(barrier, 1, device_id={'tp': lax.rem(me + k, TP)}, device_id_type=MESH)
    pl.semaphore_wait(barrier, TP - 1)

    core = lax.rem(me, 2)
    chip = me // 2
    partner = {'tp': 2 * chip + 1 - core}
    wide = posrow_ref.shape[1] // 2

    def bufs(ph, s):
        if ph == 0:
            return stage0.at[s], pair0.at[s], chips0.at[s], full.at[0, s]
        slot = ph % PARITY
        return stage.at[slot, s], pair.at[slot, s], chips.at[slot, s], full.at[slot, s]

    def send(src, dst, ph, s, step, device):
        pltpu.make_async_remote_copy(src, dst, send_sem.at[ph, s, step], recv_sem.at[ph, s, step], device_id=device, device_id_type=MESH).start()

    def wait_for(ref, sem):
        pltpu.make_async_copy(ref, ref, sem).wait()

    def sum_start(ph, s, value):
        mine, got, _, _ = bufs(ph, s)
        mine[0] = value[:, :wide]
        mine[1] = value[:, wide:]
        send(mine.at[1 - core], got, ph, s, 0, partner)

    def sum_chips(ph, s):
        mine, got, by_chip, _ = bufs(ph, s)
        wait_for(got, recv_sem.at[ph, s, 0])
        by_chip[chip] = mine[core] + got[...]
        for k in range(1, TP // 2):
            send(by_chip.at[chip], by_chip.at[chip], ph, s, 1, {'tp': 2 * lax.rem(chip + k, TP // 2) + core})
        wait_for(got, send_sem.at[ph, s, 0])

    def sum_share(ph, s):
        _, _, by_chip, both = bufs(ph, s)
        others = by_chip.at[pl.ds(0, TP // 2 - 1)]
        wait_for(others, recv_sem.at[ph, s, 1])
        total = by_chip[0].astype(F32)
        for q in range(1, TP // 2):
            total = total + by_chip[q].astype(F32)
        both[core] = total.astype(BF16)
        send(both.at[core], both.at[core], ph, s, 2, partner)
        wait_for(others, send_sem.at[ph, s, 1])

    def sum_finish(ph, s):
        both = bufs(ph, s)[3]
        wait_for(both.at[0], recv_sem.at[ph, s, 2])
        wait_for(both.at[0], send_sem.at[ph, s, 2])
        return jnp.concatenate([both[0].astype(F32), both[1].astype(F32)], axis=1)

    def head_bias(layer, which):
        b = in_bias[layer, which]
        return jnp.concatenate([b[0:1, :], b[1:2, :]], axis=1)

    def half(s):
        return pl.ds(s * hb, hb)

    def self_block(layer, s, after_proj, middle):
        hidden = norm_rows(xres[half(s), :], ln_layers[layer, 0])
        proj = lax.dot_general(hidden, wqkv[layer], NT, preferred_element_type=F32)
        qscr[half(s), :] = (proj[:, 0:128] + head_bias(layer, 0)).astype(BF16).astype(F32)
        knew[layer, half(s), :] = proj[:, 128:256].astype(BF16).astype(F32)
        vnew[layer, half(s), :] = (proj[:, 256:384] + head_bias(layer, 1)).astype(BF16).astype(F32)

        after_proj()
        for i in range(hb // 8):
            octet = s * (hb // 8) + i
            r8 = pl.ds(octet * 8, 8)
            at = pl.ds(octet * 1024, 1024)
            both, qbd = block_diag(qscr[r8, :])
            seq = lax.rem(lax.broadcasted_iota(jnp.int32, (16, 1), 0), 8)
            limit = jnp.zeros((16, 1), jnp.int32)
            for b in range(8):
                limit = jnp.where(seq == b, pos_smem[octet * 8 + b], limit)
            past = jnp.dot(qbd, ko[layer, at, :], preferred_element_type=F32) * 0.125
            t = lax.broadcasted_iota(jnp.int32, (16, ctx), 1)
            past = jnp.where(t < limit, past, -1e30)
            kn = knew[layer, r8, :]
            vn = vnew[layer, r8, :]
            new = jnp.sum(both * jnp.concatenate([kn, kn], axis=0), axis=1, keepdims=True) * 0.125
            peak = jnp.maximum(jnp.max(past, axis=1, keepdims=True), new)
            past_e = jnp.exp(past - peak)
            new_e = jnp.exp(new - peak)
            denom = jnp.sum(past_e, axis=1, keepdims=True) + new_e
            past_w = (past_e / denom).astype(BF16)
            new_w = (new_e / denom).astype(BF16).astype(F32)
            o16 = lax.dot_general(past_w, vo[layer, at, :], NT, preferred_element_type=F32)
            lane = lax.broadcasted_iota(jnp.int32, (8, 128), 1)
            oscr[r8, :] = fold_heads(o16) + jnp.where(lane < 64, new_w[0:8], new_w[8:16]) * vn
            if i == 0:
                middle()
        return jnp.dot(oscr[half(s), :].astype(BF16), wout[layer, 0], preferred_element_type=F32)

    def cross_block(layer, s, after_proj, middle):
        hidden = norm_rows(xres[half(s), :], ln_layers[layer, 1])
        proj = lax.dot_general(hidden, wcq[layer], NT, preferred_element_type=F32)
        qscr[half(s), :] = (proj + head_bias(layer, 2)).astype(BF16).astype(F32)

        after_proj()
        for i in range(hb // 8):
            octet = s * (hb // 8) + i
            r8 = pl.ds(octet * 8, 8)
            at = pl.ds(octet * 1024, 1024)
            _, qbd = block_diag(qscr[r8, :])
            cross_copy(layer, 0, octet).wait()
            scores = jnp.dot(qbd, kbuf[at, :], preferred_element_type=F32) * 0.125
            peak = jnp.max(scores, axis=1, keepdims=True)
            exps = jnp.exp(scores - peak)
            w = (exps / jnp.sum(exps, axis=1, keepdims=True)).astype(BF16)
            if i == 0:
                middle()
            cross_copy(layer, 1, octet).wait()
            o16 = lax.dot_general(w, vbuf[at, :], NT, preferred_element_type=F32)
            oscr[r8, :] = fold_heads(o16)
        return jnp.dot(oscr[half(s), :].astype(BF16), wout[layer, 1], preferred_element_type=F32)

    def mlp_block(layer, s, after_proj, middle):
        hidden = norm_rows(xres[half(s), :], ln_layers[layer, 2])
        pre = jnp.dot(hidden, fc1[layer], preferred_element_type=F32) + b_fc1[layer:layer + 1, :]
        active = (0.5 * pre * (1.0 + lax.erf(pre * (0.5 ** 0.5)))).astype(BF16)
        out = jnp.dot(active, fc2[layer], preferred_element_type=F32)
        middle()
        return out

    def write_new(layer, s):
        t = lax.broadcasted_iota(jnp.int32, (rows_per, ctx), 1)
        for new, cache in ((knew, ko), (vnew, vo)):
            cols = new[layer, half(s), :].T
            for i in range(hb):
                b = s * hb + i
                at = pl.ds(b * rows_per, rows_per)
                old = cache[layer, at, :].astype(F32)
                cache[layer, at, :] = jnp.where(t == pos_smem[b], cols[:, i:i + 1], old).astype(BF16)

    def nothing():
        pass

    def ready(nl, nk):
        if nk == 0:
            w_copy(0, nl).wait()
            self_copy(nl, 0).wait()
            self_copy(nl, 1).wait()
            w_copy(1, nl).wait()
        if nk == 1:
            w_copy(2, nl).wait()
        if nk == 2:
            w_copy(3, nl).wait()
            w_copy(4, nl).wait()

    for s in range(2):
        sum_start(0, s, picked_ref[half(s), :])
    for s in range(2):
        sum_chips(0, s)
    pump(2)
    for c in small:
        c.wait()
    sum_share(0, 0)
    for ph in range(3 * layers + 1):
        layer, kind = divmod(ph, 3)
        before, prev_kind = divmod(ph - 1, 3)

        def update(s):
            total = sum_finish(ph, s)
            if ph == 0:
                xres[half(s), :] = total + posrow_ref[half(s), :]
            else:
                xres[half(s), :] = xres[half(s), :] + total + out_bias[prev_kind, before:before + 1, :]

        if ph == 3 * layers:
            sum_share(ph, 1)
            for s in range(2):
                update(s)
                fh_ref[half(s), :] = norm_rows(xres[half(s), :], ln_final)
            break
        block = (self_block, cross_block, mlp_block)[kind]
        update(0)
        ready(layer, kind)
        share = functools.partial(sum_share, ph, 1)
        sum_start(ph + 1, 0, block(layer, 0, share if kind < 2 else nothing, nothing))
        if kind == 2:
            share()
        pump(2)
        update(1)
        sum_start(ph + 1, 1, block(layer, 1, nothing, functools.partial(sum_chips, ph + 1, 0)))
        if kind == 0:
            write_new(layer, 0)
        sum_chips(ph + 1, 1)
        pump(2)
        if kind == 0:
            write_new(layer, 1)
        sum_share(ph + 1, 0)
    for i in range(4):
        e_copy(i).wait()


def final_kernel(kv_ref, e_ref, fh_ref, logits_hbm, ko_hbm, vo_hbm, logits, sem, out_sem):
    layers, rows = kv_ref.shape[1:3]
    copies = []
    for layer in range(layers):
        for which, dst in enumerate((ko_hbm, vo_hbm)):
            for part in range(4):
                at = pl.ds(part * (rows // 4), rows // 4)
                c = pltpu.make_async_copy(kv_ref.at[which, layer, at, :], dst.at[layer, at, :], sem.at[layer, which, part])
                c.start()
                copies.append(c)
    fh = fh_ref[...]
    step = 384
    n = e_ref.shape[0] // step

    def out_copy(i):
        at = pl.ds(pl.multiple_of(i * step, step), step)
        return pltpu.make_async_copy(logits.at[:, at], logits_hbm.at[:, at], out_sem)

    def body(i, carry):
        at = pl.ds(pl.multiple_of(i * step, step), step)
        logits[:, at] = lax.dot_general(fh, e_ref[at, :], NT, preferred_element_type=F32)
        out_copy(i).start()
        return carry

    lax.fori_loop(0, n, body, 0)
    pltpu.make_async_copy(logits, logits_hbm, out_sem).wait()
    for c in copies:
        c.wait()


def solution(mesh):
    vm = pl.BlockSpec(memory_space=pltpu.VMEM)
    sm = pl.BlockSpec(memory_space=pltpu.SMEM)
    hbm = pl.BlockSpec(memory_space=pltpu.HBM)

    def local_step(tokens, positions, self_keys, self_vals, cross_keys, cross_vals, embed_table, pos_table, w_qkv, w_cq, in_bias, w_out, out_bias, w_fc1, b_fc1, w_fc2, ln_layers, ln_final):
        batch = tokens.shape[0]
        layers, _, ctx, heads, hd = self_keys.shape
        frames = cross_keys.shape[2]
        vocab, d = embed_table.shape
        ff = w_fc1.shape[2]
        rows = batch * heads * hd
        hb = batch // HALVES

        def flat(cache):
            return cache.transpose(0, 1, 3, 4, 2).reshape(layers, rows, cache.shape[2])

        picked, posrow = pl.pallas_call(
            gather_kernel,
            out_shape=(pltpu.VMEM((batch, d), BF16), pltpu.VMEM((batch, d), F32)),
            in_specs=[sm, sm, vm, vm, hbm, hbm], out_specs=(vm, vm),
            scratch_shapes=[pltpu.VMEM((16 * batch, d), BF16), pltpu.VMEM((16 * batch, d), BF16), pltpu.SemaphoreType.DMA((2,))],
            compiler_params=pltpu.CompilerParams(vmem_limit_bytes=60 * 2 ** 20),
            name='gather_rows',
        )(tokens, positions, tokens.reshape(1, batch), positions.reshape(1, batch), embed_table, pos_table)

        picked, posrow = (pltpu.with_memory_space_constraint(a, pltpu.VMEM) for a in (picked, posrow))
        kvo, eo, fh = pl.pallas_call(
            functools.partial(decoder_kernel, (layers, batch, ctx, frames)),
            out_shape=(pltpu.VMEM((2, layers, rows, ctx), BF16), pltpu.VMEM((vocab, d), BF16), pltpu.VMEM((batch, d), BF16)),
            in_specs=[sm] + [vm] * 2 + [hbm] * 15,
            out_specs=(vm, vm, vm),
            scratch_shapes=[
                pltpu.VMEM(in_bias.shape, F32), pltpu.VMEM((3, layers, d), F32), pltpu.VMEM(b_fc1.shape, F32), pltpu.VMEM(ln_layers.shape, F32), pltpu.VMEM(ln_final.shape, F32),
                pltpu.VMEM((rows, frames), BF16), pltpu.VMEM((rows, frames), BF16),
                pltpu.VMEM((layers, 3 * heads * hd, d), BF16), pltpu.VMEM((layers, heads * hd, d), BF16),
                pltpu.VMEM((layers, 2, heads * hd, d), BF16), pltpu.VMEM((layers, d, ff), BF16), pltpu.VMEM((layers, ff, d), BF16),
                pltpu.VMEM((batch, d), F32),
                pltpu.VMEM((PARITY, HALVES, 2, hb, d // 2), F32), pltpu.VMEM((HALVES, 2, hb, d // 2), BF16),
                pltpu.VMEM((PARITY, HALVES, hb, d // 2), F32), pltpu.VMEM((HALVES, hb, d // 2), BF16),
                pltpu.VMEM((PARITY, HALVES, TP // 2, hb, d // 2), F32), pltpu.VMEM((HALVES, TP // 2, hb, d // 2), BF16),
                pltpu.VMEM((PARITY, HALVES, 2, hb, d // 2), BF16),
                pltpu.VMEM((batch, 128), F32), pltpu.VMEM((batch, 128), F32),
                pltpu.VMEM((layers, batch, 128), F32), pltpu.VMEM((layers, batch, 128), F32),
                pltpu.SemaphoreType.DMA((5,)), pltpu.SemaphoreType.DMA((layers, 2)), pltpu.SemaphoreType.DMA((layers, 2, batch // 8)),
                pltpu.SemaphoreType.DMA((5, layers)), pltpu.SemaphoreType.DMA((4,)),
                pltpu.SemaphoreType.DMA((3 * layers + 1, HALVES, 3)), pltpu.SemaphoreType.DMA((3 * layers + 1, HALVES, 3)),
            ],
            compiler_params=pltpu.CompilerParams(collective_id=0, has_side_effects=True, vmem_limit_bytes=139 * 2 ** 18),
            name='decoder_layers',
        )(positions, picked, posrow, in_bias, out_bias.transpose(1, 0, 2), b_fc1, ln_layers, ln_final,
          flat(self_keys), flat(self_vals), flat(cross_keys), flat(cross_vals), embed_table,
          w_qkv.transpose(0, 2, 3, 4, 1).reshape(layers, 3 * heads * hd, d), w_cq.transpose(0, 2, 3, 1).reshape(layers, heads * hd, d),
          w_out.reshape(layers, 2, heads * hd, d), w_fc1, w_fc2)

        logits, nk, nv = pl.pallas_call(
            final_kernel,
            out_shape=(jax.ShapeDtypeStruct((batch, vocab), F32), jax.ShapeDtypeStruct((layers, rows, ctx), BF16), jax.ShapeDtypeStruct((layers, rows, ctx), BF16)),
            in_specs=[vm] * 3, out_specs=(hbm, hbm, hbm),
            scratch_shapes=[pltpu.VMEM((batch, vocab), F32), pltpu.SemaphoreType.DMA((layers, 2, 4)), pltpu.SemaphoreType.DMA],
            compiler_params=pltpu.CompilerParams(vmem_limit_bytes=2 * 2 ** 20),
            name='final_logits',
        )(kvo, eo, fh)

        def unflat(cache):
            return cache.reshape(layers, batch, heads, hd, ctx).transpose(0, 1, 4, 2, 3)

        return logits, unflat(nk), unflat(nv)

    batch_spec = P('dp')
    cache_spec = P(None, 'dp', None, 'tp', None)
    in_specs = (batch_spec, batch_spec, cache_spec, cache_spec, cache_spec, cache_spec, P('tp', None), P(None, None), P(None, None, None, 'tp', None), P(None, None, 'tp', None), P(None, None, 'tp', None), P(None, None, 'tp', None, None), P(None, None, None), P(None, None, 'tp'), P(None, 'tp'), P(None, 'tp', None), P(None, None, None, None), P(None, None))
    out_specs = (P('dp', 'tp'), cache_spec, cache_spec)
    return jax.shard_map(local_step, mesh=mesh, in_specs=in_specs, out_specs=out_specs, check_vma=False)
```

```python
import functools
import jax
import jax.numpy as jnp
from jax import lax
from jax.experimental import pallas as pl
from jax.experimental.pallas import tpu as pltpu
from jax.sharding import PartitionSpec as P

MESH = pl.DeviceIdType.MESH
F32 = jnp.float32
BF16 = jnp.bfloat16
NT = (((1,), (1,)), ((), ()))
TN = (((0,), (0,)), ((), ()))
TP = 8
HALVES = 2
PARITY = 2


def gather_kernel(tok_ref, pos_ref, tokv_ref, posv_ref, emb_hbm, pos_hbm, picked_ref, posrow_ref, ebuf, pbuf, sem):
    shard_rows = emb_hbm.shape[0]
    n = tok_ref.shape[0]
    base = lax.axis_index('tp') * shard_rows

    def start(b, carry):
        tid = jnp.clip(tok_ref[b] - base, 0, shard_rows - 1)
        pid = pos_ref[b]
        at = pl.ds(pl.multiple_of(b * 16, 16), 16)
        pltpu.make_async_copy(emb_hbm.at[pl.ds(pl.multiple_of(tid // 16 * 16, 16), 16), :], ebuf.at[at, :], sem.at[0]).start()
        pltpu.make_async_copy(pos_hbm.at[pl.ds(pl.multiple_of(pid // 16 * 16, 16), 16), :], pbuf.at[at, :], sem.at[1]).start()
        return carry

    lax.fori_loop(0, n, start, 0, unroll=4)
    tid = tokv_ref[...] - base
    owned = (tid >= 0) & (tid < shard_rows)
    lane16 = lax.broadcasted_iota(jnp.int32, (1, n), 1) * 16
    tok_row = jnp.where(owned, lane16 + jnp.clip(tid, 0, shard_rows - 1) % 16, -1)
    pos_row = lane16 + posv_ref[...] % 16
    row = lax.broadcasted_iota(jnp.int32, (16 * n, n), 0)
    tok_hot = jnp.where(row == tok_row, 1.0, 0.0).astype(BF16)
    pos_hot = jnp.where(row == pos_row, 1.0, 0.0).astype(BF16)
    pltpu.make_async_copy(ebuf, ebuf, sem.at[0]).wait()
    picked_ref[...] = lax.dot_general(tok_hot, ebuf[...], TN, preferred_element_type=F32).astype(BF16)
    pltpu.make_async_copy(pbuf, pbuf, sem.at[1]).wait()
    posrow_ref[...] = lax.dot_general(pos_hot, pbuf[...], TN, preferred_element_type=F32)


def norm_rows(x, ln):
    mean = jnp.mean(x, axis=-1, keepdims=True)
    centred = x - mean
    var = jnp.mean(centred * centred, axis=-1, keepdims=True)
    return (centred * lax.rsqrt(var + 1e-5) * ln[0:1, :] + ln[1:2, :]).astype(BF16)


def block_diag(q8):
    lane = lax.broadcasted_iota(jnp.int32, (8, 128), 1)
    qf = q8.astype(F32)
    both = jnp.concatenate([jnp.where(lane < 64, qf, 0.0), jnp.where(lane < 64, 0.0, qf)], axis=0)
    row = lax.rem(lax.broadcasted_iota(jnp.int32, (16, 128), 0), 8)
    blocks = [jnp.where(row == b, both, 0.0).astype(BF16) for b in range(8)]
    return both, jnp.concatenate(blocks, axis=1)


def fold_heads(o16):
    lane = lax.broadcasted_iota(jnp.int32, (8, 128), 1)
    row = lax.broadcasted_iota(jnp.int32, (8, 128), 0)
    out = jnp.zeros((8, 128), F32)
    for b in range(8):
        blk = jnp.where(lane < 64, o16[0:8, b * 128:(b + 1) * 128], o16[8:16, b * 128:(b + 1) * 128])
        out = jnp.where(row == b, blk, out)
    return out


def decoder_kernel(dims, pos_smem, picked_ref, posrow_ref, in_bias_hbm, out_bias_hbm, b_fc1_hbm, ln_layers_hbm, ln_final_hbm,
                   sk_hbm, sv_hbm, ck_hbm, cv_hbm, emb_hbm, wqkv_hbm, wcq_hbm, wout_hbm, fc1_hbm, fc2_hbm,
                   kvo, eo, fh_ref,
                   in_bias, out_bias, b_fc1, ln_layers, ln_final, kbuf, vbuf, wqkv, wcq, wout, fc1, fc2,
                   xres, stage, stage0, pair, pair0, chips, chips0, full, qscr, oscr, knew, vnew,
                   small_sem, self_sem, cross_sem, w_sem, e_sem, send_sem, recv_sem):
    layers, batch, ctx, frames = dims
    me = lax.axis_index('tp')
    ko, vo = kvo.at[0], kvo.at[1]
    hb = batch // HALVES
    rows_per = 128

    def self_copy(layer, which):
        src, dst = ((sk_hbm, ko), (sv_hbm, vo))[which]
        return pltpu.make_async_copy(src.at[layer], dst.at[layer], self_sem.at[layer, which])

    def cross_copy(layer, which, octet):
        src, dst = ((ck_hbm, kbuf), (cv_hbm, vbuf))[which]
        at = pl.ds(pl.multiple_of(octet * 1024, 1024), 1024)
        return pltpu.make_async_copy(src.at[layer, at, :], dst.at[at, :], cross_sem.at[layer, which, octet])

    weights = ((wqkv_hbm, wqkv), (wout_hbm, wout), (wcq_hbm, wcq), (fc1_hbm, fc1), (fc2_hbm, fc2))

    def w_copy(which, layer):
        src, dst = weights[which]
        return pltpu.make_async_copy(src.at[layer], dst.at[layer], w_sem.at[which, layer])

    small = [pltpu.make_async_copy(src, dst, small_sem.at[i]) for i, (src, dst) in enumerate((
        (ln_layers_hbm, ln_layers), (in_bias_hbm, in_bias), (out_bias_hbm, out_bias), (b_fc1_hbm, b_fc1), (ln_final_hbm, ln_final)))]
    for c in small:
        c.start()
    e_rows = emb_hbm.shape[0] // 4

    def e_copy(i):
        at = pl.ds(i * e_rows, e_rows)
        return pltpu.make_async_copy(emb_hbm.at[at, :], eo.at[at, :], e_sem.at[i])

    pending = []

    def pump(n):
        for group in pending[:n]:
            for c in group:
                c.start()
        del pending[:n]

    for octet in range(batch // 8):
        for which in range(2):
            pending.append([cross_copy(0, which, octet)])
    pending.append([w_copy(3, 0), w_copy(4, 0)])
    pending.append([w_copy(0, 1), w_copy(1, 1), w_copy(2, 1)])
    pending.append([self_copy(1, 0)])
    pending.append([self_copy(1, 1)])
    for octet in range(batch // 8):
        for which in range(2):
            pending.append([cross_copy(1, which, octet)])
    pending.append([w_copy(3, 1), w_copy(4, 1)])
    for i in range(4):
        pending.append([e_copy(i)])

    w_copy(0, 0).start()
    self_copy(0, 0).start()
    self_copy(0, 1).start()
    w_copy(1, 0).start()
    w_copy(2, 0).start()

    barrier = pltpu.get_barrier_semaphore()
    for k in range(1, TP):
        pl.semaphore_signal(barrier, 1, device_id={'tp': lax.rem(me + k, TP)}, device_id_type=MESH)
    pl.semaphore_wait(barrier, TP - 1)

    core = lax.rem(me, 2)
    chip = me // 2
    partner = {'tp': 2 * chip + 1 - core}
    wide = posrow_ref.shape[1] // 2

    def bufs(ph, s):
        if ph == 0:
            return stage0.at[s], pair0.at[s], chips0.at[s], full.at[0, s]
        slot = ph % PARITY
        return stage.at[slot, s], pair.at[slot, s], chips.at[slot, s], full.at[slot, s]

    def send(src, dst, ph, s, step, device):
        pltpu.make_async_remote_copy(src, dst, send_sem.at[ph, s, step], recv_sem.at[ph, s, step], device_id=device, device_id_type=MESH).start()

    def wait_for(ref, sem):
        pltpu.make_async_copy(ref, ref, sem).wait()

    def sum_start(ph, s, value):
        mine, got, _, _ = bufs(ph, s)
        mine[0] = value[:, :wide]
        mine[1] = value[:, wide:]
        send(mine.at[1 - core], got, ph, s, 0, partner)

    def sum_chips(ph, s):
        mine, got, by_chip, _ = bufs(ph, s)
        wait_for(got, recv_sem.at[ph, s, 0])
        by_chip[chip] = mine[core] + got[...]
        for k in range(1, TP // 2):
            send(by_chip.at[chip], by_chip.at[chip], ph, s, 1, {'tp': 2 * lax.rem(chip + k, TP // 2) + core})
        wait_for(got, send_sem.at[ph, s, 0])

    def sum_share(ph, s):
        _, _, by_chip, both = bufs(ph, s)
        others = by_chip.at[pl.ds(0, TP // 2 - 1)]
        wait_for(others, recv_sem.at[ph, s, 1])
        total = by_chip[0].astype(F32)
        for q in range(1, TP // 2):
            total = total + by_chip[q].astype(F32)
        both[core] = total.astype(BF16)
        send(both.at[core], both.at[core], ph, s, 2, partner)
        wait_for(others, send_sem.at[ph, s, 1])

    def sum_finish(ph, s):
        both = bufs(ph, s)[3]
        wait_for(both.at[0], recv_sem.at[ph, s, 2])
        wait_for(both.at[0], send_sem.at[ph, s, 2])
        return jnp.concatenate([both[0].astype(F32), both[1].astype(F32)], axis=1)

    def head_bias(layer, which):
        b = in_bias[layer, which]
        return jnp.concatenate([b[0:1, :], b[1:2, :]], axis=1)

    def half(s):
        return pl.ds(s * hb, hb)

    def self_block(layer, s, early, late):
        hidden = norm_rows(xres[half(s), :], ln_layers[layer, 0])
        proj = lax.dot_general(hidden, wqkv[layer], NT, preferred_element_type=F32)
        qscr[half(s), :] = (proj[:, 0:128] + head_bias(layer, 0)).astype(BF16).astype(F32)
        knew[layer, half(s), :] = proj[:, 128:256].astype(BF16).astype(F32)
        vnew[layer, half(s), :] = (proj[:, 256:384] + head_bias(layer, 1)).astype(BF16).astype(F32)

        for i in range(hb // 8):
            octet = s * (hb // 8) + i
            r8 = pl.ds(octet * 8, 8)
            at = pl.ds(octet * 1024, 1024)
            both, qbd = block_diag(qscr[r8, :])
            seq = lax.rem(lax.broadcasted_iota(jnp.int32, (16, 1), 0), 8)
            limit = jnp.zeros((16, 1), jnp.int32)
            for b in range(8):
                limit = jnp.where(seq == b, pos_smem[octet * 8 + b], limit)
            past = jnp.dot(qbd, ko[layer, at, :], preferred_element_type=F32) * 0.125
            t = lax.broadcasted_iota(jnp.int32, (16, ctx), 1)
            past = jnp.where(t < limit, past, -1e30)
            kn = knew[layer, r8, :]
            vn = vnew[layer, r8, :]
            new = jnp.sum(both * jnp.concatenate([kn, kn], axis=0), axis=1, keepdims=True) * 0.125
            peak = jnp.maximum(jnp.max(past, axis=1, keepdims=True), new)
            past_e = jnp.exp(past - peak)
            new_e = jnp.exp(new - peak)
            denom = jnp.sum(past_e, axis=1, keepdims=True) + new_e
            past_w = (past_e / denom).astype(BF16)
            new_w = (new_e / denom).astype(BF16).astype(F32)
            o16 = lax.dot_general(past_w, vo[layer, at, :], NT, preferred_element_type=F32)
            lane = lax.broadcasted_iota(jnp.int32, (8, 128), 1)
            oscr[r8, :] = fold_heads(o16) + jnp.where(lane < 64, new_w[0:8], new_w[8:16]) * vn
        return jnp.dot(oscr[half(s), :].astype(BF16), wout[layer, 0], preferred_element_type=F32)

    def cross_block(layer, s, early, late):
        hidden = norm_rows(xres[half(s), :], ln_layers[layer, 1])
        proj = lax.dot_general(hidden, wcq[layer], NT, preferred_element_type=F32)
        qscr[half(s), :] = (proj + head_bias(layer, 2)).astype(BF16).astype(F32)

        for i in range(hb // 8):
            octet = s * (hb // 8) + i
            r8 = pl.ds(octet * 8, 8)
            at = pl.ds(octet * 1024, 1024)
            _, qbd = block_diag(qscr[r8, :])
            cross_copy(layer, 0, octet).wait()
            scores = jnp.dot(qbd, kbuf[at, :], preferred_element_type=F32) * 0.125
            peak = jnp.max(scores, axis=1, keepdims=True)
            exps = jnp.exp(scores - peak)
            w = (exps / jnp.sum(exps, axis=1, keepdims=True)).astype(BF16)
            if i == 0:
                early()
            if i == hb // 8 - 1:
                late()
            cross_copy(layer, 1, octet).wait()
            o16 = lax.dot_general(w, vbuf[at, :], NT, preferred_element_type=F32)
            oscr[r8, :] = fold_heads(o16)
        return jnp.dot(oscr[half(s), :].astype(BF16), wout[layer, 1], preferred_element_type=F32)

    def mlp_block(layer, s, early, late):
        hidden = norm_rows(xres[half(s), :], ln_layers[layer, 2])
        pre = jnp.dot(hidden, fc1[layer], preferred_element_type=F32) + b_fc1[layer:layer + 1, :]
        active = (0.5 * pre * (1.0 + lax.erf(pre * (0.5 ** 0.5)))).astype(BF16)
        return jnp.dot(active, fc2[layer], preferred_element_type=F32)

    def write_new(layer, s):
        t = lax.broadcasted_iota(jnp.int32, (rows_per, ctx), 1)
        for new, cache in ((knew, ko), (vnew, vo)):
            cols = new[layer, half(s), :].T
            for i in range(hb):
                b = s * hb + i
                at = pl.ds(b * rows_per, rows_per)
                old = cache[layer, at, :].astype(F32)
                cache[layer, at, :] = jnp.where(t == pos_smem[b], cols[:, i:i + 1], old).astype(BF16)

    def nothing():
        pass

    def ready(nl, nk):
        if nk == 0:
            w_copy(0, nl).wait()
            self_copy(nl, 0).wait()
            self_copy(nl, 1).wait()
            w_copy(1, nl).wait()
        if nk == 1:
            w_copy(2, nl).wait()
        if nk == 2:
            w_copy(3, nl).wait()
            w_copy(4, nl).wait()

    for s in range(2):
        sum_start(0, s, picked_ref[half(s), :])
    for s in range(2):
        sum_chips(0, s)
    pump(2)
    for c in small:
        c.wait()
    sum_share(0, 0)
    for ph in range(3 * layers + 1):
        layer, kind = divmod(ph, 3)
        before, prev_kind = divmod(ph - 1, 3)

        def update(s):
            total = sum_finish(ph, s)
            if ph == 0:
                xres[half(s), :] = total + posrow_ref[half(s), :]
            else:
                xres[half(s), :] = xres[half(s), :] + total + out_bias[prev_kind, before:before + 1, :]

        if ph == 3 * layers:
            sum_share(ph, 1)
            for s in range(2):
                update(s)
                fh_ref[half(s), :] = norm_rows(xres[half(s), :], ln_final)
            break
        block = (self_block, cross_block, mlp_block)[kind]
        update(0)
        ready(layer, kind)
        share = functools.partial(sum_share, ph, 1)
        gather = functools.partial(sum_chips, ph + 1, 0)
        if kind == 1:
            sum_start(ph + 1, 0, block(layer, 0, nothing, share))
            pump(2)
            update(1)
            sum_start(ph + 1, 1, block(layer, 1, gather, nothing))
        else:
            sum_start(ph + 1, 0, block(layer, 0, nothing, nothing))
            gather()
            share()
            pump(2)
            update(1)
            sum_start(ph + 1, 1, block(layer, 1, nothing, nothing))
        if kind == 0:
            write_new(layer, 0)
        sum_chips(ph + 1, 1)
        pump(2)
        if kind == 0:
            write_new(layer, 1)
        sum_share(ph + 1, 0)
    for i in range(4):
        e_copy(i).wait()


def final_kernel(kv_ref, e_ref, fh_ref, logits_hbm, ko_hbm, vo_hbm, logits, sem, out_sem):
    layers, rows = kv_ref.shape[1:3]
    copies = []
    for layer in range(layers):
        for which, dst in enumerate((ko_hbm, vo_hbm)):
            for part in range(4):
                at = pl.ds(part * (rows // 4), rows // 4)
                c = pltpu.make_async_copy(kv_ref.at[which, layer, at, :], dst.at[layer, at, :], sem.at[layer, which, part])
                c.start()
                copies.append(c)
    fh = fh_ref[...]
    step = 384
    n = e_ref.shape[0] // step

    def out_copy(i):
        at = pl.ds(pl.multiple_of(i * step, step), step)
        return pltpu.make_async_copy(logits.at[:, at], logits_hbm.at[:, at], out_sem)

    def body(i, carry):
        at = pl.ds(pl.multiple_of(i * step, step), step)
        logits[:, at] = lax.dot_general(fh, e_ref[at, :], NT, preferred_element_type=F32)
        out_copy(i).start()
        return carry

    lax.fori_loop(0, n, body, 0)
    pltpu.make_async_copy(logits, logits_hbm, out_sem).wait()
    for c in copies:
        c.wait()


def solution(mesh):
    vm = pl.BlockSpec(memory_space=pltpu.VMEM)
    sm = pl.BlockSpec(memory_space=pltpu.SMEM)
    hbm = pl.BlockSpec(memory_space=pltpu.HBM)

    def local_step(tokens, positions, self_keys, self_vals, cross_keys, cross_vals, embed_table, pos_table, w_qkv, w_cq, in_bias, w_out, out_bias, w_fc1, b_fc1, w_fc2, ln_layers, ln_final):
        batch = tokens.shape[0]
        layers, _, ctx, heads, hd = self_keys.shape
        frames = cross_keys.shape[2]
        vocab, d = embed_table.shape
        ff = w_fc1.shape[2]
        rows = batch * heads * hd
        hb = batch // HALVES

        def flat(cache):
            return cache.transpose(0, 1, 3, 4, 2).reshape(layers, rows, cache.shape[2])

        picked, posrow = pl.pallas_call(
            gather_kernel,
            out_shape=(pltpu.VMEM((batch, d), BF16), pltpu.VMEM((batch, d), F32)),
            in_specs=[sm, sm, vm, vm, hbm, hbm], out_specs=(vm, vm),
            scratch_shapes=[pltpu.VMEM((16 * batch, d), BF16), pltpu.VMEM((16 * batch, d), BF16), pltpu.SemaphoreType.DMA((2,))],
            compiler_params=pltpu.CompilerParams(vmem_limit_bytes=60 * 2 ** 20),
            name='gather_rows',
        )(tokens, positions, tokens.reshape(1, batch), positions.reshape(1, batch), embed_table, pos_table)

        picked, posrow = (pltpu.with_memory_space_constraint(a, pltpu.VMEM) for a in (picked, posrow))
        kvo, eo, fh = pl.pallas_call(
            functools.partial(decoder_kernel, (layers, batch, ctx, frames)),
            out_shape=(pltpu.VMEM((2, layers, rows, ctx), BF16), pltpu.VMEM((vocab, d), BF16), pltpu.VMEM((batch, d), BF16)),
            in_specs=[sm] + [vm] * 2 + [hbm] * 15,
            out_specs=(vm, vm, vm),
            scratch_shapes=[
                pltpu.VMEM(in_bias.shape, F32), pltpu.VMEM((3, layers, d), F32), pltpu.VMEM(b_fc1.shape, F32), pltpu.VMEM(ln_layers.shape, F32), pltpu.VMEM(ln_final.shape, F32),
                pltpu.VMEM((rows, frames), BF16), pltpu.VMEM((rows, frames), BF16),
                pltpu.VMEM((layers, 3 * heads * hd, d), BF16), pltpu.VMEM((layers, heads * hd, d), BF16),
                pltpu.VMEM((layers, 2, heads * hd, d), BF16), pltpu.VMEM((layers, d, ff), BF16), pltpu.VMEM((layers, ff, d), BF16),
                pltpu.VMEM((batch, d), F32),
                pltpu.VMEM((PARITY, HALVES, 2, hb, d // 2), F32), pltpu.VMEM((HALVES, 2, hb, d // 2), BF16),
                pltpu.VMEM((PARITY, HALVES, hb, d // 2), F32), pltpu.VMEM((HALVES, hb, d // 2), BF16),
                pltpu.VMEM((PARITY, HALVES, TP // 2, hb, d // 2), F32), pltpu.VMEM((HALVES, TP // 2, hb, d // 2), BF16),
                pltpu.VMEM((PARITY, HALVES, 2, hb, d // 2), BF16),
                pltpu.VMEM((batch, 128), F32), pltpu.VMEM((batch, 128), F32),
                pltpu.VMEM((layers, batch, 128), F32), pltpu.VMEM((layers, batch, 128), F32),
                pltpu.SemaphoreType.DMA((5,)), pltpu.SemaphoreType.DMA((layers, 2)), pltpu.SemaphoreType.DMA((layers, 2, batch // 8)),
                pltpu.SemaphoreType.DMA((5, layers)), pltpu.SemaphoreType.DMA((4,)),
                pltpu.SemaphoreType.DMA((3 * layers + 1, HALVES, 3)), pltpu.SemaphoreType.DMA((3 * layers + 1, HALVES, 3)),
            ],
            compiler_params=pltpu.CompilerParams(collective_id=0, has_side_effects=True, vmem_limit_bytes=139 * 2 ** 18),
            name='decoder_layers',
        )(positions, picked, posrow, in_bias, out_bias.transpose(1, 0, 2), b_fc1, ln_layers, ln_final,
          flat(self_keys), flat(self_vals), flat(cross_keys), flat(cross_vals), embed_table,
          w_qkv.transpose(0, 2, 3, 4, 1).reshape(layers, 3 * heads * hd, d), w_cq.transpose(0, 2, 3, 1).reshape(layers, heads * hd, d),
          w_out.reshape(layers, 2, heads * hd, d), w_fc1, w_fc2)

        logits, nk, nv = pl.pallas_call(
            final_kernel,
            out_shape=(jax.ShapeDtypeStruct((batch, vocab), F32), jax.ShapeDtypeStruct((layers, rows, ctx), BF16), jax.ShapeDtypeStruct((layers, rows, ctx), BF16)),
            in_specs=[vm] * 3, out_specs=(hbm, hbm, hbm),
            scratch_shapes=[pltpu.VMEM((batch, vocab), F32), pltpu.SemaphoreType.DMA((layers, 2, 4)), pltpu.SemaphoreType.DMA],
            compiler_params=pltpu.CompilerParams(vmem_limit_bytes=2 * 2 ** 20),
            name='final_logits',
        )(kvo, eo, fh)

        def unflat(cache):
            return cache.reshape(layers, batch, heads, hd, ctx).transpose(0, 1, 4, 2, 3)

        return logits, unflat(nk), unflat(nv)

    batch_spec = P('dp')
    cache_spec = P(None, 'dp', None, 'tp', None)
    in_specs = (batch_spec, batch_spec, cache_spec, cache_spec, cache_spec, cache_spec, P('tp', None), P(None, None), P(None, None, None, 'tp', None), P(None, None, 'tp', None), P(None, None, 'tp', None), P(None, None, 'tp', None, None), P(None, None, None), P(None, None, 'tp'), P(None, 'tp'), P(None, 'tp', None), P(None, None, None, None), P(None, None))
    out_specs = (P('dp', 'tp'), cache_spec, cache_spec)
    return jax.shard_map(local_step, mesh=mesh, in_specs=in_specs, out_specs=out_specs, check_vma=False)
```

```python
import functools
import jax
import jax.numpy as jnp
from jax import lax
from jax.experimental import pallas as pl
from jax.experimental.pallas import tpu as pltpu
from jax.sharding import PartitionSpec as P

MESH = pl.DeviceIdType.MESH
F32 = jnp.float32
BF16 = jnp.bfloat16
NT = (((1,), (1,)), ((), ()))
TN = (((0,), (0,)), ((), ()))
TP = 8
HALVES = 2
PARITY = 2


def gather_kernel(tok_ref, pos_ref, tokv_ref, posv_ref, emb_hbm, pos_hbm, picked_ref, posrow_ref, ebuf, pbuf, sem):
    shard_rows = emb_hbm.shape[0]
    n = tok_ref.shape[0]
    base = lax.axis_index('tp') * shard_rows

    def start(b, carry):
        tid = jnp.clip(tok_ref[b] - base, 0, shard_rows - 1)
        pid = pos_ref[b]
        at = pl.ds(pl.multiple_of(b * 16, 16), 16)
        pltpu.make_async_copy(emb_hbm.at[pl.ds(pl.multiple_of(tid // 16 * 16, 16), 16), :], ebuf.at[at, :], sem.at[0]).start()
        pltpu.make_async_copy(pos_hbm.at[pl.ds(pl.multiple_of(pid // 16 * 16, 16), 16), :], pbuf.at[at, :], sem.at[1]).start()
        return carry

    lax.fori_loop(0, n, start, 0, unroll=4)
    tid = tokv_ref[...] - base
    owned = (tid >= 0) & (tid < shard_rows)
    lane16 = lax.broadcasted_iota(jnp.int32, (1, n), 1) * 16
    tok_row = jnp.where(owned, lane16 + jnp.clip(tid, 0, shard_rows - 1) % 16, -1)
    pos_row = lane16 + posv_ref[...] % 16
    row = lax.broadcasted_iota(jnp.int32, (16 * n, n), 0)
    tok_hot = jnp.where(row == tok_row, 1.0, 0.0).astype(BF16)
    pos_hot = jnp.where(row == pos_row, 1.0, 0.0).astype(BF16)
    pltpu.make_async_copy(ebuf, ebuf, sem.at[0]).wait()
    picked_ref[...] = lax.dot_general(tok_hot, ebuf[...], TN, preferred_element_type=F32).astype(BF16)
    pltpu.make_async_copy(pbuf, pbuf, sem.at[1]).wait()
    posrow_ref[...] = lax.dot_general(pos_hot, pbuf[...], TN, preferred_element_type=F32)


def norm_rows(x, ln):
    mean = jnp.mean(x, axis=-1, keepdims=True)
    centred = x - mean
    var = jnp.mean(centred * centred, axis=-1, keepdims=True)
    return (centred * lax.rsqrt(var + 1e-5) * ln[0:1, :] + ln[1:2, :]).astype(BF16)


def block_diag(q8):
    lane = lax.broadcasted_iota(jnp.int32, (8, 128), 1)
    qf = q8.astype(F32)
    both = jnp.concatenate([jnp.where(lane < 64, qf, 0.0), jnp.where(lane < 64, 0.0, qf)], axis=0)
    row = lax.rem(lax.broadcasted_iota(jnp.int32, (16, 128), 0), 8)
    blocks = [jnp.where(row == b, both, 0.0).astype(BF16) for b in range(8)]
    return both, jnp.concatenate(blocks, axis=1)


def fold_heads(o16):
    lane = lax.broadcasted_iota(jnp.int32, (8, 128), 1)
    row = lax.broadcasted_iota(jnp.int32, (8, 128), 0)
    out = jnp.zeros((8, 128), F32)
    for b in range(8):
        blk = jnp.where(lane < 64, o16[0:8, b * 128:(b + 1) * 128], o16[8:16, b * 128:(b + 1) * 128])
        out = jnp.where(row == b, blk, out)
    return out


def decoder_kernel(dims, pos_smem, picked_ref, posrow_ref, in_bias_hbm, out_bias_hbm, b_fc1_hbm, ln_layers_hbm, ln_final_hbm,
                   sk_hbm, sv_hbm, ck_hbm, cv_hbm, emb_hbm, wqkv_hbm, wcq_hbm, wout_hbm, fc1_hbm, fc2_hbm,
                   kvo, eo, fh_ref,
                   in_bias, out_bias, b_fc1, ln_layers, ln_final, kbuf, vbuf, wqkv, wcq, wout, fc1, fc2,
                   xres, stage, stage0, pair, pair0, chips, chips0, full, qscr, oscr, knew, vnew,
                   small_sem, self_sem, cross_sem, w_sem, e_sem, send_sem, recv_sem):
    layers, batch, ctx, frames = dims
    me = lax.axis_index('tp')
    ko, vo = kvo.at[0], kvo.at[1]
    hb = batch // HALVES
    rows_per = 128

    def self_copy(layer, which):
        src, dst = ((sk_hbm, ko), (sv_hbm, vo))[which]
        return pltpu.make_async_copy(src.at[layer], dst.at[layer], self_sem.at[layer, which])

    def cross_copy(layer, which, octet):
        src, dst = ((ck_hbm, kbuf), (cv_hbm, vbuf))[which]
        at = pl.ds(pl.multiple_of(octet * 1024, 1024), 1024)
        return pltpu.make_async_copy(src.at[layer, at, :], dst.at[at, :], cross_sem.at[layer, which, octet])

    weights = ((wqkv_hbm, wqkv), (wout_hbm, wout), (wcq_hbm, wcq), (fc1_hbm, fc1), (fc2_hbm, fc2))

    def w_copy(which, layer):
        src, dst = weights[which]
        return pltpu.make_async_copy(src.at[layer], dst.at[layer], w_sem.at[which, layer])

    small = [pltpu.make_async_copy(src, dst, small_sem.at[i]) for i, (src, dst) in enumerate((
        (ln_layers_hbm, ln_layers), (in_bias_hbm, in_bias), (out_bias_hbm, out_bias), (b_fc1_hbm, b_fc1), (ln_final_hbm, ln_final)))]
    for c in small:
        c.start()
    e_rows = emb_hbm.shape[0] // 4

    def e_copy(i):
        at = pl.ds(i * e_rows, e_rows)
        return pltpu.make_async_copy(emb_hbm.at[at, :], eo.at[at, :], e_sem.at[i])

    pending = []

    def pump(n):
        for group in pending[:n]:
            for c in group:
                c.start()
        del pending[:n]

    for octet in range(batch // 8):
        for which in range(2):
            pending.append([cross_copy(0, which, octet)])
    pending.append([w_copy(3, 0), w_copy(4, 0)])
    pending.append([w_copy(0, 1), w_copy(1, 1), w_copy(2, 1)])
    pending.append([self_copy(1, 0)])
    pending.append([self_copy(1, 1)])
    for octet in range(batch // 8):
        for which in range(2):
            pending.append([cross_copy(1, which, octet)])
    pending.append([w_copy(3, 1), w_copy(4, 1)])
    for i in range(4):
        pending.append([e_copy(i)])

    w_copy(0, 0).start()
    self_copy(0, 0).start()
    self_copy(0, 1).start()
    w_copy(1, 0).start()
    w_copy(2, 0).start()

    barrier = pltpu.get_barrier_semaphore()
    for k in range(1, TP):
        pl.semaphore_signal(barrier, 1, device_id={'tp': lax.rem(me + k, TP)}, device_id_type=MESH)
    pl.semaphore_wait(barrier, TP - 1)

    core = lax.rem(me, 2)
    chip = me // 2
    partner = {'tp': 2 * chip + 1 - core}
    wide = posrow_ref.shape[1] // 2

    def bufs(ph, s):
        if ph == 0:
            return stage0.at[s], pair0.at[s], chips0.at[s], full.at[0, s]
        slot = ph % PARITY
        return stage.at[slot, s], pair.at[slot, s], chips.at[slot, s], full.at[slot, s]

    def send(src, dst, ph, s, step, device):
        pltpu.make_async_remote_copy(src, dst, send_sem.at[ph, s, step], recv_sem.at[ph, s, step], device_id=device, device_id_type=MESH).start()

    def wait_for(ref, sem):
        pltpu.make_async_copy(ref, ref, sem).wait()

    def sum_start(ph, s, value):
        mine, got, _, _ = bufs(ph, s)
        mine[0] = value[:, :wide]
        mine[1] = value[:, wide:]
        send(mine.at[1 - core], got, ph, s, 0, partner)

    def sum_chips(ph, s):
        mine, got, by_chip, _ = bufs(ph, s)
        wait_for(got, recv_sem.at[ph, s, 0])
        by_chip[chip] = mine[core] + got[...]
        for k in range(1, TP // 2):
            send(by_chip.at[chip], by_chip.at[chip], ph, s, 1, {'tp': 2 * lax.rem(chip + k, TP // 2) + core})
        wait_for(got, send_sem.at[ph, s, 0])

    def sum_share(ph, s):
        _, _, by_chip, both = bufs(ph, s)
        others = by_chip.at[pl.ds(0, TP // 2 - 1)]
        wait_for(others, recv_sem.at[ph, s, 1])
        total = by_chip[0].astype(F32)
        for q in range(1, TP // 2):
            total = total + by_chip[q].astype(F32)
        both[core] = total.astype(BF16)
        send(both.at[core], both.at[core], ph, s, 2, partner)
        wait_for(others, send_sem.at[ph, s, 1])

    def sum_finish(ph, s):
        both = bufs(ph, s)[3]
        wait_for(both.at[0], recv_sem.at[ph, s, 2])
        wait_for(both.at[0], send_sem.at[ph, s, 2])
        return jnp.concatenate([both[0].astype(F32), both[1].astype(F32)], axis=1)

    def head_bias(layer, which):
        b = in_bias[layer, which]
        return jnp.concatenate([b[0:1, :], b[1:2, :]], axis=1)

    def half(s):
        return pl.ds(s * hb, hb)

    def self_block(layer, s, early, late):
        hidden = norm_rows(xres[half(s), :], ln_layers[layer, 0])
        proj = lax.dot_general(hidden, wqkv[layer], NT, preferred_element_type=F32)
        qscr[half(s), :] = (proj[:, 0:128] + head_bias(layer, 0)).astype(BF16).astype(F32)
        knew[layer, half(s), :] = proj[:, 128:256].astype(BF16).astype(F32)
        vnew[layer, half(s), :] = (proj[:, 256:384] + head_bias(layer, 1)).astype(BF16).astype(F32)

        for i in range(hb // 8):
            octet = s * (hb // 8) + i
            r8 = pl.ds(octet * 8, 8)
            at = pl.ds(octet * 1024, 1024)
            both, qbd = block_diag(qscr[r8, :])
            seq = lax.rem(lax.broadcasted_iota(jnp.int32, (16, 1), 0), 8)
            limit = jnp.zeros((16, 1), jnp.int32)
            for b in range(8):
                limit = jnp.where(seq == b, pos_smem[octet * 8 + b], limit)
            past = jnp.dot(qbd, ko[layer, at, :], preferred_element_type=F32) * 0.125
            t = lax.broadcasted_iota(jnp.int32, (16, ctx), 1)
            past = jnp.where(t < limit, past, -1e30)
            kn = knew[layer, r8, :]
            vn = vnew[layer, r8, :]
            new = jnp.sum(both * jnp.concatenate([kn, kn], axis=0), axis=1, keepdims=True) * 0.125
            peak = jnp.maximum(jnp.max(past, axis=1, keepdims=True), new)
            past_e = jnp.exp(past - peak)
            new_e = jnp.exp(new - peak)
            denom = jnp.sum(past_e, axis=1, keepdims=True) + new_e
            past_w = (past_e / denom).astype(BF16)
            new_w = (new_e / denom).astype(BF16).astype(F32)
            o16 = lax.dot_general(past_w, vo[layer, at, :], NT, preferred_element_type=F32)
            lane = lax.broadcasted_iota(jnp.int32, (8, 128), 1)
            oscr[r8, :] = fold_heads(o16) + jnp.where(lane < 64, new_w[0:8], new_w[8:16]) * vn
        return jnp.dot(oscr[half(s), :].astype(BF16), wout[layer, 0], preferred_element_type=F32)

    def cross_block(layer, s, early, late):
        hidden = norm_rows(xres[half(s), :], ln_layers[layer, 1])
        proj = lax.dot_general(hidden, wcq[layer], NT, preferred_element_type=F32)
        qscr[half(s), :] = (proj + head_bias(layer, 2)).astype(BF16).astype(F32)

        octets = range(s * (hb // 8), (s + 1) * (hb // 8))
        for octet in octets:
            cross_copy(layer, 0, octet).wait()
        scores = []
        for octet in octets:
            _, qbd = block_diag(qscr[pl.ds(octet * 8, 8), :])
            scores.append(jnp.dot(qbd, kbuf[pl.ds(octet * 1024, 1024), :], preferred_element_type=F32) * 0.125)
        early()
        for octet in octets:
            cross_copy(layer, 1, octet).wait()
        for octet, sc in zip(octets, scores):
            exps = jnp.exp(sc - jnp.max(sc, axis=1, keepdims=True))
            w = (exps / jnp.sum(exps, axis=1, keepdims=True)).astype(BF16)
            if octet == octets[-1]:
                late()
            o16 = lax.dot_general(w, vbuf[pl.ds(octet * 1024, 1024), :], NT, preferred_element_type=F32)
            oscr[pl.ds(octet * 8, 8), :] = fold_heads(o16)
        return jnp.dot(oscr[half(s), :].astype(BF16), wout[layer, 1], preferred_element_type=F32)

    def mlp_block(layer, s, early, late):
        hidden = norm_rows(xres[half(s), :], ln_layers[layer, 2])
        pre = jnp.dot(hidden, fc1[layer], preferred_element_type=F32) + b_fc1[layer:layer + 1, :]
        active = (0.5 * pre * (1.0 + lax.erf(pre * (0.5 ** 0.5)))).astype(BF16)
        return jnp.dot(active, fc2[layer], preferred_element_type=F32)

    def write_new(layer, s):
        t = lax.broadcasted_iota(jnp.int32, (rows_per, ctx), 1)
        for new, cache in ((knew, ko), (vnew, vo)):
            cols = new[layer, half(s), :].T
            for i in range(hb):
                b = s * hb + i
                at = pl.ds(b * rows_per, rows_per)
                old = cache[layer, at, :].astype(F32)
                cache[layer, at, :] = jnp.where(t == pos_smem[b], cols[:, i:i + 1], old).astype(BF16)

    def nothing():
        pass

    def ready(nl, nk):
        if nk == 0:
            w_copy(0, nl).wait()
            self_copy(nl, 0).wait()
            self_copy(nl, 1).wait()
            w_copy(1, nl).wait()
        if nk == 1:
            w_copy(2, nl).wait()
        if nk == 2:
            w_copy(3, nl).wait()
            w_copy(4, nl).wait()

    for s in range(2):
        sum_start(0, s, picked_ref[half(s), :])
    for s in range(2):
        sum_chips(0, s)
    pump(2)
    for c in small:
        c.wait()
    for s in range(2):
        sum_share(0, s)
    for ph in range(3 * layers + 1):
        layer, kind = divmod(ph, 3)
        before, prev_kind = divmod(ph - 1, 3)

        def update(s):
            total = sum_finish(ph, s)
            if ph == 0:
                xres[half(s), :] = total + posrow_ref[half(s), :]
            else:
                xres[half(s), :] = xres[half(s), :] + total + out_bias[prev_kind, before:before + 1, :]

        if ph == 3 * layers:
            sum_share(ph, 1)
            for s in range(2):
                update(s)
                fh_ref[half(s), :] = norm_rows(xres[half(s), :], ln_final)
            break
        block = (self_block, cross_block, mlp_block)[kind]
        update(0)
        ready(layer, kind)
        share = functools.partial(sum_share, ph, 1)
        gather = functools.partial(sum_chips, ph + 1, 0)
        if kind == 1:
            sum_start(ph + 1, 0, block(layer, 0, nothing, share))
            pump(2)
            update(1)
            sum_start(ph + 1, 1, block(layer, 1, gather, nothing))
        else:
            sum_start(ph + 1, 0, block(layer, 0, nothing, nothing))
            if kind == 2:
                write_new(layer, 0)
                gather()
                write_new(layer, 1)
                share()
            else:
                if ph > 0:
                    share()
                gather()
            pump(2)
            update(1)
            sum_start(ph + 1, 1, block(layer, 1, nothing, nothing))
        sum_chips(ph + 1, 1)
        pump(2)
        sum_share(ph + 1, 0)
    for i in range(4):
        e_copy(i).wait()


def final_kernel(kv_ref, e_ref, fh_ref, logits_hbm, ko_hbm, vo_hbm, logits, sem, out_sem):
    layers, rows = kv_ref.shape[1:3]
    copies = []
    for layer in range(layers):
        for which, dst in enumerate((ko_hbm, vo_hbm)):
            for part in range(4):
                at = pl.ds(part * (rows // 4), rows // 4)
                c = pltpu.make_async_copy(kv_ref.at[which, layer, at, :], dst.at[layer, at, :], sem.at[layer, which, part])
                c.start()
                copies.append(c)
    fh = fh_ref[...]
    step = 384
    n = e_ref.shape[0] // step

    def out_copy(i):
        at = pl.ds(pl.multiple_of(i * step, step), step)
        return pltpu.make_async_copy(logits.at[:, at], logits_hbm.at[:, at], out_sem)

    def body(i, carry):
        at = pl.ds(pl.multiple_of(i * step, step), step)
        logits[:, at] = lax.dot_general(fh, e_ref[at, :], NT, preferred_element_type=F32)
        out_copy(i).start()
        return carry

    lax.fori_loop(0, n, body, 0)
    pltpu.make_async_copy(logits, logits_hbm, out_sem).wait()
    for c in copies:
        c.wait()


def solution(mesh):
    vm = pl.BlockSpec(memory_space=pltpu.VMEM)
    sm = pl.BlockSpec(memory_space=pltpu.SMEM)
    hbm = pl.BlockSpec(memory_space=pltpu.HBM)

    def local_step(tokens, positions, self_keys, self_vals, cross_keys, cross_vals, embed_table, pos_table, w_qkv, w_cq, in_bias, w_out, out_bias, w_fc1, b_fc1, w_fc2, ln_layers, ln_final):
        batch = tokens.shape[0]
        layers, _, ctx, heads, hd = self_keys.shape
        frames = cross_keys.shape[2]
        vocab, d = embed_table.shape
        ff = w_fc1.shape[2]
        rows = batch * heads * hd
        hb = batch // HALVES

        def flat(cache):
            return cache.transpose(0, 1, 3, 4, 2).reshape(layers, rows, cache.shape[2])

        picked, posrow = pl.pallas_call(
            gather_kernel,
            out_shape=(pltpu.VMEM((batch, d), BF16), pltpu.VMEM((batch, d), F32)),
            in_specs=[sm, sm, vm, vm, hbm, hbm], out_specs=(vm, vm),
            scratch_shapes=[pltpu.VMEM((16 * batch, d), BF16), pltpu.VMEM((16 * batch, d), BF16), pltpu.SemaphoreType.DMA((2,))],
            compiler_params=pltpu.CompilerParams(vmem_limit_bytes=60 * 2 ** 20),
            name='gather_rows',
        )(tokens, positions, tokens.reshape(1, batch), positions.reshape(1, batch), embed_table, pos_table)

        picked, posrow = (pltpu.with_memory_space_constraint(a, pltpu.VMEM) for a in (picked, posrow))
        kvo, eo, fh = pl.pallas_call(
            functools.partial(decoder_kernel, (layers, batch, ctx, frames)),
            out_shape=(pltpu.VMEM((2, layers, rows, ctx), BF16), pltpu.VMEM((vocab, d), BF16), pltpu.VMEM((batch, d), BF16)),
            in_specs=[sm] + [vm] * 2 + [hbm] * 15,
            out_specs=(vm, vm, vm),
            scratch_shapes=[
                pltpu.VMEM(in_bias.shape, F32), pltpu.VMEM((3, layers, d), F32), pltpu.VMEM(b_fc1.shape, F32), pltpu.VMEM(ln_layers.shape, F32), pltpu.VMEM(ln_final.shape, F32),
                pltpu.VMEM((rows, frames), BF16), pltpu.VMEM((rows, frames), BF16),
                pltpu.VMEM((layers, 3 * heads * hd, d), BF16), pltpu.VMEM((layers, heads * hd, d), BF16),
                pltpu.VMEM((layers, 2, heads * hd, d), BF16), pltpu.VMEM((layers, d, ff), BF16), pltpu.VMEM((layers, ff, d), BF16),
                pltpu.VMEM((batch, d), F32),
                pltpu.VMEM((PARITY, HALVES, 2, hb, d // 2), F32), pltpu.VMEM((HALVES, 2, hb, d // 2), BF16),
                pltpu.VMEM((PARITY, HALVES, hb, d // 2), F32), pltpu.VMEM((HALVES, hb, d // 2), BF16),
                pltpu.VMEM((PARITY, HALVES, TP // 2, hb, d // 2), F32), pltpu.VMEM((HALVES, TP // 2, hb, d // 2), BF16),
                pltpu.VMEM((PARITY, HALVES, 2, hb, d // 2), BF16),
                pltpu.VMEM((batch, 128), F32), pltpu.VMEM((batch, 128), F32),
                pltpu.VMEM((layers, batch, 128), F32), pltpu.VMEM((layers, batch, 128), F32),
                pltpu.SemaphoreType.DMA((5,)), pltpu.SemaphoreType.DMA((layers, 2)), pltpu.SemaphoreType.DMA((layers, 2, batch // 8)),
                pltpu.SemaphoreType.DMA((5, layers)), pltpu.SemaphoreType.DMA((4,)),
                pltpu.SemaphoreType.DMA((3 * layers + 1, HALVES, 3)), pltpu.SemaphoreType.DMA((3 * layers + 1, HALVES, 3)),
            ],
            compiler_params=pltpu.CompilerParams(collective_id=0, has_side_effects=True, vmem_limit_bytes=139 * 2 ** 18),
            name='decoder_layers',
        )(positions, picked, posrow, in_bias, out_bias.transpose(1, 0, 2), b_fc1, ln_layers, ln_final,
          flat(self_keys), flat(self_vals), flat(cross_keys), flat(cross_vals), embed_table,
          w_qkv.transpose(0, 2, 3, 4, 1).reshape(layers, 3 * heads * hd, d), w_cq.transpose(0, 2, 3, 1).reshape(layers, heads * hd, d),
          w_out.reshape(layers, 2, heads * hd, d), w_fc1, w_fc2)

        logits, nk, nv = pl.pallas_call(
            final_kernel,
            out_shape=(jax.ShapeDtypeStruct((batch, vocab), F32), jax.ShapeDtypeStruct((layers, rows, ctx), BF16), jax.ShapeDtypeStruct((layers, rows, ctx), BF16)),
            in_specs=[vm] * 3, out_specs=(hbm, hbm, hbm),
            scratch_shapes=[pltpu.VMEM((batch, vocab), F32), pltpu.SemaphoreType.DMA((layers, 2, 4)), pltpu.SemaphoreType.DMA],
            compiler_params=pltpu.CompilerParams(vmem_limit_bytes=2 * 2 ** 20),
            name='final_logits',
        )(kvo, eo, fh)

        def unflat(cache):
            return cache.reshape(layers, batch, heads, hd, ctx).transpose(0, 1, 4, 2, 3)

        return logits, unflat(nk), unflat(nv)

    batch_spec = P('dp')
    cache_spec = P(None, 'dp', None, 'tp', None)
    in_specs = (batch_spec, batch_spec, cache_spec, cache_spec, cache_spec, cache_spec, P('tp', None), P(None, None), P(None, None, None, 'tp', None), P(None, None, 'tp', None), P(None, None, 'tp', None), P(None, None, 'tp', None, None), P(None, None, None), P(None, None, 'tp'), P(None, 'tp'), P(None, 'tp', None), P(None, None, None, None), P(None, None))
    out_specs = (P('dp', 'tp'), cache_spec, cache_spec)
    return jax.shard_map(local_step, mesh=mesh, in_specs=in_specs, out_specs=out_specs, check_vma=False)
```

```python
import functools
import jax
import jax.numpy as jnp
from jax import lax
from jax.experimental import pallas as pl
from jax.experimental.pallas import tpu as pltpu
from jax.sharding import PartitionSpec as P

MESH = pl.DeviceIdType.MESH
F32 = jnp.float32
BF16 = jnp.bfloat16
NT = (((1,), (1,)), ((), ()))
TN = (((0,), (0,)), ((), ()))
TP = 8
HALVES = 2
PARITY = 2


def gather_kernel(tok_ref, pos_ref, tokv_ref, posv_ref, emb_hbm, pos_hbm, picked_ref, posrow_ref, ebuf, pbuf, sem):
    shard_rows = emb_hbm.shape[0]
    n = tok_ref.shape[0]
    base = lax.axis_index('tp') * shard_rows

    def start(b, carry):
        tid = jnp.clip(tok_ref[b] - base, 0, shard_rows - 1)
        pid = pos_ref[b]
        at = pl.ds(pl.multiple_of(b * 16, 16), 16)
        pltpu.make_async_copy(emb_hbm.at[pl.ds(pl.multiple_of(tid // 16 * 16, 16), 16), :], ebuf.at[at, :], sem.at[0]).start()
        pltpu.make_async_copy(pos_hbm.at[pl.ds(pl.multiple_of(pid // 16 * 16, 16), 16), :], pbuf.at[at, :], sem.at[1]).start()
        return carry

    lax.fori_loop(0, n, start, 0, unroll=4)
    tid = tokv_ref[...] - base
    owned = (tid >= 0) & (tid < shard_rows)
    lane16 = lax.broadcasted_iota(jnp.int32, (1, n), 1) * 16
    tok_row = jnp.where(owned, lane16 + jnp.clip(tid, 0, shard_rows - 1) % 16, -1)
    pos_row = lane16 + posv_ref[...] % 16
    row = lax.broadcasted_iota(jnp.int32, (16 * n, n), 0)
    tok_hot = jnp.where(row == tok_row, 1.0, 0.0).astype(BF16)
    pos_hot = jnp.where(row == pos_row, 1.0, 0.0).astype(BF16)
    pltpu.make_async_copy(ebuf, ebuf, sem.at[0]).wait()
    picked_ref[...] = lax.dot_general(tok_hot, ebuf[...], TN, preferred_element_type=F32).astype(BF16)
    pltpu.make_async_copy(pbuf, pbuf, sem.at[1]).wait()
    posrow_ref[...] = lax.dot_general(pos_hot, pbuf[...], TN, preferred_element_type=F32)


def norm_rows(x, ln):
    mean = jnp.mean(x, axis=-1, keepdims=True)
    centred = x - mean
    var = jnp.mean(centred * centred, axis=-1, keepdims=True)
    return (centred * lax.rsqrt(var + 1e-5) * ln[0:1, :] + ln[1:2, :]).astype(BF16)


def block_diag(q8):
    lane = lax.broadcasted_iota(jnp.int32, (8, 128), 1)
    qf = q8.astype(F32)
    both = jnp.concatenate([jnp.where(lane < 64, qf, 0.0), jnp.where(lane < 64, 0.0, qf)], axis=0)
    row = lax.rem(lax.broadcasted_iota(jnp.int32, (16, 128), 0), 8)
    blocks = [jnp.where(row == b, both, 0.0).astype(BF16) for b in range(8)]
    return both, jnp.concatenate(blocks, axis=1)


def fold_heads(o16):
    lane = lax.broadcasted_iota(jnp.int32, (8, 128), 1)
    row = lax.broadcasted_iota(jnp.int32, (8, 128), 0)
    out = jnp.zeros((8, 128), F32)
    for b in range(8):
        blk = jnp.where(lane < 64, o16[0:8, b * 128:(b + 1) * 128], o16[8:16, b * 128:(b + 1) * 128])
        out = jnp.where(row == b, blk, out)
    return out


def decoder_kernel(dims, pos_smem, picked_ref, posrow_ref, in_bias_hbm, out_bias_hbm, b_fc1_hbm, ln_layers_hbm, ln_final_hbm,
                   sk_hbm, sv_hbm, ck_hbm, cv_hbm, emb_hbm, wqkv_hbm, wcq_hbm, wout_hbm, fc1_hbm, fc2_hbm,
                   kvo, eo, fh_ref,
                   in_bias, out_bias, b_fc1, ln_layers, ln_final, kbuf, vbuf, wqkv, wcq, wout, fc1, fc2,
                   xres, stage, stage0, pair, pair0, chips, chips0, full, qscr, oscr, knew, vnew,
                   small_sem, self_sem, cross_sem, w_sem, e_sem, send_sem, recv_sem):
    layers, batch, ctx, frames = dims
    me = lax.axis_index('tp')
    ko, vo = kvo.at[0], kvo.at[1]
    hb = batch // HALVES
    rows_per = 128

    def self_copy(layer, which):
        src, dst = ((sk_hbm, ko), (sv_hbm, vo))[which]
        return pltpu.make_async_copy(src.at[layer], dst.at[layer], self_sem.at[layer, which])

    def cross_copy(layer, which, octet):
        src, dst = ((ck_hbm, kbuf), (cv_hbm, vbuf))[which]
        at = pl.ds(pl.multiple_of(octet * 1024, 1024), 1024)
        return pltpu.make_async_copy(src.at[layer, at, :], dst.at[at, :], cross_sem.at[layer, which, octet])

    weights = ((wqkv_hbm, wqkv), (wout_hbm, wout), (wcq_hbm, wcq), (fc1_hbm, fc1), (fc2_hbm, fc2))

    def w_copy(which, layer):
        src, dst = weights[which]
        return pltpu.make_async_copy(src.at[layer], dst.at[layer], w_sem.at[which, layer])

    small = [pltpu.make_async_copy(src, dst, small_sem.at[i]) for i, (src, dst) in enumerate((
        (ln_layers_hbm, ln_layers), (in_bias_hbm, in_bias), (out_bias_hbm, out_bias), (b_fc1_hbm, b_fc1), (ln_final_hbm, ln_final)))]
    for c in small:
        c.start()
    e_rows = emb_hbm.shape[0] // 4

    def e_copy(i):
        at = pl.ds(i * e_rows, e_rows)
        return pltpu.make_async_copy(emb_hbm.at[at, :], eo.at[at, :], e_sem.at[i])

    pending = []

    def pump(n):
        for group in pending[:n]:
            for c in group:
                c.start()
        del pending[:n]

    for octet in range(batch // 8):
        for which in range(2):
            pending.append([cross_copy(0, which, octet)])
    pending.append([w_copy(3, 0), w_copy(4, 0)])
    pending.append([w_copy(0, 1), w_copy(1, 1), w_copy(2, 1)])
    pending.append([self_copy(1, 0)])
    pending.append([self_copy(1, 1)])
    for octet in range(batch // 8):
        for which in range(2):
            pending.append([cross_copy(1, which, octet)])
    pending.append([w_copy(3, 1), w_copy(4, 1)])
    for i in range(4):
        pending.append([e_copy(i)])

    w_copy(0, 0).start()
    self_copy(0, 0).start()
    self_copy(0, 1).start()
    w_copy(1, 0).start()
    w_copy(2, 0).start()

    barrier = pltpu.get_barrier_semaphore()
    for k in range(1, TP):
        pl.semaphore_signal(barrier, 1, device_id={'tp': lax.rem(me + k, TP)}, device_id_type=MESH)
    pl.semaphore_wait(barrier, TP - 1)

    core = lax.rem(me, 2)
    chip = me // 2
    partner = {'tp': 2 * chip + 1 - core}
    wide = posrow_ref.shape[1] // 2

    def bufs(ph, s):
        if ph == 0:
            return stage0.at[s], pair0.at[s], chips0.at[s], full.at[0, s]
        slot = ph % PARITY
        return stage.at[slot, s], pair.at[slot, s], chips.at[slot, s], full.at[slot, s]

    def send(src, dst, ph, s, step, device):
        pltpu.make_async_remote_copy(src, dst, send_sem.at[ph, s, step], recv_sem.at[ph, s, step], device_id=device, device_id_type=MESH).start()

    def wait_for(ref, sem):
        pltpu.make_async_copy(ref, ref, sem).wait()

    def sum_start(ph, s, value):
        mine, got, _, _ = bufs(ph, s)
        mine[0] = value[:, :wide]
        mine[1] = value[:, wide:]
        send(mine.at[1 - core], got, ph, s, 0, partner)

    def sum_chips(ph, s):
        mine, got, by_chip, _ = bufs(ph, s)
        wait_for(got, recv_sem.at[ph, s, 0])
        by_chip[chip] = mine[core] + got[...]
        for k in range(1, TP // 2):
            send(by_chip.at[chip], by_chip.at[chip], ph, s, 1, {'tp': 2 * lax.rem(chip + k, TP // 2) + core})
        wait_for(got, send_sem.at[ph, s, 0])

    def sum_share(ph, s):
        _, _, by_chip, both = bufs(ph, s)
        others = by_chip.at[pl.ds(0, TP // 2 - 1)]
        wait_for(others, recv_sem.at[ph, s, 1])
        total = by_chip[0].astype(F32)
        for q in range(1, TP // 2):
            total = total + by_chip[q].astype(F32)
        both[core] = total.astype(BF16)
        send(both.at[core], both.at[core], ph, s, 2, partner)
        wait_for(others, send_sem.at[ph, s, 1])

    def sum_finish(ph, s):
        both = bufs(ph, s)[3]
        wait_for(both.at[0], recv_sem.at[ph, s, 2])
        wait_for(both.at[0], send_sem.at[ph, s, 2])
        return jnp.concatenate([both[0].astype(F32), both[1].astype(F32)], axis=1)

    def head_bias(layer, which):
        b = in_bias[layer, which]
        return jnp.concatenate([b[0:1, :], b[1:2, :]], axis=1)

    def half(s):
        return pl.ds(s * hb, hb)

    def self_block(layer, s, early, late):
        hidden = norm_rows(xres[half(s), :], ln_layers[layer, 0])
        proj = lax.dot_general(hidden, wqkv[layer], NT, preferred_element_type=F32)
        qscr[half(s), :] = (proj[:, 0:128] + head_bias(layer, 0)).astype(BF16).astype(F32)
        knew[layer, half(s), :] = proj[:, 128:256].astype(BF16).astype(F32)
        vnew[layer, half(s), :] = (proj[:, 256:384] + head_bias(layer, 1)).astype(BF16).astype(F32)

        for i in range(hb // 8):
            octet = s * (hb // 8) + i
            r8 = pl.ds(octet * 8, 8)
            at = pl.ds(octet * 1024, 1024)
            both, qbd = block_diag(qscr[r8, :])
            seq = lax.rem(lax.broadcasted_iota(jnp.int32, (16, 1), 0), 8)
            limit = jnp.zeros((16, 1), jnp.int32)
            for b in range(8):
                limit = jnp.where(seq == b, pos_smem[octet * 8 + b], limit)
            past = jnp.dot(qbd, ko[layer, at, :], preferred_element_type=F32) * 0.125
            t = lax.broadcasted_iota(jnp.int32, (16, ctx), 1)
            past = jnp.where(t < limit, past, -1e30)
            kn = knew[layer, r8, :]
            vn = vnew[layer, r8, :]
            new = jnp.sum(both * jnp.concatenate([kn, kn], axis=0), axis=1, keepdims=True) * 0.125
            peak = jnp.maximum(jnp.max(past, axis=1, keepdims=True), new)
            past_e = jnp.exp(past - peak)
            new_e = jnp.exp(new - peak)
            denom = jnp.sum(past_e, axis=1, keepdims=True) + new_e
            past_w = (past_e / denom).astype(BF16)
            new_w = (new_e / denom).astype(BF16).astype(F32)
            o16 = lax.dot_general(past_w, vo[layer, at, :], NT, preferred_element_type=F32)
            lane = lax.broadcasted_iota(jnp.int32, (8, 128), 1)
            oscr[r8, :] = fold_heads(o16) + jnp.where(lane < 64, new_w[0:8], new_w[8:16]) * vn
        return jnp.dot(oscr[half(s), :].astype(BF16), wout[layer, 0], preferred_element_type=F32)

    def cross_block(layer, s, early, late):
        hidden = norm_rows(xres[half(s), :], ln_layers[layer, 1])
        proj = lax.dot_general(hidden, wcq[layer], NT, preferred_element_type=F32)
        qscr[half(s), :] = (proj + head_bias(layer, 2)).astype(BF16).astype(F32)

        octets = range(s * (hb // 8), (s + 1) * (hb // 8))
        for octet in octets:
            cross_copy(layer, 0, octet).wait()
        scores = []
        for octet in octets:
            _, qbd = block_diag(qscr[pl.ds(octet * 8, 8), :])
            scores.append(jnp.dot(qbd, kbuf[pl.ds(octet * 1024, 1024), :], preferred_element_type=F32) * 0.125)
        early()
        for octet in octets:
            cross_copy(layer, 1, octet).wait()
        for octet, sc in zip(octets, scores):
            exps = jnp.exp(sc - jnp.max(sc, axis=1, keepdims=True))
            w = (exps / jnp.sum(exps, axis=1, keepdims=True)).astype(BF16)
            if octet == octets[-1]:
                late()
            o16 = lax.dot_general(w, vbuf[pl.ds(octet * 1024, 1024), :], NT, preferred_element_type=F32)
            oscr[pl.ds(octet * 8, 8), :] = fold_heads(o16)
        return jnp.dot(oscr[half(s), :].astype(BF16), wout[layer, 1], preferred_element_type=F32)

    def mlp_block(layer, s, early, late):
        hidden = norm_rows(xres[half(s), :], ln_layers[layer, 2])
        pre = jnp.dot(hidden, fc1[layer], preferred_element_type=F32) + b_fc1[layer:layer + 1, :]
        active = (0.5 * pre * (1.0 + lax.erf(pre * (0.5 ** 0.5)))).astype(BF16)
        return jnp.dot(active, fc2[layer], preferred_element_type=F32)

    def write_new(layer, s):
        t = lax.broadcasted_iota(jnp.int32, (rows_per, ctx), 1)
        for new, cache in ((knew, ko), (vnew, vo)):
            cols = new[layer, half(s), :].T
            for i in range(hb):
                b = s * hb + i
                at = pl.ds(b * rows_per, rows_per)
                old = cache[layer, at, :].astype(F32)
                cache[layer, at, :] = jnp.where(t == pos_smem[b], cols[:, i:i + 1], old).astype(BF16)

    def nothing():
        pass

    def ready(nl, nk):
        if nk == 0:
            w_copy(0, nl).wait()
            self_copy(nl, 0).wait()
            self_copy(nl, 1).wait()
            w_copy(1, nl).wait()
        if nk == 1:
            w_copy(2, nl).wait()
        if nk == 2:
            w_copy(3, nl).wait()
            w_copy(4, nl).wait()

    for s in range(2):
        sum_start(0, s, picked_ref[half(s), :])
    pump(9)
    for s in range(2):
        sum_chips(0, s)
    for c in small:
        c.wait()
    for s in range(2):
        sum_share(0, s)
    for ph in range(3 * layers + 1):
        layer, kind = divmod(ph, 3)
        before, prev_kind = divmod(ph - 1, 3)

        def update(s):
            total = sum_finish(ph, s)
            if ph == 0:
                xres[half(s), :] = total + posrow_ref[half(s), :]
            else:
                xres[half(s), :] = xres[half(s), :] + total + out_bias[prev_kind, before:before + 1, :]

        if ph == 3 * layers:
            sum_share(ph, 1)
            for s in range(2):
                update(s)
                fh_ref[half(s), :] = norm_rows(xres[half(s), :], ln_final)
            break
        block = (self_block, cross_block, mlp_block)[kind]
        update(0)
        ready(layer, kind)
        share = functools.partial(sum_share, ph, 1)
        gather = functools.partial(sum_chips, ph + 1, 0)
        if kind == 1:
            sum_start(ph + 1, 0, block(layer, 0, nothing, share))
            update(1)
            sum_start(ph + 1, 1, block(layer, 1, gather, nothing))
        else:
            sum_start(ph + 1, 0, block(layer, 0, nothing, nothing))
            if kind == 2:
                write_new(layer, 0)
                gather()
                write_new(layer, 1)
                share()
            else:
                if ph > 0:
                    share()
                gather()
            if ph == 0:
                pump(3)
            if ph == 2:
                pump(4)
            update(1)
            sum_start(ph + 1, 1, block(layer, 1, nothing, nothing))
        sum_chips(ph + 1, 1)
        if ph == 1:
            pump(9)
        sum_share(ph + 1, 0)
    for i in range(4):
        e_copy(i).wait()


def final_kernel(kv_ref, e_ref, fh_ref, logits_hbm, ko_hbm, vo_hbm, logits, sem, out_sem):
    layers, rows = kv_ref.shape[1:3]
    copies = []
    for layer in range(layers):
        for which, dst in enumerate((ko_hbm, vo_hbm)):
            for part in range(4):
                at = pl.ds(part * (rows // 4), rows // 4)
                c = pltpu.make_async_copy(kv_ref.at[which, layer, at, :], dst.at[layer, at, :], sem.at[layer, which, part])
                c.start()
                copies.append(c)
    fh = fh_ref[...]
    step = 384
    n = e_ref.shape[0] // step

    def out_copy(i):
        at = pl.ds(pl.multiple_of(i * step, step), step)
        return pltpu.make_async_copy(logits.at[:, at], logits_hbm.at[:, at], out_sem)

    def body(i, carry):
        at = pl.ds(pl.multiple_of(i * step, step), step)
        logits[:, at] = lax.dot_general(fh, e_ref[at, :], NT, preferred_element_type=F32)
        out_copy(i).start()
        return carry

    lax.fori_loop(0, n, body, 0)
    pltpu.make_async_copy(logits, logits_hbm, out_sem).wait()
    for c in copies:
        c.wait()


def solution(mesh):
    vm = pl.BlockSpec(memory_space=pltpu.VMEM)
    sm = pl.BlockSpec(memory_space=pltpu.SMEM)
    hbm = pl.BlockSpec(memory_space=pltpu.HBM)

    def local_step(tokens, positions, self_keys, self_vals, cross_keys, cross_vals, embed_table, pos_table, w_qkv, w_cq, in_bias, w_out, out_bias, w_fc1, b_fc1, w_fc2, ln_layers, ln_final):
        batch = tokens.shape[0]
        layers, _, ctx, heads, hd = self_keys.shape
        frames = cross_keys.shape[2]
        vocab, d = embed_table.shape
        ff = w_fc1.shape[2]
        rows = batch * heads * hd
        hb = batch // HALVES

        def flat(cache):
            return cache.transpose(0, 1, 3, 4, 2).reshape(layers, rows, cache.shape[2])

        picked, posrow = pl.pallas_call(
            gather_kernel,
            out_shape=(pltpu.VMEM((batch, d), BF16), pltpu.VMEM((batch, d), F32)),
            in_specs=[sm, sm, vm, vm, hbm, hbm], out_specs=(vm, vm),
            scratch_shapes=[pltpu.VMEM((16 * batch, d), BF16), pltpu.VMEM((16 * batch, d), BF16), pltpu.SemaphoreType.DMA((2,))],
            compiler_params=pltpu.CompilerParams(vmem_limit_bytes=60 * 2 ** 20),
            name='gather_rows',
        )(tokens, positions, tokens.reshape(1, batch), positions.reshape(1, batch), embed_table, pos_table)

        picked, posrow = (pltpu.with_memory_space_constraint(a, pltpu.VMEM) for a in (picked, posrow))
        kvo, eo, fh = pl.pallas_call(
            functools.partial(decoder_kernel, (layers, batch, ctx, frames)),
            out_shape=(pltpu.VMEM((2, layers, rows, ctx), BF16), pltpu.VMEM((vocab, d), BF16), pltpu.VMEM((batch, d), BF16)),
            in_specs=[sm] + [vm] * 2 + [hbm] * 15,
            out_specs=(vm, vm, vm),
            scratch_shapes=[
                pltpu.VMEM(in_bias.shape, F32), pltpu.VMEM((3, layers, d), F32), pltpu.VMEM(b_fc1.shape, F32), pltpu.VMEM(ln_layers.shape, F32), pltpu.VMEM(ln_final.shape, F32),
                pltpu.VMEM((rows, frames), BF16), pltpu.VMEM((rows, frames), BF16),
                pltpu.VMEM((layers, 3 * heads * hd, d), BF16), pltpu.VMEM((layers, heads * hd, d), BF16),
                pltpu.VMEM((layers, 2, heads * hd, d), BF16), pltpu.VMEM((layers, d, ff), BF16), pltpu.VMEM((layers, ff, d), BF16),
                pltpu.VMEM((batch, d), F32),
                pltpu.VMEM((PARITY, HALVES, 2, hb, d // 2), F32), pltpu.VMEM((HALVES, 2, hb, d // 2), BF16),
                pltpu.VMEM((PARITY, HALVES, hb, d // 2), F32), pltpu.VMEM((HALVES, hb, d // 2), BF16),
                pltpu.VMEM((PARITY, HALVES, TP // 2, hb, d // 2), F32), pltpu.VMEM((HALVES, TP // 2, hb, d // 2), BF16),
                pltpu.VMEM((PARITY, HALVES, 2, hb, d // 2), BF16),
                pltpu.VMEM((batch, 128), F32), pltpu.VMEM((batch, 128), F32),
                pltpu.VMEM((layers, batch, 128), F32), pltpu.VMEM((layers, batch, 128), F32),
                pltpu.SemaphoreType.DMA((5,)), pltpu.SemaphoreType.DMA((layers, 2)), pltpu.SemaphoreType.DMA((layers, 2, batch // 8)),
                pltpu.SemaphoreType.DMA((5, layers)), pltpu.SemaphoreType.DMA((4,)),
                pltpu.SemaphoreType.DMA((3 * layers + 1, HALVES, 3)), pltpu.SemaphoreType.DMA((3 * layers + 1, HALVES, 3)),
            ],
            compiler_params=pltpu.CompilerParams(collective_id=0, has_side_effects=True, vmem_limit_bytes=139 * 2 ** 18),
            name='decoder_layers',
        )(positions, picked, posrow, in_bias, out_bias.transpose(1, 0, 2), b_fc1, ln_layers, ln_final,
          flat(self_keys), flat(self_vals), flat(cross_keys), flat(cross_vals), embed_table,
          w_qkv.transpose(0, 2, 3, 4, 1).reshape(layers, 3 * heads * hd, d), w_cq.transpose(0, 2, 3, 1).reshape(layers, heads * hd, d),
          w_out.reshape(layers, 2, heads * hd, d), w_fc1, w_fc2)

        logits, nk, nv = pl.pallas_call(
            final_kernel,
            out_shape=(jax.ShapeDtypeStruct((batch, vocab), F32), jax.ShapeDtypeStruct((layers, rows, ctx), BF16), jax.ShapeDtypeStruct((layers, rows, ctx), BF16)),
            in_specs=[vm] * 3, out_specs=(hbm, hbm, hbm),
            scratch_shapes=[pltpu.VMEM((batch, vocab), F32), pltpu.SemaphoreType.DMA((layers, 2, 4)), pltpu.SemaphoreType.DMA],
            compiler_params=pltpu.CompilerParams(vmem_limit_bytes=2 * 2 ** 20),
            name='final_logits',
        )(kvo, eo, fh)

        def unflat(cache):
            return cache.reshape(layers, batch, heads, hd, ctx).transpose(0, 1, 4, 2, 3)

        return logits, unflat(nk), unflat(nv)

    batch_spec = P('dp')
    cache_spec = P(None, 'dp', None, 'tp', None)
    in_specs = (batch_spec, batch_spec, cache_spec, cache_spec, cache_spec, cache_spec, P('tp', None), P(None, None), P(None, None, None, 'tp', None), P(None, None, 'tp', None), P(None, None, 'tp', None), P(None, None, 'tp', None, None), P(None, None, None), P(None, None, 'tp'), P(None, 'tp'), P(None, 'tp', None), P(None, None, None, None), P(None, None))
    out_specs = (P('dp', 'tp'), cache_spec, cache_spec)
    return jax.shard_map(local_step, mesh=mesh, in_specs=in_specs, out_specs=out_specs, check_vma=False)
```

```python
import functools
import jax
import jax.numpy as jnp
from jax import lax
from jax.experimental import pallas as pl
from jax.experimental.pallas import tpu as pltpu
from jax.sharding import PartitionSpec as P

MESH = pl.DeviceIdType.MESH
F32 = jnp.float32
BF16 = jnp.bfloat16
NT = (((1,), (1,)), ((), ()))
TN = (((0,), (0,)), ((), ()))
TP = 8
HALVES = 2
PARITY = 2


def gather_kernel(tok_ref, pos_ref, tokv_ref, posv_ref, emb_hbm, pos_hbm, picked_ref, posrow_ref, ebuf, pbuf, sem):
    shard_rows = emb_hbm.shape[0]
    n = tok_ref.shape[0]
    base = lax.axis_index('tp') * shard_rows

    def start(b, carry):
        tid = jnp.clip(tok_ref[b] - base, 0, shard_rows - 1)
        pid = pos_ref[b]
        at = pl.ds(pl.multiple_of(b * 16, 16), 16)
        pltpu.make_async_copy(emb_hbm.at[pl.ds(pl.multiple_of(tid // 16 * 16, 16), 16), :], ebuf.at[at, :], sem.at[0]).start()
        pltpu.make_async_copy(pos_hbm.at[pl.ds(pl.multiple_of(pid // 16 * 16, 16), 16), :], pbuf.at[at, :], sem.at[1]).start()
        return carry

    lax.fori_loop(0, n, start, 0, unroll=4)
    tid = tokv_ref[...] - base
    owned = (tid >= 0) & (tid < shard_rows)
    lane16 = lax.broadcasted_iota(jnp.int32, (1, n), 1) * 16
    tok_row = jnp.where(owned, lane16 + jnp.clip(tid, 0, shard_rows - 1) % 16, -1)
    pos_row = lane16 + posv_ref[...] % 16
    row = lax.broadcasted_iota(jnp.int32, (16 * n, n), 0)
    tok_hot = jnp.where(row == tok_row, 1.0, 0.0).astype(BF16)
    pos_hot = jnp.where(row == pos_row, 1.0, 0.0).astype(BF16)
    pltpu.make_async_copy(ebuf, ebuf, sem.at[0]).wait()
    picked_ref[...] = lax.dot_general(tok_hot, ebuf[...], TN, preferred_element_type=F32).astype(BF16)
    pltpu.make_async_copy(pbuf, pbuf, sem.at[1]).wait()
    posrow_ref[...] = lax.dot_general(pos_hot, pbuf[...], TN, preferred_element_type=F32)


def norm_rows(x, ln):
    mean = jnp.mean(x, axis=-1, keepdims=True)
    centred = x - mean
    var = jnp.mean(centred * centred, axis=-1, keepdims=True)
    return (centred * lax.rsqrt(var + 1e-5) * ln[0:1, :] + ln[1:2, :]).astype(BF16)


def block_diag(q8):
    lane = lax.broadcasted_iota(jnp.int32, (8, 128), 1)
    qf = q8.astype(F32)
    both = jnp.concatenate([jnp.where(lane < 64, qf, 0.0), jnp.where(lane < 64, 0.0, qf)], axis=0)
    row = lax.rem(lax.broadcasted_iota(jnp.int32, (16, 128), 0), 8)
    blocks = [jnp.where(row == b, both, 0.0).astype(BF16) for b in range(8)]
    return both, jnp.concatenate(blocks, axis=1)


def fold_heads(o16):
    lane = lax.broadcasted_iota(jnp.int32, (8, 128), 1)
    row = lax.broadcasted_iota(jnp.int32, (8, 128), 0)
    out = jnp.zeros((8, 128), F32)
    for b in range(8):
        blk = jnp.where(lane < 64, o16[0:8, b * 128:(b + 1) * 128], o16[8:16, b * 128:(b + 1) * 128])
        out = jnp.where(row == b, blk, out)
    return out


def decoder_kernel(dims, pos_smem, picked_ref, posrow_ref, in_bias_hbm, out_bias_hbm, b_fc1_hbm, ln_layers_hbm, ln_final_hbm,
                   sk_hbm, sv_hbm, ck_hbm, cv_hbm, emb_hbm, wqkv_hbm, wcq_hbm, wout_hbm, fc1_hbm, fc2_hbm,
                   kvo, eo, fh_ref,
                   in_bias, out_bias, b_fc1, ln_layers, ln_final, kbuf, vbuf, wqkv, wcq, wout, fc1, fc2,
                   xres, stage, stage0, pair, pair0, chips, chips0, full, qscr, oscr, knew, vnew,
                   small_sem, self_sem, cross_sem, w_sem, e_sem, send_sem, recv_sem):
    layers, batch, ctx, frames = dims
    me = lax.axis_index('tp')
    ko, vo = kvo.at[0], kvo.at[1]
    hb = batch // HALVES
    rows_per = 128

    def self_copy(layer, which):
        src, dst = ((sk_hbm, ko), (sv_hbm, vo))[which]
        return pltpu.make_async_copy(src.at[layer], dst.at[layer], self_sem.at[layer, which])

    def cross_copy(layer, which, octet):
        src, dst = ((ck_hbm, kbuf), (cv_hbm, vbuf))[which]
        at = pl.ds(pl.multiple_of(octet * 1024, 1024), 1024)
        return pltpu.make_async_copy(src.at[layer, at, :], dst.at[at, :], cross_sem.at[layer, which, octet])

    weights = ((wqkv_hbm, wqkv), (wout_hbm, wout), (wcq_hbm, wcq), (fc1_hbm, fc1), (fc2_hbm, fc2))

    def w_copy(which, layer):
        src, dst = weights[which]
        return pltpu.make_async_copy(src.at[layer], dst.at[layer], w_sem.at[which, layer])

    small = [pltpu.make_async_copy(src, dst, small_sem.at[i]) for i, (src, dst) in enumerate((
        (ln_layers_hbm, ln_layers), (in_bias_hbm, in_bias), (out_bias_hbm, out_bias), (b_fc1_hbm, b_fc1), (ln_final_hbm, ln_final)))]
    for c in small:
        c.start()
    e_rows = emb_hbm.shape[0] // 4

    def e_copy(i):
        at = pl.ds(i * e_rows, e_rows)
        return pltpu.make_async_copy(emb_hbm.at[at, :], eo.at[at, :], e_sem.at[i])

    pending = []

    def pump(n):
        for group in pending[:n]:
            for c in group:
                c.start()
        del pending[:n]

    for octet in range(batch // 8):
        for which in range(2):
            pending.append([cross_copy(0, which, octet)])
    pending.append([w_copy(3, 0), w_copy(4, 0)])
    pending.append([w_copy(0, 1), w_copy(1, 1), w_copy(2, 1)])
    pending.append([self_copy(1, 0)])
    pending.append([self_copy(1, 1)])
    for octet in range(batch // 8):
        for which in range(2):
            pending.append([cross_copy(1, which, octet)])
    pending.append([w_copy(3, 1), w_copy(4, 1)])
    for i in range(4):
        pending.append([e_copy(i)])

    w_copy(0, 0).start()
    self_copy(0, 0).start()
    self_copy(0, 1).start()
    w_copy(1, 0).start()
    w_copy(2, 0).start()

    barrier = pltpu.get_barrier_semaphore()
    for k in range(1, TP):
        pl.semaphore_signal(barrier, 1, device_id={'tp': lax.rem(me + k, TP)}, device_id_type=MESH)
    pl.semaphore_wait(barrier, TP - 1)

    core = lax.rem(me, 2)
    chip = me // 2
    partner = {'tp': 2 * chip + 1 - core}
    wide = posrow_ref.shape[1] // 2

    def bufs(ph, s):
        if ph == 0:
            return stage0.at[s], pair0.at[s], chips0.at[s], full.at[0, s]
        slot = ph % PARITY
        return stage.at[slot, s], pair.at[slot, s], chips.at[slot, s], full.at[slot, s]

    def send(src, dst, ph, s, step, device):
        pltpu.make_async_remote_copy(src, dst, send_sem.at[ph, s, step], recv_sem.at[ph, s, step], device_id=device, device_id_type=MESH).start()

    def wait_for(ref, sem):
        pltpu.make_async_copy(ref, ref, sem).wait()

    def columns(which):
        return pl.ds(pl.multiple_of(which * wide, 128), wide)

    def sum_start(ph, s, operands):
        mine, got, _, _ = bufs(ph, s)
        lhs, weight = operands
        mine[1] = jnp.dot(lhs, weight[:, columns(1 - core)], preferred_element_type=F32)
        send(mine.at[1], got, ph, s, 0, partner)
        mine[0] = jnp.dot(lhs, weight[:, columns(core)], preferred_element_type=F32)

    def sum_chips(ph, s):
        mine, got, by_chip, _ = bufs(ph, s)
        wait_for(got, recv_sem.at[ph, s, 0])
        by_chip[chip] = mine[0] + got[...]
        for k in range(1, TP // 2):
            send(by_chip.at[chip], by_chip.at[chip], ph, s, 1, {'tp': 2 * lax.rem(chip + k, TP // 2) + core})
        wait_for(got, send_sem.at[ph, s, 0])

    def sum_share(ph, s):
        _, _, by_chip, both = bufs(ph, s)
        others = by_chip.at[pl.ds(0, TP // 2 - 1)]
        wait_for(others, recv_sem.at[ph, s, 1])
        total = by_chip[0].astype(F32)
        for q in range(1, TP // 2):
            total = total + by_chip[q].astype(F32)
        both[core] = total.astype(BF16)
        send(both.at[core], both.at[core], ph, s, 2, partner)
        wait_for(others, send_sem.at[ph, s, 1])

    def sum_finish(ph, s):
        both = bufs(ph, s)[3]
        wait_for(both.at[0], recv_sem.at[ph, s, 2])
        wait_for(both.at[0], send_sem.at[ph, s, 2])
        return jnp.concatenate([both[0].astype(F32), both[1].astype(F32)], axis=1)

    def head_bias(layer, which):
        b = in_bias[layer, which]
        return jnp.concatenate([b[0:1, :], b[1:2, :]], axis=1)

    def half(s):
        return pl.ds(s * hb, hb)

    def self_block(layer, s, early, late):
        hidden = norm_rows(xres[half(s), :], ln_layers[layer, 0])
        proj = lax.dot_general(hidden, wqkv[layer], NT, preferred_element_type=F32)
        qscr[half(s), :] = (proj[:, 0:128] + head_bias(layer, 0)).astype(BF16).astype(F32)
        knew[layer, half(s), :] = proj[:, 128:256].astype(BF16).astype(F32)
        vnew[layer, half(s), :] = (proj[:, 256:384] + head_bias(layer, 1)).astype(BF16).astype(F32)

        for i in range(hb // 8):
            octet = s * (hb // 8) + i
            r8 = pl.ds(octet * 8, 8)
            at = pl.ds(octet * 1024, 1024)
            both, qbd = block_diag(qscr[r8, :])
            seq = lax.rem(lax.broadcasted_iota(jnp.int32, (16, 1), 0), 8)
            limit = jnp.zeros((16, 1), jnp.int32)
            for b in range(8):
                limit = jnp.where(seq == b, pos_smem[octet * 8 + b], limit)
            past = jnp.dot(qbd, ko[layer, at, :], preferred_element_type=F32) * 0.125
            t = lax.broadcasted_iota(jnp.int32, (16, ctx), 1)
            past = jnp.where(t < limit, past, -1e30)
            kn = knew[layer, r8, :]
            vn = vnew[layer, r8, :]
            new = jnp.sum(both * jnp.concatenate([kn, kn], axis=0), axis=1, keepdims=True) * 0.125
            peak = jnp.maximum(jnp.max(past, axis=1, keepdims=True), new)
            past_e = jnp.exp(past - peak)
            new_e = jnp.exp(new - peak)
            denom = jnp.sum(past_e, axis=1, keepdims=True) + new_e
            past_w = (past_e / denom).astype(BF16)
            new_w = (new_e / denom).astype(BF16).astype(F32)
            o16 = lax.dot_general(past_w, vo[layer, at, :], NT, preferred_element_type=F32)
            lane = lax.broadcasted_iota(jnp.int32, (8, 128), 1)
            oscr[r8, :] = fold_heads(o16) + jnp.where(lane < 64, new_w[0:8], new_w[8:16]) * vn
        return oscr[half(s), :].astype(BF16), wout.at[layer, 0]

    def cross_block(layer, s, early, late):
        hidden = norm_rows(xres[half(s), :], ln_layers[layer, 1])
        proj = lax.dot_general(hidden, wcq[layer], NT, preferred_element_type=F32)
        qscr[half(s), :] = (proj + head_bias(layer, 2)).astype(BF16).astype(F32)

        octets = range(s * (hb // 8), (s + 1) * (hb // 8))
        for octet in octets:
            cross_copy(layer, 0, octet).wait()
        scores = []
        for octet in octets:
            _, qbd = block_diag(qscr[pl.ds(octet * 8, 8), :])
            scores.append(jnp.dot(qbd, kbuf[pl.ds(octet * 1024, 1024), :], preferred_element_type=F32) * 0.125)
        early()
        for octet in octets:
            cross_copy(layer, 1, octet).wait()
        for octet, sc in zip(octets, scores):
            exps = jnp.exp(sc - jnp.max(sc, axis=1, keepdims=True))
            w = (exps * (1.0 / jnp.sum(exps, axis=1, keepdims=True))).astype(BF16)
            if octet == octets[-1]:
                late()
            o16 = lax.dot_general(w, vbuf[pl.ds(octet * 1024, 1024), :], NT, preferred_element_type=F32)
            oscr[pl.ds(octet * 8, 8), :] = fold_heads(o16)
        return oscr[half(s), :].astype(BF16), wout.at[layer, 1]

    def mlp_block(layer, s, early, late):
        hidden = norm_rows(xres[half(s), :], ln_layers[layer, 2])
        pre = jnp.dot(hidden, fc1[layer], preferred_element_type=F32) + b_fc1[layer:layer + 1, :]
        active = (0.5 * pre * (1.0 + lax.erf(pre * (0.5 ** 0.5)))).astype(BF16)
        return active, fc2.at[layer]

    def write_new(layer, s):
        t = lax.broadcasted_iota(jnp.int32, (rows_per, ctx), 1)
        for new, cache in ((knew, ko), (vnew, vo)):
            cols = new[layer, half(s), :].T
            for i in range(hb):
                b = s * hb + i
                at = pl.ds(b * rows_per, rows_per)
                old = cache[layer, at, :].astype(F32)
                cache[layer, at, :] = jnp.where(t == pos_smem[b], cols[:, i:i + 1], old).astype(BF16)

    def nothing():
        pass

    def ready(nl, nk):
        if nk == 0:
            w_copy(0, nl).wait()
            self_copy(nl, 0).wait()
            self_copy(nl, 1).wait()
            w_copy(1, nl).wait()
        if nk == 1:
            w_copy(2, nl).wait()
        if nk == 2:
            w_copy(3, nl).wait()
            w_copy(4, nl).wait()

    for s in range(2):
        mine, got = stage0.at[s], pair0.at[s]
        mine[0] = picked_ref[half(s), columns(core)]
        mine[1] = picked_ref[half(s), columns(1 - core)]
        send(mine.at[1], got, 0, s, 0, partner)
    pump(9)
    for s in range(2):
        sum_chips(0, s)
    for c in small:
        c.wait()
    for s in range(2):
        sum_share(0, s)
    for ph in range(3 * layers + 1):
        layer, kind = divmod(ph, 3)
        before, prev_kind = divmod(ph - 1, 3)

        def update(s):
            total = sum_finish(ph, s)
            if ph == 0:
                xres[half(s), :] = total + posrow_ref[half(s), :]
            else:
                xres[half(s), :] = xres[half(s), :] + total + out_bias[prev_kind, before:before + 1, :]

        if ph == 3 * layers:
            sum_share(ph, 1)
            for s in range(2):
                update(s)
                fh_ref[half(s), :] = norm_rows(xres[half(s), :], ln_final)
            break
        block = (self_block, cross_block, mlp_block)[kind]
        update(0)
        ready(layer, kind)
        share = functools.partial(sum_share, ph, 1)
        gather = functools.partial(sum_chips, ph + 1, 0)
        if kind == 1:
            sum_start(ph + 1, 0, block(layer, 0, nothing, share))
            update(1)
            sum_start(ph + 1, 1, block(layer, 1, gather, nothing))
        else:
            sum_start(ph + 1, 0, block(layer, 0, nothing, nothing))
            if kind == 2:
                write_new(layer, 0)
                gather()
                share()
                write_new(layer, 1)
            else:
                if ph > 0:
                    share()
                gather()
            if ph == 0:
                pump(3)
            if ph == 2:
                pump(4)
            update(1)
            sum_start(ph + 1, 1, block(layer, 1, nothing, nothing))
        sum_chips(ph + 1, 1)
        if ph == 1:
            pump(9)
        sum_share(ph + 1, 0)
    for i in range(4):
        e_copy(i).wait()


def final_kernel(kv_ref, e_ref, fh_ref, logits_hbm, ko_hbm, vo_hbm, logits, sem, out_sem):
    layers, rows = kv_ref.shape[1:3]
    copies = []
    for layer in range(layers):
        for which, dst in enumerate((ko_hbm, vo_hbm)):
            for part in range(4):
                at = pl.ds(part * (rows // 4), rows // 4)
                c = pltpu.make_async_copy(kv_ref.at[which, layer, at, :], dst.at[layer, at, :], sem.at[layer, which, part])
                c.start()
                copies.append(c)
    fh = fh_ref[...]
    step = 384
    n = e_ref.shape[0] // step

    def out_copy(i):
        at = pl.ds(pl.multiple_of(i * step, step), step)
        return pltpu.make_async_copy(logits.at[:, at], logits_hbm.at[:, at], out_sem)

    def body(i, carry):
        at = pl.ds(pl.multiple_of(i * step, step), step)
        logits[:, at] = lax.dot_general(fh, e_ref[at, :], NT, preferred_element_type=F32)
        out_copy(i).start()
        return carry

    lax.fori_loop(0, n, body, 0)
    pltpu.make_async_copy(logits, logits_hbm, out_sem).wait()
    for c in copies:
        c.wait()


def solution(mesh):
    vm = pl.BlockSpec(memory_space=pltpu.VMEM)
    sm = pl.BlockSpec(memory_space=pltpu.SMEM)
    hbm = pl.BlockSpec(memory_space=pltpu.HBM)

    def local_step(tokens, positions, self_keys, self_vals, cross_keys, cross_vals, embed_table, pos_table, w_qkv, w_cq, in_bias, w_out, out_bias, w_fc1, b_fc1, w_fc2, ln_layers, ln_final):
        batch = tokens.shape[0]
        layers, _, ctx, heads, hd = self_keys.shape
        frames = cross_keys.shape[2]
        vocab, d = embed_table.shape
        ff = w_fc1.shape[2]
        rows = batch * heads * hd
        hb = batch // HALVES

        def flat(cache):
            return cache.transpose(0, 1, 3, 4, 2).reshape(layers, rows, cache.shape[2])

        picked, posrow = pl.pallas_call(
            gather_kernel,
            out_shape=(pltpu.VMEM((batch, d), BF16), pltpu.VMEM((batch, d), F32)),
            in_specs=[sm, sm, vm, vm, hbm, hbm], out_specs=(vm, vm),
            scratch_shapes=[pltpu.VMEM((16 * batch, d), BF16), pltpu.VMEM((16 * batch, d), BF16), pltpu.SemaphoreType.DMA((2,))],
            compiler_params=pltpu.CompilerParams(vmem_limit_bytes=60 * 2 ** 20),
            name='gather_rows',
        )(tokens, positions, tokens.reshape(1, batch), positions.reshape(1, batch), embed_table, pos_table)

        picked, posrow = (pltpu.with_memory_space_constraint(a, pltpu.VMEM) for a in (picked, posrow))
        kvo, eo, fh = pl.pallas_call(
            functools.partial(decoder_kernel, (layers, batch, ctx, frames)),
            out_shape=(pltpu.VMEM((2, layers, rows, ctx), BF16), pltpu.VMEM((vocab, d), BF16), pltpu.VMEM((batch, d), BF16)),
            in_specs=[sm] + [vm] * 2 + [hbm] * 15,
            out_specs=(vm, vm, vm),
            scratch_shapes=[
                pltpu.VMEM(in_bias.shape, F32), pltpu.VMEM((3, layers, d), F32), pltpu.VMEM(b_fc1.shape, F32), pltpu.VMEM(ln_layers.shape, F32), pltpu.VMEM(ln_final.shape, F32),
                pltpu.VMEM((rows, frames), BF16), pltpu.VMEM((rows, frames), BF16),
                pltpu.VMEM((layers, 3 * heads * hd, d), BF16), pltpu.VMEM((layers, heads * hd, d), BF16),
                pltpu.VMEM((layers, 2, heads * hd, d), BF16), pltpu.VMEM((layers, d, ff), BF16), pltpu.VMEM((layers, ff, d), BF16),
                pltpu.VMEM((batch, d), F32),
                pltpu.VMEM((PARITY, HALVES, 2, hb, d // 2), F32), pltpu.VMEM((HALVES, 2, hb, d // 2), BF16),
                pltpu.VMEM((PARITY, HALVES, hb, d // 2), F32), pltpu.VMEM((HALVES, hb, d // 2), BF16),
                pltpu.VMEM((PARITY, HALVES, TP // 2, hb, d // 2), F32), pltpu.VMEM((HALVES, TP // 2, hb, d // 2), BF16),
                pltpu.VMEM((PARITY, HALVES, 2, hb, d // 2), BF16),
                pltpu.VMEM((batch, 128), F32), pltpu.VMEM((batch, 128), F32),
                pltpu.VMEM((layers, batch, 128), F32), pltpu.VMEM((layers, batch, 128), F32),
                pltpu.SemaphoreType.DMA((5,)), pltpu.SemaphoreType.DMA((layers, 2)), pltpu.SemaphoreType.DMA((layers, 2, batch // 8)),
                pltpu.SemaphoreType.DMA((5, layers)), pltpu.SemaphoreType.DMA((4,)),
                pltpu.SemaphoreType.DMA((3 * layers + 1, HALVES, 3)), pltpu.SemaphoreType.DMA((3 * layers + 1, HALVES, 3)),
            ],
            compiler_params=pltpu.CompilerParams(collective_id=0, has_side_effects=True, vmem_limit_bytes=139 * 2 ** 18),
            name='decoder_layers',
        )(positions, picked, posrow, in_bias, out_bias.transpose(1, 0, 2), b_fc1, ln_layers, ln_final,
          flat(self_keys), flat(self_vals), flat(cross_keys), flat(cross_vals), embed_table,
          w_qkv.transpose(0, 2, 3, 4, 1).reshape(layers, 3 * heads * hd, d), w_cq.transpose(0, 2, 3, 1).reshape(layers, heads * hd, d),
          w_out.reshape(layers, 2, heads * hd, d), w_fc1, w_fc2)

        logits, nk, nv = pl.pallas_call(
            final_kernel,
            out_shape=(jax.ShapeDtypeStruct((batch, vocab), F32), jax.ShapeDtypeStruct((layers, rows, ctx), BF16), jax.ShapeDtypeStruct((layers, rows, ctx), BF16)),
            in_specs=[vm] * 3, out_specs=(hbm, hbm, hbm),
            scratch_shapes=[pltpu.VMEM((batch, vocab), F32), pltpu.SemaphoreType.DMA((layers, 2, 4)), pltpu.SemaphoreType.DMA],
            compiler_params=pltpu.CompilerParams(vmem_limit_bytes=2 * 2 ** 20),
            name='final_logits',
        )(kvo, eo, fh)

        def unflat(cache):
            return cache.reshape(layers, batch, heads, hd, ctx).transpose(0, 1, 4, 2, 3)

        return logits, unflat(nk), unflat(nv)

    batch_spec = P('dp')
    cache_spec = P(None, 'dp', None, 'tp', None)
    in_specs = (batch_spec, batch_spec, cache_spec, cache_spec, cache_spec, cache_spec, P('tp', None), P(None, None), P(None, None, None, 'tp', None), P(None, None, 'tp', None), P(None, None, 'tp', None), P(None, None, 'tp', None, None), P(None, None, None), P(None, None, 'tp'), P(None, 'tp'), P(None, 'tp', None), P(None, None, None, None), P(None, None))
    out_specs = (P('dp', 'tp'), cache_spec, cache_spec)
    return jax.shard_map(local_step, mesh=mesh, in_specs=in_specs, out_specs=out_specs, check_vma=False)
```

```python
import functools
import jax
import jax.numpy as jnp
from jax import lax
from jax.experimental import pallas as pl
from jax.experimental.pallas import tpu as pltpu
from jax.sharding import PartitionSpec as P

MESH = pl.DeviceIdType.MESH
F32 = jnp.float32
BF16 = jnp.bfloat16
NT = (((1,), (1,)), ((), ()))
TN = (((0,), (0,)), ((), ()))
TP = 8
HALVES = 2
PARITY = 2


def gather_kernel(tok_ref, pos_ref, tokv_ref, posv_ref, emb_hbm, pos_hbm, picked_ref, posrow_ref, ebuf, pbuf, sem):
    shard_rows = emb_hbm.shape[0]
    n = tok_ref.shape[0]
    base = lax.axis_index('tp') * shard_rows

    def start(b, carry):
        tid = jnp.clip(tok_ref[b] - base, 0, shard_rows - 1)
        pid = pos_ref[b]
        at = pl.ds(pl.multiple_of(b * 16, 16), 16)
        pltpu.make_async_copy(emb_hbm.at[pl.ds(pl.multiple_of(tid // 16 * 16, 16), 16), :], ebuf.at[at, :], sem.at[0]).start()
        pltpu.make_async_copy(pos_hbm.at[pl.ds(pl.multiple_of(pid // 16 * 16, 16), 16), :], pbuf.at[at, :], sem.at[1]).start()
        return carry

    lax.fori_loop(0, n, start, 0, unroll=4)
    tid = tokv_ref[...] - base
    owned = (tid >= 0) & (tid < shard_rows)
    lane16 = lax.broadcasted_iota(jnp.int32, (1, n), 1) * 16
    tok_row = jnp.where(owned, lane16 + jnp.clip(tid, 0, shard_rows - 1) % 16, -1)
    pos_row = lane16 + posv_ref[...] % 16
    row = lax.broadcasted_iota(jnp.int32, (16 * n, n), 0)
    tok_hot = jnp.where(row == tok_row, 1.0, 0.0).astype(BF16)
    pos_hot = jnp.where(row == pos_row, 1.0, 0.0).astype(BF16)
    pltpu.make_async_copy(ebuf, ebuf, sem.at[0]).wait()
    picked_ref[...] = lax.dot_general(tok_hot, ebuf[...], TN, preferred_element_type=F32).astype(BF16)
    pltpu.make_async_copy(pbuf, pbuf, sem.at[1]).wait()
    posrow_ref[...] = lax.dot_general(pos_hot, pbuf[...], TN, preferred_element_type=F32)


def norm_rows(x, ln):
    mean = jnp.mean(x, axis=-1, keepdims=True)
    centred = x - mean
    var = jnp.mean(centred * centred, axis=-1, keepdims=True)
    return (centred * lax.rsqrt(var + 1e-5) * ln[0:1, :] + ln[1:2, :]).astype(BF16)


def block_diag(q8):
    lane = lax.broadcasted_iota(jnp.int32, (8, 128), 1)
    qf = q8.astype(F32)
    both = jnp.concatenate([jnp.where(lane < 64, qf, 0.0), jnp.where(lane < 64, 0.0, qf)], axis=0)
    row = lax.rem(lax.broadcasted_iota(jnp.int32, (16, 128), 0), 8)
    blocks = [jnp.where(row == b, both, 0.0).astype(BF16) for b in range(8)]
    return both, jnp.concatenate(blocks, axis=1)


def fold_heads(o16):
    lane = lax.broadcasted_iota(jnp.int32, (8, 128), 1)
    row = lax.broadcasted_iota(jnp.int32, (8, 128), 0)
    out = jnp.zeros((8, 128), F32)
    for b in range(8):
        blk = jnp.where(lane < 64, o16[0:8, b * 128:(b + 1) * 128], o16[8:16, b * 128:(b + 1) * 128])
        out = jnp.where(row == b, blk, out)
    return out


def decoder_kernel(dims, pos_smem, picked_ref, posrow_ref, in_bias_hbm, out_bias_hbm, b_fc1_hbm, ln_layers_hbm, ln_final_hbm,
                   sk_hbm, sv_hbm, ck_hbm, cv_hbm, emb_hbm, wqkv_hbm, wcq_hbm, wout_hbm, fc1_hbm, fc2_hbm,
                   kvo, eo, fh_ref,
                   in_bias, out_bias, b_fc1, ln_layers, ln_final, kbuf, vbuf, wqkv, wcq, wout, fc1, fc2,
                   xres, stage, stage0, pair, pair0, chips, chips0, full, qscr, oscr, knew, vnew,
                   small_sem, self_sem, cross_sem, w_sem, e_sem, send_sem, recv_sem):
    layers, batch, ctx, frames = dims
    me = lax.axis_index('tp')
    ko, vo = kvo.at[0], kvo.at[1]
    hb = batch // HALVES
    rows_per = 128

    def self_copy(layer, which):
        src, dst = ((sk_hbm, ko), (sv_hbm, vo))[which]
        return pltpu.make_async_copy(src.at[layer], dst.at[layer], self_sem.at[layer, which])

    def cross_copy(layer, which, octet):
        src, dst = ((ck_hbm, kbuf), (cv_hbm, vbuf))[which]
        at = pl.ds(pl.multiple_of(octet * 1024, 1024), 1024)
        return pltpu.make_async_copy(src.at[layer, at, :], dst.at[at, :], cross_sem.at[layer, which, octet])

    weights = ((wqkv_hbm, wqkv), (wout_hbm, wout), (wcq_hbm, wcq), (fc1_hbm, fc1), (fc2_hbm, fc2))

    def w_copy(which, layer):
        src, dst = weights[which]
        return pltpu.make_async_copy(src.at[layer], dst.at[layer], w_sem.at[which, layer])

    small = [pltpu.make_async_copy(src, dst, small_sem.at[i]) for i, (src, dst) in enumerate((
        (ln_layers_hbm, ln_layers), (in_bias_hbm, in_bias), (out_bias_hbm, out_bias), (b_fc1_hbm, b_fc1), (ln_final_hbm, ln_final)))]
    for c in small:
        c.start()
    e_rows = emb_hbm.shape[0] // 4

    def e_copy(i):
        at = pl.ds(i * e_rows, e_rows)
        return pltpu.make_async_copy(emb_hbm.at[at, :], eo.at[at, :], e_sem.at[i])

    pending = []

    def pump(n):
        for group in pending[:n]:
            for c in group:
                c.start()
        del pending[:n]

    for octet in range(batch // 8):
        for which in range(2):
            pending.append([cross_copy(0, which, octet)])
    pending.append([w_copy(3, 0), w_copy(4, 0)])
    pending.append([w_copy(0, 1), w_copy(1, 1), w_copy(2, 1)])
    pending.append([self_copy(1, 0)])
    pending.append([self_copy(1, 1)])
    for octet in range(batch // 8):
        for which in range(2):
            pending.append([cross_copy(1, which, octet)])
    pending.append([w_copy(3, 1), w_copy(4, 1)])
    for i in range(4):
        pending.append([e_copy(i)])

    w_copy(0, 0).start()
    self_copy(0, 0).start()
    self_copy(0, 1).start()
    w_copy(1, 0).start()
    w_copy(2, 0).start()

    barrier = pltpu.get_barrier_semaphore()
    for k in range(1, TP):
        pl.semaphore_signal(barrier, 1, device_id={'tp': lax.rem(me + k, TP)}, device_id_type=MESH)
    pl.semaphore_wait(barrier, TP - 1)

    core = lax.rem(me, 2)
    chip = me // 2
    partner = {'tp': 2 * chip + 1 - core}
    wide = posrow_ref.shape[1] // 2

    def bufs(ph, s):
        if ph == 0:
            return stage0.at[s], pair0.at[s], chips0.at[s], full.at[0, s]
        slot = ph % PARITY
        return stage.at[slot, s], pair.at[slot, s], chips.at[slot, s], full.at[slot, s]

    def send(src, dst, ph, s, step, device):
        pltpu.make_async_remote_copy(src, dst, send_sem.at[ph, s, step], recv_sem.at[ph, s, step], device_id=device, device_id_type=MESH).start()

    def wait_for(ref, sem):
        pltpu.make_async_copy(ref, ref, sem).wait()

    def columns(which):
        return pl.ds(pl.multiple_of(which * wide, 128), wide)

    def sum_start(ph, s, operands):
        mine, got, _, _ = bufs(ph, s)
        lhs, weight = operands
        mine[1] = jnp.dot(lhs, weight[:, columns(1 - core)], preferred_element_type=F32)
        send(mine.at[1], got, ph, s, 0, partner)
        mine[0] = jnp.dot(lhs, weight[:, columns(core)], preferred_element_type=F32)

    def sum_chips(ph, s):
        mine, got, by_chip, _ = bufs(ph, s)
        wait_for(got, recv_sem.at[ph, s, 0])
        by_chip[chip] = mine[0] + got[...]
        for other in (TP // 2 - 1 - chip, chip + 1 - 2 * lax.rem(chip, 2), lax.rem(chip + 2, TP // 2)):
            send(by_chip.at[chip], by_chip.at[chip], ph, s, 1, {'tp': 2 * other + core})
        wait_for(got, send_sem.at[ph, s, 0])

    def sum_share(ph, s):
        _, _, by_chip, both = bufs(ph, s)
        others = by_chip.at[pl.ds(0, TP // 2 - 1)]
        wait_for(others, recv_sem.at[ph, s, 1])
        total = by_chip[0].astype(F32)
        for q in range(1, TP // 2):
            total = total + by_chip[q].astype(F32)
        both[core] = total.astype(BF16)
        send(both.at[core], both.at[core], ph, s, 2, partner)
        wait_for(others, send_sem.at[ph, s, 1])

    def sum_finish(ph, s):
        both = bufs(ph, s)[3]
        wait_for(both.at[0], recv_sem.at[ph, s, 2])
        wait_for(both.at[0], send_sem.at[ph, s, 2])
        return jnp.concatenate([both[0].astype(F32), both[1].astype(F32)], axis=1)

    def head_bias(layer, which):
        b = in_bias[layer, which]
        return jnp.concatenate([b[0:1, :], b[1:2, :]], axis=1)

    def half(s):
        return pl.ds(s * hb, hb)

    def self_block(layer, s, early, late):
        hidden = norm_rows(xres[half(s), :], ln_layers[layer, 0])
        proj = lax.dot_general(hidden, wqkv[layer], NT, preferred_element_type=F32)
        qscr[half(s), :] = (proj[:, 0:128] + head_bias(layer, 0)).astype(BF16).astype(F32)
        knew[layer, half(s), :] = proj[:, 128:256].astype(BF16).astype(F32)
        vnew[layer, half(s), :] = (proj[:, 256:384] + head_bias(layer, 1)).astype(BF16).astype(F32)

        for i in range(hb // 8):
            octet = s * (hb // 8) + i
            r8 = pl.ds(octet * 8, 8)
            at = pl.ds(octet * 1024, 1024)
            both, qbd = block_diag(qscr[r8, :])
            seq = lax.rem(lax.broadcasted_iota(jnp.int32, (16, 1), 0), 8)
            limit = jnp.zeros((16, 1), jnp.int32)
            for b in range(8):
                limit = jnp.where(seq == b, pos_smem[octet * 8 + b], limit)
            past = jnp.dot(qbd, ko[layer, at, :], preferred_element_type=F32) * 0.125
            t = lax.broadcasted_iota(jnp.int32, (16, ctx), 1)
            past = jnp.where(t < limit, past, -1e30)
            kn = knew[layer, r8, :]
            vn = vnew[layer, r8, :]
            new = jnp.sum(both * jnp.concatenate([kn, kn], axis=0), axis=1, keepdims=True) * 0.125
            peak = jnp.maximum(jnp.max(past, axis=1, keepdims=True), new)
            past_e = jnp.exp(past - peak)
            new_e = jnp.exp(new - peak)
            denom = jnp.sum(past_e, axis=1, keepdims=True) + new_e
            past_w = (past_e / denom).astype(BF16)
            new_w = (new_e / denom).astype(BF16).astype(F32)
            o16 = lax.dot_general(past_w, vo[layer, at, :], NT, preferred_element_type=F32)
            lane = lax.broadcasted_iota(jnp.int32, (8, 128), 1)
            oscr[r8, :] = fold_heads(o16) + jnp.where(lane < 64, new_w[0:8], new_w[8:16]) * vn
        return oscr[half(s), :].astype(BF16), wout.at[layer, 0]

    def cross_block(layer, s, early, late):
        hidden = norm_rows(xres[half(s), :], ln_layers[layer, 1])
        proj = lax.dot_general(hidden, wcq[layer], NT, preferred_element_type=F32)
        qscr[half(s), :] = (proj + head_bias(layer, 2)).astype(BF16).astype(F32)

        octets = range(s * (hb // 8), (s + 1) * (hb // 8))
        for octet in octets:
            cross_copy(layer, 0, octet).wait()
        scores = []
        for octet in octets:
            _, qbd = block_diag(qscr[pl.ds(octet * 8, 8), :])
            scores.append(jnp.dot(qbd, kbuf[pl.ds(octet * 1024, 1024), :], preferred_element_type=F32) * 0.125)
            if octet == octets[0]:
                early()
        for octet in octets:
            cross_copy(layer, 1, octet).wait()
        for octet, sc in zip(octets, scores):
            exps = jnp.exp(sc - jnp.max(sc, axis=1, keepdims=True))
            w = (exps * (1.0 / jnp.sum(exps, axis=1, keepdims=True))).astype(BF16)
            if octet == octets[-1]:
                late()
            o16 = lax.dot_general(w, vbuf[pl.ds(octet * 1024, 1024), :], NT, preferred_element_type=F32)
            oscr[pl.ds(octet * 8, 8), :] = fold_heads(o16)
        return oscr[half(s), :].astype(BF16), wout.at[layer, 1]

    def mlp_block(layer, s, early, late):
        hidden = norm_rows(xres[half(s), :], ln_layers[layer, 2])
        pre = jnp.dot(hidden, fc1[layer], preferred_element_type=F32) + b_fc1[layer:layer + 1, :]
        active = (0.5 * pre * (1.0 + lax.erf(pre * (0.5 ** 0.5)))).astype(BF16)
        return active, fc2.at[layer]

    def write_new(layer, s):
        t = lax.broadcasted_iota(jnp.int32, (rows_per, ctx), 1)
        for new, cache in ((knew, ko), (vnew, vo)):
            cols = new[layer, half(s), :].T
            for i in range(hb):
                b = s * hb + i
                at = pl.ds(b * rows_per, rows_per)
                old = cache[layer, at, :].astype(F32)
                cache[layer, at, :] = jnp.where(t == pos_smem[b], cols[:, i:i + 1], old).astype(BF16)

    def nothing():
        pass

    def ready(nl, nk):
        if nk == 0:
            w_copy(0, nl).wait()
            self_copy(nl, 0).wait()
            self_copy(nl, 1).wait()
            w_copy(1, nl).wait()
        if nk == 1:
            w_copy(2, nl).wait()
        if nk == 2:
            w_copy(3, nl).wait()
            w_copy(4, nl).wait()

    for s in range(2):
        mine, got = stage0.at[s], pair0.at[s]
        mine[0] = picked_ref[half(s), columns(core)]
        mine[1] = picked_ref[half(s), columns(1 - core)]
        send(mine.at[1], got, 0, s, 0, partner)
    pump(9)
    for s in range(2):
        sum_chips(0, s)
    for c in small:
        c.wait()
    for s in range(2):
        sum_share(0, s)
    for ph in range(3 * layers + 1):
        layer, kind = divmod(ph, 3)
        before, prev_kind = divmod(ph - 1, 3)

        def update(s):
            total = sum_finish(ph, s)
            if ph == 0:
                xres[half(s), :] = total + posrow_ref[half(s), :]
            else:
                xres[half(s), :] = xres[half(s), :] + total + out_bias[prev_kind, before:before + 1, :]

        if ph == 3 * layers:
            sum_share(ph, 1)
            for s in range(2):
                update(s)
                fh_ref[half(s), :] = norm_rows(xres[half(s), :], ln_final)
            break
        block = (self_block, cross_block, mlp_block)[kind]
        update(0)
        ready(layer, kind)
        share = functools.partial(sum_share, ph, 1)
        gather = functools.partial(sum_chips, ph + 1, 0)
        if kind == 1:
            sum_start(ph + 1, 0, block(layer, 0, nothing, share))
            update(1)
            sum_start(ph + 1, 1, block(layer, 1, gather, nothing))
        else:
            sum_start(ph + 1, 0, block(layer, 0, nothing, nothing))
            if kind == 2:
                write_new(layer, 0)
                gather()
                share()
                write_new(layer, 1)
            else:
                if ph > 0:
                    share()
                gather()
            if ph == 0:
                pump(3)
            if ph == 2:
                pump(4)
            update(1)
            sum_start(ph + 1, 1, block(layer, 1, nothing, nothing))
        sum_chips(ph + 1, 1)
        if ph == 1:
            pump(9)
        sum_share(ph + 1, 0)
    for i in range(4):
        e_copy(i).wait()


def final_kernel(kv_ref, e_ref, fh_ref, logits_hbm, ko_hbm, vo_hbm, logits, sem, out_sem):
    layers, rows = kv_ref.shape[1:3]
    copies = []
    for layer in range(layers):
        for which, dst in enumerate((ko_hbm, vo_hbm)):
            for part in range(4):
                at = pl.ds(part * (rows // 4), rows // 4)
                c = pltpu.make_async_copy(kv_ref.at[which, layer, at, :], dst.at[layer, at, :], sem.at[layer, which, part])
                c.start()
                copies.append(c)
    fh = fh_ref[...]
    step = 384
    n = e_ref.shape[0] // step

    def out_copy(i):
        at = pl.ds(pl.multiple_of(i * step, step), step)
        return pltpu.make_async_copy(logits.at[:, at], logits_hbm.at[:, at], out_sem)

    def body(i, carry):
        at = pl.ds(pl.multiple_of(i * step, step), step)
        logits[:, at] = lax.dot_general(fh, e_ref[at, :], NT, preferred_element_type=F32)
        out_copy(i).start()
        return carry

    lax.fori_loop(0, n, body, 0)
    pltpu.make_async_copy(logits, logits_hbm, out_sem).wait()
    for c in copies:
        c.wait()


def solution(mesh):
    vm = pl.BlockSpec(memory_space=pltpu.VMEM)
    sm = pl.BlockSpec(memory_space=pltpu.SMEM)
    hbm = pl.BlockSpec(memory_space=pltpu.HBM)

    def local_step(tokens, positions, self_keys, self_vals, cross_keys, cross_vals, embed_table, pos_table, w_qkv, w_cq, in_bias, w_out, out_bias, w_fc1, b_fc1, w_fc2, ln_layers, ln_final):
        batch = tokens.shape[0]
        layers, _, ctx, heads, hd = self_keys.shape
        frames = cross_keys.shape[2]
        vocab, d = embed_table.shape
        ff = w_fc1.shape[2]
        rows = batch * heads * hd
        hb = batch // HALVES

        def flat(cache):
            return cache.transpose(0, 1, 3, 4, 2).reshape(layers, rows, cache.shape[2])

        picked, posrow = pl.pallas_call(
            gather_kernel,
            out_shape=(pltpu.VMEM((batch, d), BF16), pltpu.VMEM((batch, d), F32)),
            in_specs=[sm, sm, vm, vm, hbm, hbm], out_specs=(vm, vm),
            scratch_shapes=[pltpu.VMEM((16 * batch, d), BF16), pltpu.VMEM((16 * batch, d), BF16), pltpu.SemaphoreType.DMA((2,))],
            compiler_params=pltpu.CompilerParams(vmem_limit_bytes=60 * 2 ** 20),
            name='gather_rows',
        )(tokens, positions, tokens.reshape(1, batch), positions.reshape(1, batch), embed_table, pos_table)

        picked, posrow = (pltpu.with_memory_space_constraint(a, pltpu.VMEM) for a in (picked, posrow))
        kvo, eo, fh = pl.pallas_call(
            functools.partial(decoder_kernel, (layers, batch, ctx, frames)),
            out_shape=(pltpu.VMEM((2, layers, rows, ctx), BF16), pltpu.VMEM((vocab, d), BF16), pltpu.VMEM((batch, d), BF16)),
            in_specs=[sm] + [vm] * 2 + [hbm] * 15,
            out_specs=(vm, vm, vm),
            scratch_shapes=[
                pltpu.VMEM(in_bias.shape, F32), pltpu.VMEM((3, layers, d), F32), pltpu.VMEM(b_fc1.shape, F32), pltpu.VMEM(ln_layers.shape, F32), pltpu.VMEM(ln_final.shape, F32),
                pltpu.VMEM((rows, frames), BF16), pltpu.VMEM((rows, frames), BF16),
                pltpu.VMEM((layers, 3 * heads * hd, d), BF16), pltpu.VMEM((layers, heads * hd, d), BF16),
                pltpu.VMEM((layers, 2, heads * hd, d), BF16), pltpu.VMEM((layers, d, ff), BF16), pltpu.VMEM((layers, ff, d), BF16),
                pltpu.VMEM((batch, d), F32),
                pltpu.VMEM((PARITY, HALVES, 2, hb, d // 2), F32), pltpu.VMEM((HALVES, 2, hb, d // 2), BF16),
                pltpu.VMEM((PARITY, HALVES, hb, d // 2), F32), pltpu.VMEM((HALVES, hb, d // 2), BF16),
                pltpu.VMEM((PARITY, HALVES, TP // 2, hb, d // 2), F32), pltpu.VMEM((HALVES, TP // 2, hb, d // 2), BF16),
                pltpu.VMEM((PARITY, HALVES, 2, hb, d // 2), BF16),
                pltpu.VMEM((batch, 128), F32), pltpu.VMEM((batch, 128), F32),
                pltpu.VMEM((layers, batch, 128), F32), pltpu.VMEM((layers, batch, 128), F32),
                pltpu.SemaphoreType.DMA((5,)), pltpu.SemaphoreType.DMA((layers, 2)), pltpu.SemaphoreType.DMA((layers, 2, batch // 8)),
                pltpu.SemaphoreType.DMA((5, layers)), pltpu.SemaphoreType.DMA((4,)),
                pltpu.SemaphoreType.DMA((3 * layers + 1, HALVES, 3)), pltpu.SemaphoreType.DMA((3 * layers + 1, HALVES, 3)),
            ],
            compiler_params=pltpu.CompilerParams(collective_id=0, has_side_effects=True, vmem_limit_bytes=139 * 2 ** 18),
            name='decoder_layers',
        )(positions, picked, posrow, in_bias, out_bias.transpose(1, 0, 2), b_fc1, ln_layers, ln_final,
          flat(self_keys), flat(self_vals), flat(cross_keys), flat(cross_vals), embed_table,
          w_qkv.transpose(0, 2, 3, 4, 1).reshape(layers, 3 * heads * hd, d), w_cq.transpose(0, 2, 3, 1).reshape(layers, heads * hd, d),
          w_out.reshape(layers, 2, heads * hd, d), w_fc1, w_fc2)

        logits, nk, nv = pl.pallas_call(
            final_kernel,
            out_shape=(jax.ShapeDtypeStruct((batch, vocab), F32), jax.ShapeDtypeStruct((layers, rows, ctx), BF16), jax.ShapeDtypeStruct((layers, rows, ctx), BF16)),
            in_specs=[vm] * 3, out_specs=(hbm, hbm, hbm),
            scratch_shapes=[pltpu.VMEM((batch, vocab), F32), pltpu.SemaphoreType.DMA((layers, 2, 4)), pltpu.SemaphoreType.DMA],
            compiler_params=pltpu.CompilerParams(vmem_limit_bytes=2 * 2 ** 20),
            name='final_logits',
        )(kvo, eo, fh)

        def unflat(cache):
            return cache.reshape(layers, batch, heads, hd, ctx).transpose(0, 1, 4, 2, 3)

        return logits, unflat(nk), unflat(nv)

    batch_spec = P('dp')
    cache_spec = P(None, 'dp', None, 'tp', None)
    in_specs = (batch_spec, batch_spec, cache_spec, cache_spec, cache_spec, cache_spec, P('tp', None), P(None, None), P(None, None, None, 'tp', None), P(None, None, 'tp', None), P(None, None, 'tp', None), P(None, None, 'tp', None, None), P(None, None, None), P(None, None, 'tp'), P(None, 'tp'), P(None, 'tp', None), P(None, None, None, None), P(None, None))
    out_specs = (P('dp', 'tp'), cache_spec, cache_spec)
    return jax.shard_map(local_step, mesh=mesh, in_specs=in_specs, out_specs=out_specs, check_vma=False)
```
